32 devices in a mesh: gx: 4 (over y, x), gy: 2 (over core), gz: 4 (over z).
Axes of the slice: x: 2, y: 2, z: 4, core: 2. Of those that a mesh axis runs over, the one named last changes fastest.
Arguments:
- right_side: float32 [8, 32, 64, 512], P(None, 'gx', 'gy', 'gz'), may hold values from -12 to 12
- shift: float32 [32, 64, 512], P('gx', 'gy', 'gz'), may hold values from 0.02 to 2
Outputs:
- solution_block: float32 [8, 32, 64, 512], P(None, 'gx', 'gy', 'gz')
- residual_norms: float32 [8], replicated
The draws below stay inside these ranges and needn't reach their ends.
All inputs are finite; a program needn't handle non-finite values.
Results may differ from the reference program's by a relative error of at most 0.0003.
Values sent between devices are 32-bit elements; how exact they have to be, the bound alone decides.
No kernel may reach another device: no remote copies, remote signals or barrier semaphores. Data moves between devices by JAX's collectives and lax.ppermute only.
A program may use at most 128 MiB of HBM per device.

```python
import math
import jax
import jax.numpy as jnp
from jax import lax

S = 8
ITERS = 2
NX = 32
NY = 64
NZ = 512


def draw_right_side(key, part):
    first = jax.random.fold_in(key, 11)
    ramp_x = jnp.arange(NX, dtype=jnp.float32)[:, None, None] / NX
    ramp_y = jnp.arange(NY, dtype=jnp.float32)[None, :, None] / NY
    ramp_z = jnp.arange(NZ, dtype=jnp.float32)[None, None, :] / NZ
    ramp = 1.0 + (ramp_x + ramp_y + ramp_z) * 2.0 / 3.0
    values = jax.random.normal(first, (S, NX, NY, NZ), jnp.float32) * ramp[None]
    return jnp.clip(values, -12.0, 12.0)


def level_of(key, dims, cuts, low, top_value):
    gain, own = 1.0, jax.random.fold_in(key, 6)
    for dim, parts in cuts:
        heights = jnp.exp(jax.random.uniform(jax.random.fold_in(own, dim), (parts,), jnp.float32, low / len(cuts), top_value / len(cuts)))
        gain = gain * jnp.repeat(heights, dims[dim] // parts).reshape([-1 if axis == dim else 1 for axis in range(len(dims))])
    return gain


def setup_inputs(seed: int = 0) -> dict:
    key_of = jax.random.split(jax.random.key(seed), 3)
    right_side = draw_right_side(jax.random.fold_in(key_of[2], 71), 0)
    shift = jnp.clip(jnp.exp(math.log(2.0) - 4.6051702 * jax.random.uniform(key_of[1], (NX, NY, NZ), jnp.float32) ** level_of(key_of[1], (NX, NY, NZ), ((0, 4), (1, 2), (2, 4)), -0.2, 0.2)), 0.02, 2.0)
    return dict(right_side=right_side, shift=shift)


def operate(fields, shift):
    padded = jnp.pad(fields, ((0, 0), (1, 1), (1, 1), (1, 1)))
    beside = padded[:, 2:, 1:-1, 1:-1] + padded[:, :-2, 1:-1, 1:-1]
    beside = beside + padded[:, 1:-1, 2:, 1:-1] + padded[:, 1:-1, :-2, 1:-1]
    beside = beside + padded[:, 1:-1, 1:-1, 2:] + padded[:, 1:-1, 1:-1, :-2]
    return (6.0 + shift)[None] * fields - beside

def lower_inverse(lower):
    count = lower.shape[0]
    return jax.scipy.linalg.solve_triangular(lower, jnp.eye(count, dtype=lower.dtype), lower=True)

def small_dot(left, right):
    return jnp.dot(left, right, precision=lax.Precision.HIGHEST)

def reference(right_side, shift):
    width = right_side.shape[0]
    shape = right_side.shape
    rows = right_side.reshape(width, -1)
    gram = small_dot(rows, rows.T)
    lower = jnp.linalg.cholesky(gram)
    start_coeff = lower.T
    basis = [small_dot(lower_inverse(lower), rows)]
    hessen = jnp.zeros(((ITERS + 1) * width, ITERS * width), jnp.float32)
    for step in range(ITERS):
        image = operate(basis[step].reshape(shape), shift).reshape(width, -1)
        stacked = jnp.concatenate(basis, axis=0)
        products = small_dot(jnp.concatenate([stacked, image], axis=0), image.T)
        coeffs = products[:-width]
        gram = products[-width:] - small_dot(coeffs.T, coeffs)
        lower = jnp.linalg.cholesky(gram)
        hessen = hessen.at[:(step + 1) * width, step * width:(step + 1) * width].set(coeffs)
        hessen = hessen.at[(step + 1) * width:(step + 2) * width, step * width:(step + 1) * width].set(lower.T)
        if step + 1 < ITERS:
            projected = image - small_dot(coeffs.T, stacked)
            basis.append(small_dot(lower_inverse(lower), projected))
    target = jnp.zeros(((ITERS + 1) * width, width), jnp.float32).at[:width].set(start_coeff)
    normal = small_dot(hessen.T, hessen)
    factor = jnp.linalg.cholesky(normal)
    coeff_y = jax.scipy.linalg.cho_solve((factor, True), small_dot(hessen.T, target))
    solution = small_dot(coeff_y.T, jnp.concatenate(basis, axis=0)).reshape(shape)
    leftover = target - small_dot(hessen, coeff_y)
    norms = jnp.sqrt(lax.optimization_barrier(jnp.sum(leftover * leftover, axis=0)))
    return (solution, norms)
```

```python
import functools

import jax
import jax.numpy as jnp
from jax import lax
from jax.experimental import pallas as pl
from jax.experimental.pallas import tpu as pltpu
from jax.sharding import PartitionSpec as P

AXES = ("gx", "gy", "gz")
CENTRE = 7.0
LANES = 128
F32 = jnp.float32


def swap_pairs(count):
    first = [(i, j) for a in range(0, count - 1, 2) for i, j in ((a, a + 1), (a + 1, a))]
    second = [(i, j) for a in range(1, count - 1, 2) for i, j in ((a, a + 1), (a + 1, a))]
    return [pairs for pairs in (first, second) if pairs]


def rounds_of():
    return tuple(len(swap_pairs(lax.axis_size(axis))) for axis in AXES)


def parity(axis):
    return lax.rem(lax.axis_index(axis), 2) == 1


def write_xy_faces(v_ref, x_refs, y_refs):
    width, nx, ny, _ = v_ref.shape
    odd_x, odd_y = parity("gx"), parity("gy")
    for k, ref in enumerate(x_refs):
        high = jnp.logical_xor(odd_x, k == 0)
        ref[...] = v_ref[:, jnp.where(high, nx - 1, 0)]
    for k, ref in enumerate(y_refs):
        high = jnp.logical_xor(odd_y, k == 0)
        ref[...] = jnp.where(high, v_ref[:, :, ny - 1 : ny, :], v_ref[:, :, 0:1, :])


def packed_ends(tile, m, packed, lane):
    at = 2 * m
    hit = (lane == at) | (lane == lax.rem(at + LANES - 1, LANES))
    return jnp.where(hit, pltpu.roll(tile, at, 1), packed)


def pack_kernel(nx_r, ny_r, v_ref, *refs):
    width, nx, ny, _ = v_ref.shape
    x_refs, y_refs, z_ref = refs[:nx_r], refs[nx_r : nx_r + ny_r], refs[nx_r + ny_r]
    write_xy_faces(v_ref, x_refs, y_refs)
    lane = lax.broadcasted_iota(jnp.int32, (ny, LANES), 1)

    def field(f, packed):
        for x in range(nx):
            packed = packed_ends(v_ref[f, x], f * nx + x, packed, lane)
        return packed

    z_ref[...] = lax.fori_loop(0, width, field, jnp.zeros((ny, LANES), F32))


def pick(odd, refs, load):
    first = load(refs[0]) if refs else 0.0
    second = load(refs[1]) if len(refs) > 1 else jnp.zeros_like(first)
    return jnp.where(odd, first, second), jnp.where(odd, second, first)


def apply_operator(v_ref, shift_ref, x_in, y_in, z_in, out_ref, packed=None):
    width, nx, ny, _ = v_ref.shape
    odd_x, odd_y, odd_z = parity("gx"), parity("gy"), parity("gz")
    lane = lax.broadcasted_iota(jnp.int32, (ny, LANES), 1)
    row = lax.broadcasted_iota(jnp.int32, (ny, LANES), 0)
    low_z, high_z = pick(odd_z, z_in, lambda ref: ref[...])
    ends = jnp.where(
        lax.rem(lane, 2) == 0, pltpu.roll(low_z, 1, 1), pltpu.roll(high_z, LANES - 1, 1)
    )

    def field(f, packed):
        low_x, high_x = pick(odd_x, x_in, lambda ref: ref[f])
        for x in range(nx):
            m = f * nx + x
            low_y, high_y = pick(odd_y, y_in, lambda ref: ref[f, x])
            v = v_ref[f, x]
            end = pltpu.roll(ends, lax.rem(LANES - 2 * m, LANES), 1)
            beside = (v_ref[f, x - 1] if x > 0 else low_x) + (v_ref[f, x + 1] if x < nx - 1 else high_x)
            beside += jnp.where(row == 0, low_y, pltpu.roll(v, 1, 0))
            beside += jnp.where(row == ny - 1, high_y, pltpu.roll(v, ny - 1, 0))
            beside += jnp.where(lane == 0, end, pltpu.roll(v, 1, 1))
            beside += jnp.where(lane == LANES - 1, end, pltpu.roll(v, LANES - 1, 1))
            out = ((6.0 - CENTRE) + shift_ref[x]) * v - beside
            out_ref[f, x] = out
            if packed is not None:
                packed = packed_ends(out, m, packed, lane)
        return packed

    if packed is None:
        lax.fori_loop(0, width, lambda f, c: (field(f, None), c)[1], 0)
        return None
    return lax.fori_loop(0, width, field, packed)


def operator_kernel(nx_r, ny_r, nz_r, *refs):
    v_ref, shift_ref = refs[:2]
    at = 2
    x_in, y_in, z_in = refs[at : at + nx_r], refs[at + nx_r : at + nx_r + ny_r], refs[at + nx_r + ny_r : at + nx_r + ny_r + nz_r]
    outs = refs[at + nx_r + ny_r + nz_r :]
    out_ref = outs[0]
    x_out, y_out, z_out = outs[1 : 1 + nx_r], outs[1 + nx_r : 1 + nx_r + ny_r], outs[1 + nx_r + ny_r]
    ny = v_ref.shape[2]
    z_out[...] = apply_operator(v_ref, shift_ref, x_in, y_in, z_in, out_ref, jnp.zeros((ny, LANES), F32))
    write_xy_faces(out_ref, x_out, y_out)


def add_moment(a_ref, b_ref, at, payload):
    width, nx, ny, _ = a_ref.shape
    pairs = [(i, j) for i in range(width) for j in range(i + 1)]

    def plane(x, sums):
        sums = list(sums)
        for y in range(0, ny, 8):
            a = [a_ref[f, x, y : y + 8, :] for f in range(width)]
            b = a if b_ref is a_ref else [b_ref[f, x, y : y + 8, :] for f in range(width)]
            for k, (i, j) in enumerate(pairs):
                sums[k] = sums[k] + a[i] * b[j]
        return tuple(sums)

    sums = lax.fori_loop(0, nx, plane, tuple(jnp.zeros((8, LANES), F32) for _ in pairs))
    rows = {}
    for (i, j), value in zip(pairs, sums):
        rows[i, j] = rows[j, i] = jnp.sum(value, axis=0, keepdims=True)
    lane = lax.broadcasted_iota(jnp.int32, (8, LANES), 1)
    for i in range(width):
        column = jnp.sum(jnp.concatenate([rows[i, j] for j in range(width)], axis=0), axis=1, keepdims=True)
        payload = jnp.where(lane == at + i, column, payload)
    return payload


def early_moments_kernel(b_ref, u_ref, out_ref):
    width = b_ref.shape[0]
    payload = add_moment(b_ref, b_ref, 0, jnp.zeros((8, LANES), F32))
    payload = add_moment(b_ref, u_ref, width, payload)
    out_ref[...] = add_moment(u_ref, u_ref, 2 * width, payload)


def late_moments_kernel(nx_r, ny_r, nz_r, *refs):
    u_ref, shift_ref = refs[:2]
    at = 2
    x_in, y_in, z_in = refs[at : at + nx_r], refs[at + nx_r : at + nx_r + ny_r], refs[at + nx_r + ny_r : at + nx_r + ny_r + nz_r]
    early_ref, out_ref, t_ref = refs[at + nx_r + ny_r + nz_r :]
    width = u_ref.shape[0]
    apply_operator(u_ref, shift_ref, x_in, y_in, z_in, t_ref)
    payload = add_moment(u_ref, t_ref, 3 * width, early_ref[...])
    payload = add_moment(t_ref, t_ref, 4 * width, payload)
    out_ref[...] = jnp.broadcast_to(payload[None], out_ref.shape)


def lanes_of(matrix, j):
    return jnp.broadcast_to(matrix[:, j : j + 1], matrix.shape)


def rows_of(matrix, i):
    return jnp.broadcast_to(matrix[i : i + 1, :], matrix.shape)


def times(left, at, right):
    count = left.shape[0]
    total = lanes_of(left, at) * rows_of(right, 0)
    for k in range(1, count):
        total = total + lanes_of(left, at + k) * rows_of(right, k)
    return total


def shift_lanes(matrix, by):
    return pltpu.roll(matrix, by % LANES, 1)


def eliminate(blocks):
    size = blocks[0].shape[0]
    sub = lax.broadcasted_iota(jnp.int32, blocks[0].shape, 0)
    for j in range(size * len(blocks)):
        own, local = divmod(j, size)
        columns = [lanes_of(block, j) for block in blocks]
        pivot = rows_of(blocks[own], local) / rows_of(columns[own], local)
        blocks = [block - column * pivot for block, column in zip(blocks, columns)]
        blocks[own] = jnp.where(sub == local, pivot, blocks[own])
    return blocks


def small_algebra(s):
    n = s.shape[0]
    c0 = CENTRE
    lane = lax.broadcasted_iota(jnp.int32, s.shape, 1)
    sub = lax.broadcasted_iota(jnp.int32, s.shape, 0)
    n0, n1, n2, n3, n4 = shift_lanes(s, n), s, shift_lanes(s, -n), shift_lanes(s, -2 * n), shift_lanes(s, -3 * n)
    (e,) = eliminate([s])
    p1 = times(s, n, e)
    p2 = times(s, 2 * n, e)
    p3 = times(s, 3 * n, e)
    cc = times(e, n, e)
    e2c = times(e, 2 * n, e)
    g = n2 - p1
    q = shift_lanes(e, -n) - cc
    n3c = n3 - p2
    f3 = n3c - times(s, n, q)
    f4 = n4 - p3 - times(s, n, shift_lanes(e, -2 * n) - e2c)
    m11 = n2 + 2.0 * c0 * n1 + c0 * c0 * n0
    m12 = n3c + 2.0 * c0 * g
    m21 = n3 - shift_lanes(p1, -n) + 2.0 * c0 * g
    m22 = f4 + 2.0 * c0 * f3 + c0 * c0 * g
    r1 = n1 + c0 * n0

    def assemble(first, second, third):
        joined = jnp.where(lane < n, shift_lanes(first, -n), second)
        return jnp.where(lane < 2 * n, joined, shift_lanes(third, n))

    pa, qa = eliminate([assemble(m11, m12, r1), assemble(m21, m22, g)])
    cq = times(e, n, qa)
    on_b = pa - cq
    unit = jnp.where(lane == sub + 2 * n, 1.0, 0.0)
    part = unit - times(e, n, pa) - c0 * pa - times(q, n, qa)
    squares = part * times(s, 0, part)
    pq = pa + c0 * qa
    squares = squares + pq * (times(g, n, pq) + 2.0 * times(f3, n, qa))
    squares = squares + qa * times(f4 - times(g, n, q), n, qa)
    return on_b, qa, jnp.sum(squares, axis=0, keepdims=True)


def finish_kernel(parts_ref, b_ref, u_ref, out_ref, norms_ref, coeff_ref):
    width, nx, ny, _ = b_ref.shape
    n = width
    total = jnp.sum(parts_ref[...], axis=0)
    on_b, on_u, squares = small_algebra(total)
    norms_ref[...] = jnp.sqrt(shift_lanes(squares, -2 * n))[:, :n]
    for f in range(width):
        coeff_ref[0, f] = lanes_of(on_b, 2 * n + f)
        coeff_ref[1, f] = lanes_of(on_u, 2 * n + f)
    group = 2

    def fields(k, carry):
        first = [[[rows_of(coeff_ref[h, group * k + d], g) for g in range(width)] for h in range(2)] for d in range(group)]

        def plane(x, carry):
            for y in range(0, ny, 8):
                b = [b_ref[g, x, y : y + 8, :] for g in range(width)]
                u = [u_ref[g, x, y : y + 8, :] for g in range(width)]
                for d in range(group):
                    total = first[d][0][0] * b[0] + first[d][1][0] * u[0]
                    for g in range(1, width):
                        total = total + (first[d][0][g] * b[g] + first[d][1][g] * u[g])
                    out_ref[group * k + d, x, y : y + 8, :] = total
            return carry

        return lax.fori_loop(0, nx, plane, carry)

    lax.fori_loop(0, width // group, fields, 0)


def call(kernel, out_shape, operands, scratch=(), flops=1_000_000, name=None):
    return pl.pallas_call(
        kernel,
        out_shape=out_shape,
        in_specs=[pl.BlockSpec(memory_space=pltpu.VMEM)] * len(operands),
        out_specs=jax.tree.map(lambda _: pl.BlockSpec(memory_space=pltpu.VMEM), out_shape),
        scratch_shapes=list(scratch),
        cost_estimate=pl.CostEstimate(flops=flops, bytes_accessed=1 << 20, transcendentals=0),
        name=name,
    )(*operands)


def trade(x_faces, y_faces, ends):
    pairs_x, pairs_y, pairs_z = (swap_pairs(lax.axis_size(axis)) for axis in AXES)
    got_x = [lax.ppermute(face, "gx", pairs) for face, pairs in zip(x_faces, pairs_x)]
    got_z = [lax.ppermute(ends, "gz", pairs) for pairs in pairs_z]
    got_y = [lax.ppermute(face, "gy", pairs) for face, pairs in zip(y_faces, pairs_y)]
    return [*got_x, *got_y, *got_z]


def body(right_side, shift):
    width, nx, ny, nz = right_side.shape
    assert width == 8 and nz == LANES and ny % 8 == 0 and width * nx <= LANES // 2
    nx_r, ny_r, nz_r = rounds_of()
    devices = 1
    for axis in AXES:
        devices *= lax.axis_size(axis)
    block = jax.ShapeDtypeStruct(right_side.shape, F32)
    faces = [jax.ShapeDtypeStruct((width, ny, nz), F32)] * nx_r
    faces += [jax.ShapeDtypeStruct((width, nx, 1, nz), F32)] * ny_r
    faces += [jax.ShapeDtypeStruct((ny, LANES), F32)]

    packed = call(functools.partial(pack_kernel, nx_r, ny_r), faces, [right_side], name="pack")
    halo = trade(packed[:nx_r], packed[nx_r : nx_r + ny_r], packed[-1])
    u, *packed = call(
        functools.partial(operator_kernel, nx_r, ny_r, nz_r), [block, *faces], [right_side, shift, *halo], name="operator"
    )
    halo = trade(packed[:nx_r], packed[nx_r : nx_r + ny_r], packed[-1])
    early = call(
        early_moments_kernel, jax.ShapeDtypeStruct((8, LANES), F32), [right_side, u], flops=30_000_000, name="early"
    )
    copies = call(
        functools.partial(late_moments_kernel, nx_r, ny_r, nz_r),
        jax.ShapeDtypeStruct((devices, 8, LANES), F32),
        [u, shift, *halo, early],
        scratch=[pltpu.VMEM(right_side.shape, F32)],
        name="late",
    )
    parts = lax.all_to_all(copies, AXES, 0, 0, tiled=True)
    out, norms = call(
        finish_kernel,
        [block, jax.ShapeDtypeStruct((1, width), F32)],
        [parts, right_side, u],
        scratch=[pltpu.VMEM((2, width, 8, LANES), F32)],
        name="finish",
    )
    return out, norms.reshape(width)


def solution(mesh):
    in_specs = (P(None, "gx", "gy", "gz"), P("gx", "gy", "gz"))
    out_specs = (P(None, "gx", "gy", "gz"), P())
    return jax.shard_map(body, mesh=mesh, in_specs=in_specs, out_specs=out_specs, check_vma=False)
```

```python
import functools

import jax
import jax.numpy as jnp
from jax import lax
from jax.experimental import pallas as pl
from jax.experimental.pallas import tpu as pltpu
from jax.sharding import PartitionSpec as P

AXES = ("gx", "gy", "gz")
CENTRE = 7.0
LANES = 128
F32 = jnp.float32


def swap_pairs(count):
    first = [(i, j) for a in range(0, count - 1, 2) for i, j in ((a, a + 1), (a + 1, a))]
    second = [(i, j) for a in range(1, count - 1, 2) for i, j in ((a, a + 1), (a + 1, a))]
    return [pairs for pairs in (first, second) if pairs]


def rounds_of():
    return tuple(len(swap_pairs(lax.axis_size(axis))) for axis in AXES)


def parity(axis):
    return lax.rem(lax.axis_index(axis), 2) == 1


def write_xy_faces(v_ref, x_refs, y_refs):
    width, nx, ny, _ = v_ref.shape
    odd_x, odd_y = parity("gx"), parity("gy")
    for k, ref in enumerate(x_refs):
        high = jnp.logical_xor(odd_x, k == 0)
        ref[...] = v_ref[:, jnp.where(high, nx - 1, 0)]
    for k, ref in enumerate(y_refs):
        high = jnp.logical_xor(odd_y, k == 0)
        ref[...] = jnp.where(high, v_ref[:, :, ny - 1 : ny, :], v_ref[:, :, 0:1, :])


def packed_ends(tile, m, packed, lane):
    at = 2 * m
    hit = (lane == at) | (lane == lax.rem(at + LANES - 1, LANES))
    return jnp.where(hit, pltpu.roll(tile, at, 1), packed)


def pack_kernel(nx_r, ny_r, v_ref, *refs):
    width, nx, ny, _ = v_ref.shape
    x_refs, y_refs, z_ref = refs[:nx_r], refs[nx_r : nx_r + ny_r], refs[nx_r + ny_r]
    write_xy_faces(v_ref, x_refs, y_refs)
    lane = lax.broadcasted_iota(jnp.int32, (ny, LANES), 1)

    def field(f, packed):
        for x in range(nx):
            packed = packed_ends(v_ref[f, x], f * nx + x, packed, lane)
        return packed

    z_ref[...] = lax.fori_loop(0, width, field, jnp.zeros((ny, LANES), F32))


def pick(odd, refs, load):
    first = load(refs[0]) if refs else 0.0
    second = load(refs[1]) if len(refs) > 1 else jnp.zeros_like(first)
    return jnp.where(odd, first, second), jnp.where(odd, second, first)


def apply_operator(v_ref, shift_ref, x_in, y_in, z_in, out_ref, packed=None):
    width, nx, ny, _ = v_ref.shape
    odd_x, odd_y, odd_z = parity("gx"), parity("gy"), parity("gz")
    lane = lax.broadcasted_iota(jnp.int32, (ny, LANES), 1)
    row = lax.broadcasted_iota(jnp.int32, (ny, LANES), 0)
    low_z, high_z = pick(odd_z, z_in, lambda ref: ref[...])
    ends = jnp.where(
        lax.rem(lane, 2) == 0, pltpu.roll(low_z, 1, 1), pltpu.roll(high_z, LANES - 1, 1)
    )

    def field(f, packed):
        low_x, high_x = pick(odd_x, x_in, lambda ref: ref[f])
        for x in range(nx):
            m = f * nx + x
            low_y, high_y = pick(odd_y, y_in, lambda ref: ref[f, x])
            v = v_ref[f, x]
            end = pltpu.roll(ends, lax.rem(LANES - 2 * m, LANES), 1)
            beside = (v_ref[f, x - 1] if x > 0 else low_x) + (v_ref[f, x + 1] if x < nx - 1 else high_x)
            beside += jnp.where(row == 0, low_y, pltpu.roll(v, 1, 0))
            beside += jnp.where(row == ny - 1, high_y, pltpu.roll(v, ny - 1, 0))
            beside += jnp.where(lane == 0, end, pltpu.roll(v, 1, 1))
            beside += jnp.where(lane == LANES - 1, end, pltpu.roll(v, LANES - 1, 1))
            out = ((6.0 - CENTRE) + shift_ref[x]) * v - beside
            out_ref[f, x] = out
            if packed is not None:
                packed = packed_ends(out, m, packed, lane)
        return packed

    if packed is None:
        lax.fori_loop(0, width, lambda f, c: (field(f, None), c)[1], 0)
        return None
    return lax.fori_loop(0, width, field, packed)


def operator_kernel(nx_r, ny_r, nz_r, *refs):
    v_ref, shift_ref = refs[:2]
    at = 2
    x_in, y_in, z_in = refs[at : at + nx_r], refs[at + nx_r : at + nx_r + ny_r], refs[at + nx_r + ny_r : at + nx_r + ny_r + nz_r]
    outs = refs[at + nx_r + ny_r + nz_r :]
    out_ref = outs[0]
    x_out, y_out, z_out = outs[1 : 1 + nx_r], outs[1 + nx_r : 1 + nx_r + ny_r], outs[1 + nx_r + ny_r]
    ny = v_ref.shape[2]
    z_out[...] = apply_operator(v_ref, shift_ref, x_in, y_in, z_in, out_ref, jnp.zeros((ny, LANES), F32))
    write_xy_faces(out_ref, x_out, y_out)


def add_moment(a_ref, b_ref, at, payload):
    width, nx, ny, _ = a_ref.shape
    pairs = [(i, j) for i in range(width) for j in range(i + 1)]

    def plane(x, sums):
        sums = list(sums)
        for y in range(0, ny, 8):
            a = [a_ref[f, x, y : y + 8, :] for f in range(width)]
            b = a if b_ref is a_ref else [b_ref[f, x, y : y + 8, :] for f in range(width)]
            for k, (i, j) in enumerate(pairs):
                sums[k] = sums[k] + a[i] * b[j]
        return tuple(sums)

    sums = lax.fori_loop(0, nx, plane, tuple(jnp.zeros((8, LANES), F32) for _ in pairs))
    rows = {}
    for (i, j), value in zip(pairs, sums):
        rows[i, j] = rows[j, i] = jnp.sum(value, axis=0, keepdims=True)
    lane = lax.broadcasted_iota(jnp.int32, (8, LANES), 1)
    for i in range(width):
        column = jnp.sum(jnp.concatenate([rows[i, j] for j in range(width)], axis=0), axis=1, keepdims=True)
        payload = jnp.where(lane == at + i, column, payload)
    return payload


def early_moments_kernel(b_ref, u_ref, out_ref):
    width = b_ref.shape[0]
    payload = add_moment(b_ref, b_ref, 0, jnp.zeros((8, LANES), F32))
    payload = add_moment(b_ref, u_ref, width, payload)
    out_ref[...] = add_moment(u_ref, u_ref, 2 * width, payload)


def late_moments_kernel(nx_r, ny_r, nz_r, *refs):
    u_ref, shift_ref = refs[:2]
    at = 2
    x_in, y_in, z_in = refs[at : at + nx_r], refs[at + nx_r : at + nx_r + ny_r], refs[at + nx_r + ny_r : at + nx_r + ny_r + nz_r]
    early_ref, out_ref, t_ref = refs[at + nx_r + ny_r + nz_r :]
    width = u_ref.shape[0]
    apply_operator(u_ref, shift_ref, x_in, y_in, z_in, t_ref)
    payload = add_moment(u_ref, t_ref, 3 * width, early_ref[...])
    payload = add_moment(t_ref, t_ref, 4 * width, payload)
    out_ref[...] = jnp.broadcast_to(payload[None], out_ref.shape)


def lanes_of(matrix, j):
    return jnp.broadcast_to(matrix[:, j : j + 1], matrix.shape)


def rows_of(matrix, i):
    return jnp.broadcast_to(matrix[i : i + 1, :], matrix.shape)


def times(left, at, right):
    count = left.shape[0]
    total = lanes_of(left, at) * rows_of(right, 0)
    for k in range(1, count):
        total = total + lanes_of(left, at + k) * rows_of(right, k)
    return total


def shift_lanes(matrix, by):
    return pltpu.roll(matrix, by % LANES, 1)


def eliminate(blocks):
    size = blocks[0].shape[0]
    sub = lax.broadcasted_iota(jnp.int32, blocks[0].shape, 0)
    for j in range(size * len(blocks)):
        own, local = divmod(j, size)
        columns = [lanes_of(block, j) for block in blocks]
        pivot = rows_of(blocks[own], local) / rows_of(columns[own], local)
        blocks = [block - column * pivot for block, column in zip(blocks, columns)]
        blocks[own] = jnp.where(sub == local, pivot, blocks[own])
    return blocks


def small_algebra(s):
    n = s.shape[0]
    c0 = CENTRE
    lane = lax.broadcasted_iota(jnp.int32, s.shape, 1)
    sub = lax.broadcasted_iota(jnp.int32, s.shape, 0)
    n0, n1, n2, n3, n4 = shift_lanes(s, n), s, shift_lanes(s, -n), shift_lanes(s, -2 * n), shift_lanes(s, -3 * n)
    (e,) = eliminate([s])
    p1 = times(s, n, e)
    p2 = times(s, 2 * n, e)
    p3 = times(s, 3 * n, e)
    cc = times(e, n, e)
    e2c = times(e, 2 * n, e)
    g = n2 - p1
    q = shift_lanes(e, -n) - cc
    n3c = n3 - p2
    f3 = n3c - times(s, n, q)
    f4 = n4 - p3 - times(s, n, shift_lanes(e, -2 * n) - e2c)
    m11 = n2 + 2.0 * c0 * n1 + c0 * c0 * n0
    m12 = n3c + 2.0 * c0 * g
    m21 = n3 - shift_lanes(p1, -n) + 2.0 * c0 * g
    m22 = f4 + 2.0 * c0 * f3 + c0 * c0 * g
    r1 = n1 + c0 * n0

    def assemble(first, second, third):
        joined = jnp.where(lane < n, shift_lanes(first, -n), second)
        return jnp.where(lane < 2 * n, joined, shift_lanes(third, n))

    pa, qa = eliminate([assemble(m11, m12, r1), assemble(m21, m22, g)])
    cq = times(e, n, qa)
    on_b = pa - cq
    unit = jnp.where(lane == sub + 2 * n, 1.0, 0.0)
    part = unit - times(e, n, pa) - c0 * pa - times(q, n, qa)
    squares = part * times(s, 0, part)
    pq = pa + c0 * qa
    squares = squares + pq * (times(g, n, pq) + 2.0 * times(f3, n, qa))
    squares = squares + qa * times(f4 - times(g, n, q), n, qa)
    return on_b, qa, jnp.sum(squares, axis=0, keepdims=True)


def finish_kernel(parts_ref, b_ref, u_ref, out_ref, norms_ref, coeff_ref):
    width, nx, ny, _ = b_ref.shape
    n = width
    total = jnp.sum(parts_ref[...], axis=0)
    on_b, on_u, squares = small_algebra(total)
    norms_ref[...] = jnp.sqrt(shift_lanes(squares, -2 * n))[:, :n]
    for f in range(width):
        coeff_ref[0, f] = lanes_of(on_b, 2 * n + f)
        coeff_ref[1, f] = lanes_of(on_u, 2 * n + f)
    group = 2

    def fields(k, carry):
        first = [[[rows_of(coeff_ref[h, group * k + d], g) for g in range(width)] for h in range(2)] for d in range(group)]

        def plane(x, carry):
            for y in range(0, ny, 8):
                b = [b_ref[g, x, y : y + 8, :] for g in range(width)]
                u = [u_ref[g, x, y : y + 8, :] for g in range(width)]
                for d in range(group):
                    total = first[d][0][0] * b[0] + first[d][1][0] * u[0]
                    for g in range(1, width):
                        total = total + (first[d][0][g] * b[g] + first[d][1][g] * u[g])
                    out_ref[group * k + d, x, y : y + 8, :] = total
            return carry

        return lax.fori_loop(0, nx, plane, carry)

    lax.fori_loop(0, width // group, fields, 0)


def call(kernel, out_shape, operands, scratch=(), flops=1_000_000, name=None):
    return pl.pallas_call(
        kernel,
        out_shape=out_shape,
        in_specs=[pl.BlockSpec(memory_space=pltpu.VMEM)] * len(operands),
        out_specs=jax.tree.map(lambda _: pl.BlockSpec(memory_space=pltpu.VMEM), out_shape),
        scratch_shapes=list(scratch),
        compiler_params=pltpu.CompilerParams(vmem_limit_bytes=8 << 20),
        cost_estimate=pl.CostEstimate(flops=flops, bytes_accessed=1 << 20, transcendentals=0),
        name=name,
    )(*operands)


def trade(x_faces, y_faces, ends):
    pairs_x, pairs_y, pairs_z = (swap_pairs(lax.axis_size(axis)) for axis in AXES)
    got_x = [lax.ppermute(face, "gx", pairs) for face, pairs in zip(x_faces, pairs_x)]
    got_z = [lax.ppermute(ends, "gz", pairs) for pairs in pairs_z]
    got_y = [lax.ppermute(face, "gy", pairs) for face, pairs in zip(y_faces, pairs_y)]
    return [*got_x, *got_y, *got_z]


def body(right_side, shift):
    width, nx, ny, nz = right_side.shape
    assert width == 8 and nz == LANES and ny % 8 == 0 and width * nx <= LANES // 2
    nx_r, ny_r, nz_r = rounds_of()
    devices = 1
    for axis in AXES:
        devices *= lax.axis_size(axis)
    block = jax.ShapeDtypeStruct(right_side.shape, F32)
    faces = [jax.ShapeDtypeStruct((width, ny, nz), F32)] * nx_r
    faces += [jax.ShapeDtypeStruct((width, nx, 1, nz), F32)] * ny_r
    faces += [jax.ShapeDtypeStruct((ny, LANES), F32)]

    packed = call(functools.partial(pack_kernel, nx_r, ny_r), faces, [right_side], name="pack")
    halo = trade(packed[:nx_r], packed[nx_r : nx_r + ny_r], packed[-1])
    u, *packed = call(
        functools.partial(operator_kernel, nx_r, ny_r, nz_r), [block, *faces], [right_side, shift, *halo], name="operator"
    )
    halo = trade(packed[:nx_r], packed[nx_r : nx_r + ny_r], packed[-1])
    early = call(
        early_moments_kernel, jax.ShapeDtypeStruct((8, LANES), F32), [right_side, u], flops=30_000_000, name="early"
    )
    copies = call(
        functools.partial(late_moments_kernel, nx_r, ny_r, nz_r),
        jax.ShapeDtypeStruct((devices, 8, LANES), F32),
        [u, shift, *halo, early],
        scratch=[pltpu.VMEM(right_side.shape, F32)],
        name="late",
    )
    parts = lax.all_to_all(copies, AXES, 0, 0, tiled=True)
    out, norms = call(
        finish_kernel,
        [block, jax.ShapeDtypeStruct((1, width), F32)],
        [parts, right_side, u],
        scratch=[pltpu.VMEM((2, width, 8, LANES), F32)],
        name="finish",
    )
    return out, norms.reshape(width)


def solution(mesh):
    in_specs = (P(None, "gx", "gy", "gz"), P("gx", "gy", "gz"))
    out_specs = (P(None, "gx", "gy", "gz"), P())
    return jax.shard_map(body, mesh=mesh, in_specs=in_specs, out_specs=out_specs, check_vma=False)
```

```python
import functools

import jax
import jax.numpy as jnp
from jax import lax
from jax.experimental import pallas as pl
from jax.experimental.pallas import tpu as pltpu
from jax.sharding import PartitionSpec as P

AXES = ("gx", "gy", "gz")
CENTRE = 7.0
LANES = 128
F32 = jnp.float32


def swap_pairs(count):
    first = [(i, j) for a in range(0, count - 1, 2) for i, j in ((a, a + 1), (a + 1, a))]
    second = [(i, j) for a in range(1, count - 1, 2) for i, j in ((a, a + 1), (a + 1, a))]
    return [pairs for pairs in (first, second) if pairs]


def swap(values, axis, pairs):
    side = lax.axis_size("gy")
    if axis == "gy" or side % 2:
        return lax.ppermute(values, axis, pairs)
    count = lax.axis_size(axis)
    named = {i for i, _ in pairs}
    at = (lambda i, y: i * side + y) if axis == "gx" else (lambda i, y: y * count + i)
    joint = [(at(i, y), at(j, y)) for i, j in pairs for y in range(side)]
    joint += [(at(i, y), at(i, y ^ 1)) for i in range(count) if i not in named for y in range(side)]
    return lax.ppermute(values, ("gx", "gy") if axis == "gx" else ("gy", "gz"), joint)


def rounds_of():
    return tuple(len(swap_pairs(lax.axis_size(axis))) for axis in AXES)


def parity(axis):
    return lax.rem(lax.axis_index(axis), 2) == 1


def write_xy_faces(v_ref, x_refs, y_refs):
    width, nx, ny, _ = v_ref.shape
    odd_x, odd_y = parity("gx"), parity("gy")
    for k, ref in enumerate(x_refs):
        high = jnp.logical_xor(odd_x, k == 0)
        ref[...] = v_ref[:, jnp.where(high, nx - 1, 0)]
    for k, ref in enumerate(y_refs):
        high = jnp.logical_xor(odd_y, k == 0)
        ref[...] = jnp.where(high, v_ref[:, :, ny - 1 : ny, :], v_ref[:, :, 0:1, :])


def packed_ends(tile, m, packed, lane):
    at = 2 * m
    hit = (lane == at) | (lane == lax.rem(at + LANES - 1, LANES))
    return jnp.where(hit, pltpu.roll(tile, at, 1), packed)


def pack_kernel(nx_r, ny_r, v_ref, *refs):
    width, nx, ny, _ = v_ref.shape
    x_refs, y_refs, z_ref = refs[:nx_r], refs[nx_r : nx_r + ny_r], refs[nx_r + ny_r]
    write_xy_faces(v_ref, x_refs, y_refs)
    lane = lax.broadcasted_iota(jnp.int32, (ny, LANES), 1)

    def field(f, packed):
        for x in range(nx):
            packed = packed_ends(v_ref[f, x], f * nx + x, packed, lane)
        return packed

    z_ref[...] = lax.fori_loop(0, width, field, jnp.zeros((ny, LANES), F32))


def pick(axis, refs, load):
    if not refs:
        return 0.0, 0.0
    odd, at = parity(axis), lax.axis_index(axis)
    first = load(refs[0])
    second = load(refs[1]) if len(refs) > 1 else jnp.zeros_like(first)
    low = jnp.where(at == 0, 0.0, jnp.where(odd, first, second))
    high = jnp.where(at == lax.axis_size(axis) - 1, 0.0, jnp.where(odd, second, first))
    return low, high


def apply_operator(v_ref, shift_ref, x_in, y_in, z_in, out_ref, packed=None):
    width, nx, ny, _ = v_ref.shape
    lane = lax.broadcasted_iota(jnp.int32, (ny, LANES), 1)
    row = lax.broadcasted_iota(jnp.int32, (ny, LANES), 0)
    low_z, high_z = pick("gz", z_in, lambda ref: ref[...])
    ends = jnp.where(
        lax.rem(lane, 2) == 0, pltpu.roll(low_z, 1, 1), pltpu.roll(high_z, LANES - 1, 1)
    )

    def field(f, packed):
        low_x, high_x = pick("gx", x_in, lambda ref: ref[f])
        for x in range(nx):
            m = f * nx + x
            low_y, high_y = pick("gy", y_in, lambda ref: ref[f, x])
            v = v_ref[f, x]
            end = pltpu.roll(ends, lax.rem(LANES - 2 * m, LANES), 1)
            beside = (v_ref[f, x - 1] if x > 0 else low_x) + (v_ref[f, x + 1] if x < nx - 1 else high_x)
            beside += jnp.where(row == 0, low_y, pltpu.roll(v, 1, 0))
            beside += jnp.where(row == ny - 1, high_y, pltpu.roll(v, ny - 1, 0))
            beside += jnp.where(lane == 0, end, pltpu.roll(v, 1, 1))
            beside += jnp.where(lane == LANES - 1, end, pltpu.roll(v, LANES - 1, 1))
            out = ((6.0 - CENTRE) + shift_ref[x]) * v - beside
            out_ref[f, x] = out
            if packed is not None:
                packed = packed_ends(out, m, packed, lane)
        return packed

    if packed is None:
        lax.fori_loop(0, width, lambda f, c: (field(f, None), c)[1], 0)
        return None
    return lax.fori_loop(0, width, field, packed)


def operator_kernel(nx_r, ny_r, nz_r, *refs):
    v_ref, shift_ref = refs[:2]
    at = 2
    x_in, y_in, z_in = refs[at : at + nx_r], refs[at + nx_r : at + nx_r + ny_r], refs[at + nx_r + ny_r : at + nx_r + ny_r + nz_r]
    outs = refs[at + nx_r + ny_r + nz_r :]
    out_ref = outs[0]
    x_out, y_out, z_out = outs[1 : 1 + nx_r], outs[1 + nx_r : 1 + nx_r + ny_r], outs[1 + nx_r + ny_r]
    ny = v_ref.shape[2]
    z_out[...] = apply_operator(v_ref, shift_ref, x_in, y_in, z_in, out_ref, jnp.zeros((ny, LANES), F32))
    write_xy_faces(out_ref, x_out, y_out)


def add_moment(a_ref, b_ref, at, payload):
    width, nx, ny, _ = a_ref.shape
    pairs = [(i, j) for i in range(width) for j in range(i + 1)]

    def plane(x, sums):
        sums = list(sums)
        for y in range(0, ny, 8):
            a = [a_ref[f, x, y : y + 8, :] for f in range(width)]
            b = a if b_ref is a_ref else [b_ref[f, x, y : y + 8, :] for f in range(width)]
            for k, (i, j) in enumerate(pairs):
                sums[k] = sums[k] + a[i] * b[j]
        return tuple(sums)

    sums = lax.fori_loop(0, nx, plane, tuple(jnp.zeros((8, LANES), F32) for _ in pairs))
    rows = {}
    for (i, j), value in zip(pairs, sums):
        rows[i, j] = rows[j, i] = jnp.sum(value, axis=0, keepdims=True)
    lane = lax.broadcasted_iota(jnp.int32, (8, LANES), 1)
    for i in range(width):
        column = jnp.sum(jnp.concatenate([rows[i, j] for j in range(width)], axis=0), axis=1, keepdims=True)
        payload = jnp.where(lane == at + i, column, payload)
    return payload


def early_moments_kernel(b_ref, u_ref, out_ref):
    width = b_ref.shape[0]
    payload = add_moment(b_ref, b_ref, 0, jnp.zeros((8, LANES), F32))
    payload = add_moment(b_ref, u_ref, width, payload)
    out_ref[...] = add_moment(u_ref, u_ref, 2 * width, payload)


def late_moments_kernel(nx_r, ny_r, nz_r, *refs):
    u_ref, shift_ref = refs[:2]
    at = 2
    x_in, y_in, z_in = refs[at : at + nx_r], refs[at + nx_r : at + nx_r + ny_r], refs[at + nx_r + ny_r : at + nx_r + ny_r + nz_r]
    early_ref, out_ref, t_ref = refs[at + nx_r + ny_r + nz_r :]
    width = u_ref.shape[0]
    apply_operator(u_ref, shift_ref, x_in, y_in, z_in, t_ref)
    payload = add_moment(u_ref, t_ref, 3 * width, early_ref[...])
    payload = add_moment(t_ref, t_ref, 4 * width, payload)
    out_ref[...] = jnp.broadcast_to(payload[None], out_ref.shape)


def lanes_of(matrix, j):
    return jnp.broadcast_to(matrix[:, j : j + 1], matrix.shape)


def rows_of(matrix, i):
    return jnp.broadcast_to(matrix[i : i + 1, :], matrix.shape)


def times(left, at, right):
    count = left.shape[0]
    total = lanes_of(left, at) * rows_of(right, 0)
    for k in range(1, count):
        total = total + lanes_of(left, at + k) * rows_of(right, k)
    return total


def shift_lanes(matrix, by):
    return pltpu.roll(matrix, by % LANES, 1)


def eliminate(blocks):
    size = blocks[0].shape[0]
    sub = lax.broadcasted_iota(jnp.int32, blocks[0].shape, 0)
    for j in range(size * len(blocks)):
        own, local = divmod(j, size)
        columns = [lanes_of(block, j) for block in blocks]
        pivot = rows_of(blocks[own], local) / rows_of(columns[own], local)
        blocks = [block - column * pivot for block, column in zip(blocks, columns)]
        blocks[own] = jnp.where(sub == local, pivot, blocks[own])
    return blocks


def small_algebra(s):
    n = s.shape[0]
    c0 = CENTRE
    lane = lax.broadcasted_iota(jnp.int32, s.shape, 1)
    sub = lax.broadcasted_iota(jnp.int32, s.shape, 0)
    n0, n1, n2, n3, n4 = shift_lanes(s, n), s, shift_lanes(s, -n), shift_lanes(s, -2 * n), shift_lanes(s, -3 * n)
    (e,) = eliminate([s])
    p1 = times(s, n, e)
    p2 = times(s, 2 * n, e)
    p3 = times(s, 3 * n, e)
    cc = times(e, n, e)
    e2c = times(e, 2 * n, e)
    g = n2 - p1
    q = shift_lanes(e, -n) - cc
    n3c = n3 - p2
    f3 = n3c - times(s, n, q)
    f4 = n4 - p3 - times(s, n, shift_lanes(e, -2 * n) - e2c)
    m11 = n2 + 2.0 * c0 * n1 + c0 * c0 * n0
    m12 = n3c + 2.0 * c0 * g
    m21 = n3 - shift_lanes(p1, -n) + 2.0 * c0 * g
    m22 = f4 + 2.0 * c0 * f3 + c0 * c0 * g
    r1 = n1 + c0 * n0

    def assemble(first, second, third):
        joined = jnp.where(lane < n, shift_lanes(first, -n), second)
        return jnp.where(lane < 2 * n, joined, shift_lanes(third, n))

    pa, qa = eliminate([assemble(m11, m12, r1), assemble(m21, m22, g)])
    cq = times(e, n, qa)
    on_b = pa - cq
    unit = jnp.where(lane == sub + 2 * n, 1.0, 0.0)
    part = unit - times(e, n, pa) - c0 * pa - times(q, n, qa)
    squares = part * times(s, 0, part)
    pq = pa + c0 * qa
    squares = squares + pq * (times(g, n, pq) + 2.0 * times(f3, n, qa))
    squares = squares + qa * times(f4 - times(g, n, q), n, qa)
    return on_b, qa, jnp.sum(squares, axis=0, keepdims=True)


def finish_kernel(parts_ref, b_ref, u_ref, out_ref, norms_ref, coeff_ref):
    width, nx, ny, _ = b_ref.shape
    n = width
    total = jnp.sum(parts_ref[...], axis=0)
    on_b, on_u, squares = small_algebra(total)
    norms_ref[...] = jnp.sqrt(shift_lanes(squares, -2 * n))[:, :n]
    for f in range(width):
        coeff_ref[0, f] = lanes_of(on_b, 2 * n + f)
        coeff_ref[1, f] = lanes_of(on_u, 2 * n + f)
    group = 2

    def fields(k, carry):
        first = [[[rows_of(coeff_ref[h, group * k + d], g) for g in range(width)] for h in range(2)] for d in range(group)]

        def plane(x, carry):
            for y in range(0, ny, 8):
                b = [b_ref[g, x, y : y + 8, :] for g in range(width)]
                u = [u_ref[g, x, y : y + 8, :] for g in range(width)]
                for d in range(group):
                    total = first[d][0][0] * b[0] + first[d][1][0] * u[0]
                    for g in range(1, width):
                        total = total + (first[d][0][g] * b[g] + first[d][1][g] * u[g])
                    out_ref[group * k + d, x, y : y + 8, :] = total
            return carry

        return lax.fori_loop(0, nx, plane, carry)

    lax.fori_loop(0, width // group, fields, 0)


def call(kernel, out_shape, operands, scratch=(), flops=1_000_000, name=None):
    return pl.pallas_call(
        kernel,
        out_shape=out_shape,
        in_specs=[pl.BlockSpec(memory_space=pltpu.VMEM)] * len(operands),
        out_specs=jax.tree.map(lambda _: pl.BlockSpec(memory_space=pltpu.VMEM), out_shape),
        scratch_shapes=list(scratch),
        compiler_params=pltpu.CompilerParams(vmem_limit_bytes=8 << 20),
        cost_estimate=pl.CostEstimate(flops=flops, bytes_accessed=1 << 20, transcendentals=0),
        name=name,
    )(*operands)


def trade(x_faces, y_faces, ends):
    pairs_x, pairs_y, pairs_z = (swap_pairs(lax.axis_size(axis)) for axis in AXES)
    got_x = [swap(face, "gx", pairs) for face, pairs in zip(x_faces, pairs_x)]
    got_z = [swap(ends, "gz", pairs) for pairs in pairs_z]
    got_y = [swap(face, "gy", pairs) for face, pairs in zip(y_faces, pairs_y)]
    return [*got_x, *got_y, *got_z]


def body(right_side, shift):
    width, nx, ny, nz = right_side.shape
    assert width == 8 and nz == LANES and ny % 8 == 0 and width * nx <= LANES // 2
    nx_r, ny_r, nz_r = rounds_of()
    devices = 1
    for axis in AXES:
        devices *= lax.axis_size(axis)
    block = jax.ShapeDtypeStruct(right_side.shape, F32)
    faces = [jax.ShapeDtypeStruct((width, ny, nz), F32)] * nx_r
    faces += [jax.ShapeDtypeStruct((width, nx, 1, nz), F32)] * ny_r
    faces += [jax.ShapeDtypeStruct((ny, LANES), F32)]

    packed = call(functools.partial(pack_kernel, nx_r, ny_r), faces, [right_side], name="pack")
    halo = trade(packed[:nx_r], packed[nx_r : nx_r + ny_r], packed[-1])
    u, *packed = call(
        functools.partial(operator_kernel, nx_r, ny_r, nz_r), [block, *faces], [right_side, shift, *halo], name="operator"
    )
    halo = trade(packed[:nx_r], packed[nx_r : nx_r + ny_r], packed[-1])
    early = call(
        early_moments_kernel, jax.ShapeDtypeStruct((8, LANES), F32), [right_side, u], flops=30_000_000, name="early"
    )
    copies = call(
        functools.partial(late_moments_kernel, nx_r, ny_r, nz_r),
        jax.ShapeDtypeStruct((devices, 8, LANES), F32),
        [u, shift, *halo, early],
        scratch=[pltpu.VMEM(right_side.shape, F32)],
        name="late",
    )
    parts = lax.all_to_all(copies, AXES, 0, 0, tiled=True)
    out, norms = call(
        finish_kernel,
        [block, jax.ShapeDtypeStruct((1, width), F32)],
        [parts, right_side, u],
        scratch=[pltpu.VMEM((2, width, 8, LANES), F32)],
        name="finish",
    )
    return out, norms.reshape(width)


def solution(mesh):
    in_specs = (P(None, "gx", "gy", "gz"), P("gx", "gy", "gz"))
    out_specs = (P(None, "gx", "gy", "gz"), P())
    return jax.shard_map(body, mesh=mesh, in_specs=in_specs, out_specs=out_specs, check_vma=False)
```

```python
import functools

import jax
import jax.numpy as jnp
from jax import lax
from jax.experimental import pallas as pl
from jax.experimental.pallas import tpu as pltpu
from jax.sharding import PartitionSpec as P

AXES = ("gx", "gy", "gz")
CENTRE = 7.0
LANES = 128
F32 = jnp.float32


def swap_pairs(count):
    first = [(i, j) for a in range(0, count - 1, 2) for i, j in ((a, a + 1), (a + 1, a))]
    second = [(i, j) for a in range(1, count - 1, 2) for i, j in ((a, a + 1), (a + 1, a))]
    return [pairs for pairs in (first, second) if pairs]


def swap(values, axis, pairs):
    side = lax.axis_size("gy")
    if axis == "gy" or side % 2:
        return lax.ppermute(values, axis, pairs)
    count = lax.axis_size(axis)
    named = {i for i, _ in pairs}
    at = (lambda i, y: i * side + y) if axis == "gx" else (lambda i, y: y * count + i)
    joint = [(at(i, y), at(j, y)) for i, j in pairs for y in range(side)]
    joint += [(at(i, y), at(i, y ^ 1)) for i in range(count) if i not in named for y in range(side)]
    return lax.ppermute(values, ("gx", "gy") if axis == "gx" else ("gy", "gz"), joint)


def rounds_of():
    return tuple(len(swap_pairs(lax.axis_size(axis))) for axis in AXES)


def parity(axis):
    return lax.rem(lax.axis_index(axis), 2) == 1


def x_plane(k, nx):
    return jnp.where(jnp.logical_xor(parity("gx"), k == 0), nx - 1, 0)


def cut_x_kernel(v_ref, *refs):
    faces, sems = refs[:-1], refs[-1]
    copies = [
        pltpu.make_async_copy(v_ref.at[:, x_plane(k, v_ref.shape[1])], ref, sems.at[k]) for k, ref in enumerate(faces)
    ]
    for copy in copies:
        copy.start()
    for copy in copies:
        copy.wait()


def write_y_faces(v_ref, y_refs):
    ny = v_ref.shape[2]
    odd = parity("gy")
    for k, ref in enumerate(y_refs):
        high = jnp.logical_xor(odd, k == 0)
        ref[...] = jnp.where(high, v_ref[:, :, ny - 1 : ny, :], v_ref[:, :, 0:1, :])


def packed_ends(tile, m, packed, lane):
    at = 2 * m
    hit = (lane == at) | (lane == lax.rem(at + LANES - 1, LANES))
    return jnp.where(hit, pltpu.roll(tile, at, 1), packed)


def pack_kernel(v_ref, *refs):
    width, nx, ny, _ = v_ref.shape
    write_y_faces(v_ref, refs[:-1])
    lane = lax.broadcasted_iota(jnp.int32, (ny, LANES), 1)

    def field(f, packed):
        for x in range(nx):
            packed = packed_ends(v_ref[f, x], f * nx + x, packed, lane)
        return packed

    refs[-1][...] = lax.fori_loop(0, width, field, jnp.zeros((ny, LANES), F32))


def pick(axis, refs, load):
    if not refs:
        return 0.0, 0.0
    odd, at = parity(axis), lax.axis_index(axis)
    first = load(refs[0])
    second = load(refs[1]) if len(refs) > 1 else jnp.zeros_like(first)
    low = jnp.where(at == 0, 0.0, jnp.where(odd, first, second))
    high = jnp.where(at == lax.axis_size(axis) - 1, 0.0, jnp.where(odd, second, first))
    return low, high


def apply_operator(planes, v_ref, shift_ref, x_in, y_in, z_in, out_ref, packed=None):
    width, nx, ny, _ = v_ref.shape
    lane = lax.broadcasted_iota(jnp.int32, (ny, LANES), 1)
    row = lax.broadcasted_iota(jnp.int32, (ny, LANES), 0)
    low_z, high_z = pick("gz", z_in, lambda ref: ref[...])
    ends = jnp.where(
        lax.rem(lane, 2) == 0, pltpu.roll(low_z, 1, 1), pltpu.roll(high_z, LANES - 1, 1)
    )

    def field(f, packed):
        low_x, high_x = pick("gx", x_in, lambda ref: ref[f])
        for x in planes:
            m = f * nx + x
            low_y, high_y = pick("gy", y_in, lambda ref: ref[f, x])
            v = v_ref[f, x]
            end = pltpu.roll(ends, lax.rem(LANES - 2 * m, LANES), 1)
            beside = (v_ref[f, x - 1] if x > 0 else low_x) + (v_ref[f, x + 1] if x < nx - 1 else high_x)
            beside += jnp.where(row == 0, low_y, pltpu.roll(v, 1, 0))
            beside += jnp.where(row == ny - 1, high_y, pltpu.roll(v, ny - 1, 0))
            beside += jnp.where(lane == 0, end, pltpu.roll(v, 1, 1))
            beside += jnp.where(lane == LANES - 1, end, pltpu.roll(v, LANES - 1, 1))
            out = ((6.0 - CENTRE) + shift_ref[x]) * v - beside
            out_ref[f, x] = out
            if packed is not None:
                packed = packed_ends(out, m, packed, lane)
        return packed

    if packed is None:
        lax.fori_loop(0, width, lambda f, c: (field(f, None), c)[1], 0)
        return None
    return lax.fori_loop(0, width, field, packed)


def split(refs, *counts):
    parts, at = [], 0
    for count in counts:
        parts.append(refs[at : at + count])
        at += count
    return (*parts, refs[at:])


def inner_planes(ref):
    return range(1, ref.shape[1] - 1)


def outer_planes(ref):
    return (0, ref.shape[1] - 1)


def inner_operator_kernel(ny_r, nz_r, v_ref, shift_ref, *refs):
    y_in, z_in, (out_ref, ends_ref) = split(refs, ny_r, nz_r)
    start = jnp.zeros(ends_ref.shape, F32)
    ends_ref[...] = apply_operator(inner_planes(v_ref), v_ref, shift_ref, (), y_in, z_in, out_ref, start)


def outer_operator_kernel(nx_r, ny_r, nz_r, v_ref, shift_ref, inner_ref, ends_ref, *refs):
    x_in, y_in, z_in, (out_ref,), x_out, y_out, (z_out,) = split(refs, nx_r, ny_r, nz_r, 1, nx_r, ny_r)
    planes = outer_planes(v_ref)
    z_out[...] = apply_operator(planes, v_ref, shift_ref, x_in, y_in, z_in, out_ref, ends_ref[...])
    for k, ref in enumerate(x_out):
        ref[...] = out_ref[:, x_plane(k, v_ref.shape[1])]
    write_y_faces(out_ref, y_out)


def pairs_of(width):
    return [(i, j) for i in range(width) for j in range(i + 1)]


def moment_sums(first, last, step, a_ref, b_ref, sums):
    width, _, ny, _ = a_ref.shape
    pairs = pairs_of(width)

    def plane(k, sums):
        sums, x = list(sums), first + k * step
        for y in range(0, ny, 8):
            a = [a_ref[f, x, y : y + 8, :] for f in range(width)]
            b = a if b_ref is a_ref else [b_ref[f, x, y : y + 8, :] for f in range(width)]
            for k, (i, j) in enumerate(pairs):
                sums[k] = sums[k] + a[i] * b[j]
        return tuple(sums)

    return lax.fori_loop(0, -((first - last) // step), plane, tuple(sums))


def no_sums(width):
    return [jnp.zeros((8, LANES), F32) for _ in pairs_of(width)]


def put_moment(width, sums, at, payload):
    rows = {}
    for (i, j), value in zip(pairs_of(width), sums):
        rows[i, j] = rows[j, i] = jnp.sum(value, axis=0, keepdims=True)
    lane = lax.broadcasted_iota(jnp.int32, (8, LANES), 1)
    for i in range(width):
        column = jnp.sum(jnp.concatenate([rows[i, j] for j in range(width)], axis=0), axis=1, keepdims=True)
        payload = jnp.where(lane == at + i, column, payload)
    return payload


def early_moments_kernel(b_ref, u_ref, out_ref):
    width, nx = b_ref.shape[:2]
    payload = jnp.zeros((8, LANES), F32)
    for k, (left, right) in enumerate(((b_ref, b_ref), (b_ref, u_ref), (u_ref, u_ref))):
        payload = put_moment(width, moment_sums(0, nx, 1, left, right, no_sums(width)), k * width, payload)
    out_ref[...] = payload


def inner_late_kernel(ny_r, nz_r, u_ref, shift_ref, *refs):
    y_in, z_in, (sums_ref, t_ref) = split(refs, ny_r, nz_r)
    width, nx = u_ref.shape[:2]
    apply_operator(inner_planes(u_ref), u_ref, shift_ref, (), y_in, z_in, t_ref)
    for h, left in enumerate((u_ref, t_ref)):
        for k, value in enumerate(moment_sums(1, nx - 1, 1, left, t_ref, no_sums(width))):
            sums_ref[h, k] = value


def outer_late_kernel(nx_r, ny_r, nz_r, u_ref, shift_ref, sums_ref, early_ref, *refs):
    x_in, y_in, z_in, (out_ref, t_ref) = split(refs, nx_r, ny_r, nz_r)
    width, nx = u_ref.shape[:2]
    apply_operator(outer_planes(u_ref), u_ref, shift_ref, x_in, y_in, z_in, t_ref)
    payload = early_ref[...]
    for h, left in enumerate((u_ref, t_ref)):
        inner = [sums_ref[h, k] for k in range(len(pairs_of(width)))]
        payload = put_moment(width, moment_sums(0, nx, nx - 1, left, t_ref, inner), (3 + h) * width, payload)
    out_ref[...] = jnp.broadcast_to(payload[None], out_ref.shape)


def lanes_of(matrix, j):
    return jnp.broadcast_to(matrix[:, j : j + 1], matrix.shape)


def rows_of(matrix, i):
    return jnp.broadcast_to(matrix[i : i + 1, :], matrix.shape)


def times(left, at, right):
    count = left.shape[0]
    total = lanes_of(left, at) * rows_of(right, 0)
    for k in range(1, count):
        total = total + lanes_of(left, at + k) * rows_of(right, k)
    return total


def shift_lanes(matrix, by):
    return pltpu.roll(matrix, by % LANES, 1)


def eliminate(blocks):
    size = blocks[0].shape[0]
    sub = lax.broadcasted_iota(jnp.int32, blocks[0].shape, 0)
    for j in range(size * len(blocks)):
        own, local = divmod(j, size)
        columns = [lanes_of(block, j) for block in blocks]
        pivot = rows_of(blocks[own], local) / rows_of(columns[own], local)
        blocks = [block - column * pivot for block, column in zip(blocks, columns)]
        blocks[own] = jnp.where(sub == local, pivot, blocks[own])
    return blocks


def small_algebra(s):
    n = s.shape[0]
    c0 = CENTRE
    lane = lax.broadcasted_iota(jnp.int32, s.shape, 1)
    sub = lax.broadcasted_iota(jnp.int32, s.shape, 0)
    n0, n1, n2, n3, n4 = shift_lanes(s, n), s, shift_lanes(s, -n), shift_lanes(s, -2 * n), shift_lanes(s, -3 * n)
    (e,) = eliminate([s])
    p1 = times(s, n, e)
    p2 = times(s, 2 * n, e)
    p3 = times(s, 3 * n, e)
    cc = times(e, n, e)
    e2c = times(e, 2 * n, e)
    g = n2 - p1
    q = shift_lanes(e, -n) - cc
    n3c = n3 - p2
    f3 = n3c - times(s, n, q)
    f4 = n4 - p3 - times(s, n, shift_lanes(e, -2 * n) - e2c)
    m11 = n2 + 2.0 * c0 * n1 + c0 * c0 * n0
    m12 = n3c + 2.0 * c0 * g
    m21 = n3 - shift_lanes(p1, -n) + 2.0 * c0 * g
    m22 = f4 + 2.0 * c0 * f3 + c0 * c0 * g
    r1 = n1 + c0 * n0

    def assemble(first, second, third):
        joined = jnp.where(lane < n, shift_lanes(first, -n), second)
        return jnp.where(lane < 2 * n, joined, shift_lanes(third, n))

    pa, qa = eliminate([assemble(m11, m12, r1), assemble(m21, m22, g)])
    cq = times(e, n, qa)
    on_b = pa - cq
    unit = jnp.where(lane == sub + 2 * n, 1.0, 0.0)
    part = unit - times(e, n, pa) - c0 * pa - times(q, n, qa)
    squares = part * times(s, 0, part)
    pq = pa + c0 * qa
    squares = squares + pq * (times(g, n, pq) + 2.0 * times(f3, n, qa))
    squares = squares + qa * times(f4 - times(g, n, q), n, qa)
    return on_b, qa, jnp.sum(squares, axis=0, keepdims=True)


def finish_kernel(parts_ref, b_ref, u_ref, out_ref, norms_ref, coeff_ref):
    width, nx, ny, _ = b_ref.shape
    n = width
    total = jnp.sum(parts_ref[...], axis=0)
    on_b, on_u, squares = small_algebra(total)
    norms_ref[...] = jnp.sqrt(shift_lanes(squares, -2 * n))[:, :n]
    for f in range(width):
        coeff_ref[0, f] = lanes_of(on_b, 2 * n + f)
        coeff_ref[1, f] = lanes_of(on_u, 2 * n + f)
    group = 2

    def fields(k, carry):
        first = [[[rows_of(coeff_ref[h, group * k + d], g) for g in range(width)] for h in range(2)] for d in range(group)]

        def plane(x, carry):
            for y in range(0, ny, 8):
                b = [b_ref[g, x, y : y + 8, :] for g in range(width)]
                u = [u_ref[g, x, y : y + 8, :] for g in range(width)]
                for d in range(group):
                    total = first[d][0][0] * b[0] + first[d][1][0] * u[0]
                    for g in range(1, width):
                        total = total + (first[d][0][g] * b[g] + first[d][1][g] * u[g])
                    out_ref[group * k + d, x, y : y + 8, :] = total
            return carry

        return lax.fori_loop(0, nx, plane, carry)

    lax.fori_loop(0, width // group, fields, 0)


def call(kernel, out_shape, operands, scratch=(), flops=1_000_000, name=None, aliases=None, far=False):
    return pl.pallas_call(
        kernel,
        out_shape=out_shape,
        in_specs=[pl.BlockSpec(memory_space=pl.ANY if far else pltpu.VMEM)] * len(operands),
        out_specs=jax.tree.map(lambda _: pl.BlockSpec(memory_space=pltpu.VMEM), out_shape),
        scratch_shapes=list(scratch),
        input_output_aliases=aliases or {},
        compiler_params=pltpu.CompilerParams(vmem_limit_bytes=8 << 20),
        cost_estimate=pl.CostEstimate(flops=flops, bytes_accessed=1 << 20, transcendentals=0),
        name=name,
    )(*operands)


def trade(turn, axis, faces):
    out = []
    for k, (face, pairs) in enumerate(zip(faces, swap_pairs(lax.axis_size(axis)))):
        with jax.named_scope(f"turn{turn}_{axis}_{k}"):
            out.append(swap(face, axis, pairs))
    return out


def body(right_side, shift):
    width, nx, ny, nz = right_side.shape
    assert width == 8 and nz == LANES and ny % 8 == 0 and nx > 2 and width * nx <= LANES // 2
    nx_r, ny_r, nz_r = rounds_of()
    devices = 1
    for axis in AXES:
        devices *= lax.axis_size(axis)
    block = jax.ShapeDtypeStruct(right_side.shape, F32)
    x_faces = [jax.ShapeDtypeStruct((width, ny, nz), F32)] * nx_r
    y_faces = [jax.ShapeDtypeStruct((width, nx, 1, nz), F32)] * ny_r
    ends_of = jax.ShapeDtypeStruct((ny, LANES), F32)
    full = pltpu.VMEM(right_side.shape, F32)
    kernel = functools.partial

    faces = call(cut_x_kernel, x_faces, [right_side], scratch=[pltpu.SemaphoreType.DMA((max(nx_r, 1),))], name="cut", far=True)
    halo_x = trade(1, "gx", faces)
    *faces, ends = call(pack_kernel, [*y_faces, ends_of], [right_side], name="pack")
    halo = [*trade(1, "gy", faces), *trade(1, "gz", [ends] * nz_r)]
    inner, ends = call(
        kernel(inner_operator_kernel, ny_r, nz_r), [block, ends_of], [right_side, shift, *halo], flops=20_000_000, name="inner1"
    )
    u, *faces = call(
        kernel(outer_operator_kernel, nx_r, ny_r, nz_r),
        [block, *x_faces, *y_faces, ends_of],
        [right_side, shift, inner, ends, *halo_x, *halo],
        aliases={2: 0},
        name="outer1",
    )
    halo_x = trade(2, "gx", faces[:nx_r])
    halo = [*trade(2, "gy", faces[nx_r:-1]), *trade(2, "gz", faces[-1:] * nz_r)]
    early = call(early_moments_kernel, jax.ShapeDtypeStruct((8, LANES), F32), [right_side, u], flops=15_000_000, name="early")
    sums = call(
        kernel(inner_late_kernel, ny_r, nz_r),
        jax.ShapeDtypeStruct((2, len(pairs_of(width)), 8, LANES), F32),
        [u, shift, *halo],
        scratch=[full],
        flops=15_000_000,
        name="inner2",
    )
    copies = call(
        kernel(outer_late_kernel, nx_r, ny_r, nz_r),
        jax.ShapeDtypeStruct((devices, 8, LANES), F32),
        [u, shift, sums, early, *halo_x, *halo],
        scratch=[full],
        name="outer2",
    )
    parts = lax.all_to_all(copies, AXES, 0, 0, tiled=True)
    out, norms = call(
        finish_kernel,
        [block, jax.ShapeDtypeStruct((1, width), F32)],
        [parts, right_side, u],
        scratch=[pltpu.VMEM((2, width, 8, LANES), F32)],
        name="finish",
    )
    return out, norms.reshape(width)


def solution(mesh):
    in_specs = (P(None, "gx", "gy", "gz"), P("gx", "gy", "gz"))
    out_specs = (P(None, "gx", "gy", "gz"), P())
    return jax.shard_map(body, mesh=mesh, in_specs=in_specs, out_specs=out_specs, check_vma=False)
```

```python
import functools

import jax
import jax.numpy as jnp
from jax import lax
from jax.experimental import pallas as pl
from jax.experimental.pallas import tpu as pltpu
from jax.sharding import PartitionSpec as P

AXES = ("gx", "gy", "gz")
CENTRE = 7.0
LANES = 128
F32 = jnp.float32


def swap_pairs(count):
    first = [(i, j) for a in range(0, count - 1, 2) for i, j in ((a, a + 1), (a + 1, a))]
    second = [(i, j) for a in range(1, count - 1, 2) for i, j in ((a, a + 1), (a + 1, a))]
    return [pairs for pairs in (first, second) if pairs]


def swap(values, axis, pairs):
    side = lax.axis_size("gy")
    if axis == "gy" or side % 2:
        return lax.ppermute(values, axis, pairs)
    count = lax.axis_size(axis)
    named = {i for i, _ in pairs}
    at = (lambda i, y: i * side + y) if axis == "gx" else (lambda i, y: y * count + i)
    joint = [(at(i, y), at(j, y)) for i, j in pairs for y in range(side)]
    joint += [(at(i, y), at(i, y ^ 1)) for i in range(count) if i not in named for y in range(side)]
    return lax.ppermute(values, ("gx", "gy") if axis == "gx" else ("gy", "gz"), joint)


def rounds_of():
    return tuple(len(swap_pairs(lax.axis_size(axis))) for axis in AXES)


def parity(axis):
    return lax.rem(lax.axis_index(axis), 2) == 1


def x_plane(k, nx):
    return jnp.where(jnp.logical_xor(parity("gx"), k == 0), nx - 1, 0)


def cut_x_kernel(v_ref, *refs):
    faces, sems = refs[:-1], refs[-1]
    copies = [
        pltpu.make_async_copy(v_ref.at[:, x_plane(k, v_ref.shape[1])], ref, sems.at[k]) for k, ref in enumerate(faces)
    ]
    for copy in copies:
        copy.start()
    for copy in copies:
        copy.wait()


def write_y_faces(v_ref, y_refs):
    ny = v_ref.shape[2]
    odd = parity("gy")
    for k, ref in enumerate(y_refs):
        high = jnp.logical_xor(odd, k == 0)
        ref[...] = jnp.where(high, v_ref[:, :, ny - 1 : ny, :], v_ref[:, :, 0:1, :])


def packed_ends(tile, m, lane, near, far=None):
    def at(offset):
        return lane == lax.rem(2 * m + offset + LANES, LANES)

    turned = pltpu.roll(tile, 2 * m, 1)
    near = jnp.where(at(0) | at(-1), turned, near)
    if far is None:
        return near
    return near, jnp.where(at(1) | at(-2), turned, far)


def pack_kernel(v_ref, shift_ref, *refs):
    width, nx, ny, _ = v_ref.shape
    write_y_faces(v_ref, refs[:-1])
    lane = lax.broadcasted_iota(jnp.int32, (ny, LANES), 1)
    nothing = jnp.zeros((ny, LANES), F32)

    def field(f, packed):
        for x in range(nx):
            packed = packed_ends(v_ref[f, x], f * nx + x, lane, *packed)
        return packed

    near, far = lax.fori_loop(0, width, field, (nothing, nothing))
    diagonal = nothing
    for x in range(nx):
        diagonal = packed_ends((6.0 - CENTRE) + shift_ref[x], x, lane, diagonal)
    copies = 1
    while copies < width:
        diagonal = diagonal + pltpu.roll(diagonal, 2 * nx * copies, 1)
        copies *= 2
    refs[-1][0] = near
    refs[-1][1] = far
    refs[-1][2] = diagonal


def pick(axis, refs, load):
    if not refs:
        return 0.0, 0.0
    odd, at = parity(axis), lax.axis_index(axis)
    first = load(refs[0])
    second = load(refs[1]) if len(refs) > 1 else jnp.zeros_like(first)
    low = jnp.where(at == 0, 0.0, jnp.where(odd, first, second))
    high = jnp.where(at == lax.axis_size(axis) - 1, 0.0, jnp.where(odd, second, first))
    return low, high


def halo_ends(z_in, layer):
    low, high = pick("gz", z_in, lambda ref: ref[layer])
    if not z_in:
        return None
    lane = lax.broadcasted_iota(jnp.int32, low.shape, 1)
    by = 2 if layer == 1 else 1
    return jnp.where(lax.rem(lane, 2) == 0, pltpu.roll(low, by, 1), pltpu.roll(high, LANES - by, 1))


def inside_grid(lane):
    low = jnp.where(lax.axis_index("gz") == 0, 0.0, 1.0)
    high = jnp.where(lax.axis_index("gz") == lax.axis_size("gz") - 1, 0.0, 1.0)
    return jnp.where(lax.rem(lane, 2) == 0, low, high)


def lane_x(lane, nx):
    return lax.rem((lane + 1) // 2, nx)


def operator_on_ends(nx, own, z_in):
    near, far, diagonal = (halo_ends(z_in, layer) for layer in range(3))
    ny = near.shape[0]
    lane = lax.broadcasted_iota(jnp.int32, near.shape, 1)
    row = lax.broadcasted_iota(jnp.int32, near.shape, 0)
    x = lane_x(lane, nx)
    beside = own + far
    beside += jnp.where(x == 0, 0.0, pltpu.roll(near, 2, 1)) + jnp.where(x == nx - 1, 0.0, pltpu.roll(near, LANES - 2, 1))
    beside += jnp.where(row == 0, 0.0, pltpu.roll(near, 1, 0)) + jnp.where(row == ny - 1, 0.0, pltpu.roll(near, ny - 1, 0))
    return near, inside_grid(lane) * (diagonal * near - beside)


def finished_ends(nx, base, x_in, y_in, width):
    ny = base.shape[0]
    lane = lax.broadcasted_iota(jnp.int32, base.shape, 1)
    row = lax.broadcasted_iota(jnp.int32, base.shape, 0)
    low_y, high_y = pick("gy", y_in, lambda ref: ref[width, 0])
    beside = jnp.where(row == 0, low_y, 0.0) + jnp.where(row == ny - 1, high_y, 0.0)
    if x_in:
        x, by = lane_x(lane, nx), 2 * (nx - 1)
        low_x, high_x = pick("gx", x_in, lambda ref: ref[width])
        beside += jnp.where(x == 0, pltpu.roll(low_x, LANES - by, 1), 0.0)
        beside += jnp.where(x == nx - 1, pltpu.roll(high_x, by, 1), 0.0)
    return base - inside_grid(lane) * beside


def apply_operator(planes, v_ref, shift_ref, x_in, y_in, ends, out_ref):
    width, nx, ny, _ = v_ref.shape
    lane = lax.broadcasted_iota(jnp.int32, (ny, LANES), 1)
    row = lax.broadcasted_iota(jnp.int32, (ny, LANES), 0)
    def field(f, carry):
        low_x, high_x = pick("gx", x_in, lambda ref: ref[f])
        for x in planes:
            low_y, high_y = pick("gy", y_in, lambda ref: ref[f, x])
            v = v_ref[f, x]
            end = pltpu.roll(ends, lax.rem(LANES - 2 * (f * nx + x), LANES), 1)
            beside = (v_ref[f, x - 1] if x > 0 else low_x) + (v_ref[f, x + 1] if x < nx - 1 else high_x)
            beside += jnp.where(row == 0, low_y, pltpu.roll(v, 1, 0))
            beside += jnp.where(row == ny - 1, high_y, pltpu.roll(v, ny - 1, 0))
            beside += jnp.where(lane == 0, end, pltpu.roll(v, 1, 1))
            beside += jnp.where(lane == LANES - 1, end, pltpu.roll(v, LANES - 1, 1))
            out_ref[f, x] = ((6.0 - CENTRE) + shift_ref[x]) * v - beside
        return carry

    lax.fori_loop(0, width, field, 0)


def split(refs, *counts):
    parts, at = [], 0
    for count in counts:
        parts.append(refs[at : at + count])
        at += count
    return (*parts, refs[at:])


def inner_planes(ref):
    return range(1, ref.shape[1] - 1)


def outer_planes(ref):
    return (0, ref.shape[1] - 1)


def inner_operator_kernel(ny_r, nz_r, v_ref, shift_ref, own_ref, *refs):
    y_in, z_in, (out_ref, ends_ref) = split(refs, ny_r, nz_r)
    near, base = operator_on_ends(v_ref.shape[1], own_ref[0], z_in)
    ends_ref[0] = near
    ends_ref[1] = base
    apply_operator(inner_planes(v_ref), v_ref, shift_ref, (), y_in, near, out_ref)


def outer_operator_kernel(nx_r, ny_r, v_ref, shift_ref, inner_ref, ends_ref, *refs):
    x_in, y_in, (out_ref,), x_out, y_out = split(refs, nx_r, ny_r, 1, nx_r)
    width, nx, ny, _ = v_ref.shape
    near = ends_ref[0]
    apply_operator(outer_planes(v_ref), v_ref, shift_ref, x_in, y_in, near, out_ref)
    for k, ref in enumerate(x_out):
        ref[:width] = out_ref[:, x_plane(k, nx)]
        ref[width] = near
    write_y_faces(out_ref, [ref.at[:width] for ref in y_out])
    for k, ref in enumerate(y_out):
        high = jnp.logical_xor(parity("gy"), k == 0)
        line = jnp.where(high, near[ny - 1 : ny], near[0:1])
        for x in range(nx):
            ref[width, x] = line


def pairs_of(width):
    return [(i, j) for i in range(width) for j in range(i + 1)]


def moment_sums(first, last, step, a_ref, b_ref, sums):
    width, _, ny, _ = a_ref.shape
    pairs = pairs_of(width)

    def plane(k, sums):
        sums, x = list(sums), first + k * step
        for y in range(0, ny, 8):
            a = [a_ref[f, x, y : y + 8, :] for f in range(width)]
            b = a if b_ref is a_ref else [b_ref[f, x, y : y + 8, :] for f in range(width)]
            for k, (i, j) in enumerate(pairs):
                sums[k] = sums[k] + a[i] * b[j]
        return tuple(sums)

    return lax.fori_loop(0, -((first - last) // step), plane, tuple(sums))


def no_sums(width):
    return [jnp.zeros((8, LANES), F32) for _ in pairs_of(width)]


def put_moment(width, sums, at, payload):
    rows = {}
    for (i, j), value in zip(pairs_of(width), sums):
        rows[i, j] = rows[j, i] = jnp.sum(value, axis=0, keepdims=True)
    lane = lax.broadcasted_iota(jnp.int32, (8, LANES), 1)
    for i in range(width):
        column = jnp.sum(jnp.concatenate([rows[i, j] for j in range(width)], axis=0), axis=1, keepdims=True)
        payload = jnp.where(lane == at + i, column, payload)
    return payload


def early_moments_kernel(b_ref, u_ref, out_ref):
    width, nx = b_ref.shape[:2]
    payload = jnp.zeros((8, LANES), F32)
    for k, (left, right) in enumerate(((b_ref, b_ref), (b_ref, u_ref), (u_ref, u_ref))):
        payload = put_moment(width, moment_sums(0, nx, 1, left, right, no_sums(width)), k * width, payload)
    out_ref[...] = payload


def inner_late_kernel(ny_r, u_ref, shift_ref, ends_ref, *refs):
    y_in, (sums_ref, t_ref) = split(refs, ny_r)
    width, nx = u_ref.shape[:2]
    ends = finished_ends(nx, ends_ref[1], (), y_in, width)
    apply_operator(inner_planes(u_ref), u_ref, shift_ref, (), y_in, ends, t_ref)
    for h, left in enumerate((u_ref, t_ref)):
        for k, value in enumerate(moment_sums(1, nx - 1, 1, left, t_ref, no_sums(width))):
            sums_ref[h, k] = value


def outer_late_kernel(nx_r, ny_r, u_ref, shift_ref, ends_ref, sums_ref, early_ref, *refs):
    x_in, y_in, (out_ref, t_ref) = split(refs, nx_r, ny_r)
    width, nx = u_ref.shape[:2]
    ends = finished_ends(nx, ends_ref[1], x_in, y_in, width)
    apply_operator(outer_planes(u_ref), u_ref, shift_ref, x_in, y_in, ends, t_ref)
    payload = early_ref[...]
    for h, left in enumerate((u_ref, t_ref)):
        inner = [sums_ref[h, k] for k in range(len(pairs_of(width)))]
        payload = put_moment(width, moment_sums(0, nx, nx - 1, left, t_ref, inner), (3 + h) * width, payload)
    out_ref[...] = jnp.broadcast_to(payload[None], out_ref.shape)


def lanes_of(matrix, j):
    return jnp.broadcast_to(matrix[:, j : j + 1], matrix.shape)


def rows_of(matrix, i):
    return jnp.broadcast_to(matrix[i : i + 1, :], matrix.shape)


def times(left, at, right):
    count = left.shape[0]
    total = lanes_of(left, at) * rows_of(right, 0)
    for k in range(1, count):
        total = total + lanes_of(left, at + k) * rows_of(right, k)
    return total


def shift_lanes(matrix, by):
    return pltpu.roll(matrix, by % LANES, 1)


def eliminate(blocks):
    size = blocks[0].shape[0]
    sub = lax.broadcasted_iota(jnp.int32, blocks[0].shape, 0)
    for j in range(size * len(blocks)):
        own, local = divmod(j, size)
        columns = [lanes_of(block, j) for block in blocks]
        pivot = rows_of(blocks[own], local) / rows_of(columns[own], local)
        blocks = [block - column * pivot for block, column in zip(blocks, columns)]
        blocks[own] = jnp.where(sub == local, pivot, blocks[own])
    return blocks


def small_algebra(s):
    n = s.shape[0]
    c0 = CENTRE
    lane = lax.broadcasted_iota(jnp.int32, s.shape, 1)
    sub = lax.broadcasted_iota(jnp.int32, s.shape, 0)
    n0, n1, n2, n3, n4 = shift_lanes(s, n), s, shift_lanes(s, -n), shift_lanes(s, -2 * n), shift_lanes(s, -3 * n)
    (e,) = eliminate([s])
    p1 = times(s, n, e)
    p2 = times(s, 2 * n, e)
    p3 = times(s, 3 * n, e)
    cc = times(e, n, e)
    e2c = times(e, 2 * n, e)
    g = n2 - p1
    q = shift_lanes(e, -n) - cc
    n3c = n3 - p2
    f3 = n3c - times(s, n, q)
    f4 = n4 - p3 - times(s, n, shift_lanes(e, -2 * n) - e2c)
    m11 = n2 + 2.0 * c0 * n1 + c0 * c0 * n0
    m12 = n3c + 2.0 * c0 * g
    m21 = n3 - shift_lanes(p1, -n) + 2.0 * c0 * g
    m22 = f4 + 2.0 * c0 * f3 + c0 * c0 * g
    r1 = n1 + c0 * n0

    def assemble(first, second, third):
        joined = jnp.where(lane < n, shift_lanes(first, -n), second)
        return jnp.where(lane < 2 * n, joined, shift_lanes(third, n))

    pa, qa = eliminate([assemble(m11, m12, r1), assemble(m21, m22, g)])
    cq = times(e, n, qa)
    on_b = pa - cq
    unit = jnp.where(lane == sub + 2 * n, 1.0, 0.0)
    part = unit - times(e, n, pa) - c0 * pa - times(q, n, qa)
    squares = part * times(s, 0, part)
    pq = pa + c0 * qa
    squares = squares + pq * (times(g, n, pq) + 2.0 * times(f3, n, qa))
    squares = squares + qa * times(f4 - times(g, n, q), n, qa)
    return on_b, qa, jnp.sum(squares, axis=0, keepdims=True)


def finish_kernel(parts_ref, b_ref, u_ref, out_ref, norms_ref, coeff_ref):
    width, nx, ny, _ = b_ref.shape
    n = width
    total = jnp.sum(parts_ref[...], axis=0)
    on_b, on_u, squares = small_algebra(total)
    norms_ref[...] = jnp.sqrt(shift_lanes(squares, -2 * n))[:, :n]
    for f in range(width):
        coeff_ref[0, f] = lanes_of(on_b, 2 * n + f)
        coeff_ref[1, f] = lanes_of(on_u, 2 * n + f)
    group = 2

    def fields(k, carry):
        first = [[[rows_of(coeff_ref[h, group * k + d], g) for g in range(width)] for h in range(2)] for d in range(group)]

        def plane(x, carry):
            for y in range(0, ny, 8):
                b = [b_ref[g, x, y : y + 8, :] for g in range(width)]
                u = [u_ref[g, x, y : y + 8, :] for g in range(width)]
                for d in range(group):
                    total = first[d][0][0] * b[0] + first[d][1][0] * u[0]
                    for g in range(1, width):
                        total = total + (first[d][0][g] * b[g] + first[d][1][g] * u[g])
                    out_ref[group * k + d, x, y : y + 8, :] = total
            return carry

        return lax.fori_loop(0, nx, plane, carry)

    lax.fori_loop(0, width // group, fields, 0)


def call(kernel, out_shape, operands, scratch=(), flops=1_000_000, name=None, aliases=None, far=False):
    return pl.pallas_call(
        kernel,
        out_shape=out_shape,
        in_specs=[pl.BlockSpec(memory_space=pl.ANY if far else pltpu.VMEM)] * len(operands),
        out_specs=jax.tree.map(lambda _: pl.BlockSpec(memory_space=pltpu.VMEM), out_shape),
        scratch_shapes=list(scratch),
        input_output_aliases=aliases or {},
        compiler_params=pltpu.CompilerParams(vmem_limit_bytes=8 << 20),
        cost_estimate=pl.CostEstimate(flops=flops, bytes_accessed=1 << 20, transcendentals=0),
        name=name,
    )(*operands)


def trade(turn, axis, faces):
    out = []
    for k, (face, pairs) in enumerate(zip(faces, swap_pairs(lax.axis_size(axis)))):
        with jax.named_scope(f"turn{turn}_{axis}_{k}"):
            out.append(swap(face, axis, pairs))
    return out


def body(right_side, shift):
    width, nx, ny, nz = right_side.shape
    assert width == 8 and nz == LANES and ny % 8 == 0 and nx > 2 and width * nx <= LANES // 2
    nx_r, ny_r, nz_r = rounds_of()
    devices = 1
    for axis in AXES:
        devices *= lax.axis_size(axis)
    assert nz_r > 0
    block = jax.ShapeDtypeStruct(right_side.shape, F32)
    full = pltpu.VMEM(right_side.shape, F32)
    kernel = functools.partial

    def x_faces(fields):
        return [jax.ShapeDtypeStruct((fields, ny, nz), F32)] * nx_r

    def y_faces(fields):
        return [jax.ShapeDtypeStruct((fields, nx, 1, nz), F32)] * ny_r

    def ends_of(layers):
        return jax.ShapeDtypeStruct((layers, ny, LANES), F32)

    faces = call(cut_x_kernel, x_faces(width), [right_side], scratch=[pltpu.SemaphoreType.DMA((max(nx_r, 1),))], name="cut", far=True)
    halo_x = trade(1, "gx", faces)
    *faces, own = call(pack_kernel, [*y_faces(width), ends_of(3)], [right_side, shift], name="pack")
    halo_y = trade(1, "gy", faces)
    halo_z = trade(1, "gz", [own] * nz_r)
    inner, ends = call(
        kernel(inner_operator_kernel, ny_r, nz_r),
        [block, ends_of(2)],
        [right_side, shift, own, *halo_y, *halo_z],
        flops=20_000_000,
        name="inner1",
    )
    u, *faces = call(
        kernel(outer_operator_kernel, nx_r, ny_r),
        [block, *x_faces(width + 1), *y_faces(width + 1)],
        [right_side, shift, inner, ends, *halo_x, *halo_y],
        aliases={2: 0},
        name="outer1",
    )
    halo_x = trade(2, "gx", faces[:nx_r])
    halo_y = trade(2, "gy", faces[nx_r:])
    early = call(early_moments_kernel, jax.ShapeDtypeStruct((8, LANES), F32), [right_side, u], flops=15_000_000, name="early")
    sums = call(
        kernel(inner_late_kernel, ny_r),
        jax.ShapeDtypeStruct((2, len(pairs_of(width)), 8, LANES), F32),
        [u, shift, ends, *halo_y],
        scratch=[full],
        flops=15_000_000,
        name="inner2",
    )
    copies = call(
        kernel(outer_late_kernel, nx_r, ny_r),
        jax.ShapeDtypeStruct((devices, 8, LANES), F32),
        [u, shift, ends, sums, early, *halo_x, *halo_y],
        scratch=[full],
        name="outer2",
    )
    parts = lax.all_to_all(copies, AXES, 0, 0, tiled=True)
    out, norms = call(
        finish_kernel,
        [block, jax.ShapeDtypeStruct((1, width), F32)],
        [parts, right_side, u],
        scratch=[pltpu.VMEM((2, width, 8, LANES), F32)],
        name="finish",
    )
    return out, norms.reshape(width)


def solution(mesh):
    in_specs = (P(None, "gx", "gy", "gz"), P("gx", "gy", "gz"))
    out_specs = (P(None, "gx", "gy", "gz"), P())
    return jax.shard_map(body, mesh=mesh, in_specs=in_specs, out_specs=out_specs, check_vma=False)
```

```python
import functools

import jax
import jax.numpy as jnp
from jax import lax
from jax.experimental import pallas as pl
from jax.experimental.pallas import tpu as pltpu
from jax.sharding import PartitionSpec as P

AXES = ("gx", "gy", "gz")
CENTRE = 7.0
LANES = 128
F32 = jnp.float32


def swap_pairs(count):
    first = [(i, j) for a in range(0, count - 1, 2) for i, j in ((a, a + 1), (a + 1, a))]
    second = [(i, j) for a in range(1, count - 1, 2) for i, j in ((a, a + 1), (a + 1, a))]
    return [pairs for pairs in (first, second) if pairs]


def swap(values, axis, pairs):
    side = lax.axis_size("gy")
    if axis == "gy" or side % 2:
        return lax.ppermute(values, axis, pairs)
    count = lax.axis_size(axis)
    named = {i for i, _ in pairs}
    at = (lambda i, y: i * side + y) if axis == "gx" else (lambda i, y: y * count + i)
    joint = [(at(i, y), at(j, y)) for i, j in pairs for y in range(side)]
    joint += [(at(i, y), at(i, y ^ 1)) for i in range(count) if i not in named for y in range(side)]
    return lax.ppermute(values, ("gx", "gy") if axis == "gx" else ("gy", "gz"), joint)


def rounds_of():
    return tuple(len(swap_pairs(lax.axis_size(axis))) for axis in AXES)


def parity(axis):
    return lax.rem(lax.axis_index(axis), 2) == 1


def x_plane(k, nx):
    return jnp.where(jnp.logical_xor(parity("gx"), k == 0), nx - 1, 0)


def cut_x_kernel(v_ref, *refs):
    faces, sems = refs[:-1], refs[-1]
    copies = [
        pltpu.make_async_copy(v_ref.at[:, x_plane(k, v_ref.shape[1])], ref, sems.at[k]) for k, ref in enumerate(faces)
    ]
    for copy in copies:
        copy.start()
    for copy in copies:
        copy.wait()


def write_y_faces(v_ref, y_refs):
    ny = v_ref.shape[2]
    odd = parity("gy")
    for k, ref in enumerate(y_refs):
        high = jnp.logical_xor(odd, k == 0)
        ref[...] = jnp.where(high, v_ref[:, :, ny - 1 : ny, :], v_ref[:, :, 0:1, :])


def packed_ends(tile, m, lane, near, far=None):
    def at(offset):
        return lane == lax.rem(2 * m + offset + LANES, LANES)

    turned = pltpu.roll(tile, 2 * m, 1)
    near = jnp.where(at(0) | at(-1), turned, near)
    if far is None:
        return near
    return near, jnp.where(at(1) | at(-2), turned, far)


def pack_kernel(v_ref, shift_ref, *refs):
    width, nx, ny, _ = v_ref.shape
    write_y_faces(v_ref, refs[:-1])
    lane = lax.broadcasted_iota(jnp.int32, (ny, LANES), 1)
    nothing = jnp.zeros((ny, LANES), F32)

    def field(f, packed):
        for x in range(nx):
            packed = packed_ends(v_ref[f, x], f * nx + x, lane, *packed)
        return packed

    near, far = lax.fori_loop(0, width, field, (nothing, nothing))
    diagonal = nothing
    for x in range(nx):
        diagonal = packed_ends((6.0 - CENTRE) + shift_ref[x], x, lane, diagonal)
    copies = 1
    while copies < width:
        diagonal = diagonal + pltpu.roll(diagonal, 2 * nx * copies, 1)
        copies *= 2
    refs[-1][0] = near
    refs[-1][1] = far
    refs[-1][2] = diagonal


def pick(axis, refs, load):
    if not refs:
        return 0.0, 0.0
    odd, at = parity(axis), lax.axis_index(axis)
    first = load(refs[0])
    second = load(refs[1]) if len(refs) > 1 else jnp.zeros_like(first)
    low = jnp.where(at == 0, 0.0, jnp.where(odd, first, second))
    high = jnp.where(at == lax.axis_size(axis) - 1, 0.0, jnp.where(odd, second, first))
    return low, high


def halo_ends(z_in, layer):
    low, high = pick("gz", z_in, lambda ref: ref[layer])
    if not z_in:
        return None
    lane = lax.broadcasted_iota(jnp.int32, low.shape, 1)
    by = 2 if layer == 1 else 1
    return jnp.where(lax.rem(lane, 2) == 0, pltpu.roll(low, by, 1), pltpu.roll(high, LANES - by, 1))


def inside_grid(lane):
    low = jnp.where(lax.axis_index("gz") == 0, 0.0, 1.0)
    high = jnp.where(lax.axis_index("gz") == lax.axis_size("gz") - 1, 0.0, 1.0)
    return jnp.where(lax.rem(lane, 2) == 0, low, high)


def lane_x(lane, nx):
    return lax.rem((lane + 1) // 2, nx)


def operator_on_ends(nx, own, z_in):
    near, far, diagonal = (halo_ends(z_in, layer) for layer in range(3))
    ny = near.shape[0]
    lane = lax.broadcasted_iota(jnp.int32, near.shape, 1)
    row = lax.broadcasted_iota(jnp.int32, near.shape, 0)
    x = lane_x(lane, nx)
    beside = own + far
    beside += jnp.where(x == 0, 0.0, pltpu.roll(near, 2, 1)) + jnp.where(x == nx - 1, 0.0, pltpu.roll(near, LANES - 2, 1))
    beside += jnp.where(row == 0, 0.0, pltpu.roll(near, 1, 0)) + jnp.where(row == ny - 1, 0.0, pltpu.roll(near, ny - 1, 0))
    return near, inside_grid(lane) * (diagonal * near - beside)


def finished_ends(nx, base, x_in, y_in, width):
    ny = base.shape[0]
    lane = lax.broadcasted_iota(jnp.int32, base.shape, 1)
    row = lax.broadcasted_iota(jnp.int32, base.shape, 0)
    low_y, high_y = pick("gy", y_in, lambda ref: ref[width, 0])
    beside = jnp.where(row == 0, low_y, 0.0) + jnp.where(row == ny - 1, high_y, 0.0)
    if x_in:
        x, by = lane_x(lane, nx), 2 * (nx - 1)
        low_x, high_x = pick("gx", x_in, lambda ref: ref[width])
        beside += jnp.where(x == 0, pltpu.roll(low_x, LANES - by, 1), 0.0)
        beside += jnp.where(x == nx - 1, pltpu.roll(high_x, by, 1), 0.0)
    return base - inside_grid(lane) * beside


def apply_operator(planes, v_ref, shift_ref, x_in, y_in, ends, out_ref):
    width, nx, ny, _ = v_ref.shape
    lane = lax.broadcasted_iota(jnp.int32, (ny, LANES), 1)
    row = lax.broadcasted_iota(jnp.int32, (ny, LANES), 0)
    def field(f, carry):
        low_x, high_x = pick("gx", x_in, lambda ref: ref[f])
        for x in planes:
            low_y, high_y = pick("gy", y_in, lambda ref: ref[f, x])
            v = v_ref[f, x]
            end = pltpu.roll(ends, lax.rem(LANES - 2 * (f * nx + x), LANES), 1)
            beside = (v_ref[f, x - 1] if x > 0 else low_x) + (v_ref[f, x + 1] if x < nx - 1 else high_x)
            beside += jnp.where(row == 0, low_y, pltpu.roll(v, 1, 0))
            beside += jnp.where(row == ny - 1, high_y, pltpu.roll(v, ny - 1, 0))
            beside += jnp.where(lane == 0, end, pltpu.roll(v, 1, 1))
            beside += jnp.where(lane == LANES - 1, end, pltpu.roll(v, LANES - 1, 1))
            out_ref[f, x] = ((6.0 - CENTRE) + shift_ref[x]) * v - beside
        return carry

    lax.fori_loop(0, width, field, 0)


def split(refs, *counts):
    parts, at = [], 0
    for count in counts:
        parts.append(refs[at : at + count])
        at += count
    return (*parts, refs[at:])


def inner_planes(ref):
    return range(1, ref.shape[1] - 1)


def outer_planes(ref):
    return (0, ref.shape[1] - 1)


def inner_operator_kernel(ny_r, nz_r, v_ref, shift_ref, own_ref, *refs):
    y_in, z_in, (out_ref, ends_ref) = split(refs, ny_r, nz_r)
    near, base = operator_on_ends(v_ref.shape[1], own_ref[0], z_in)
    ends_ref[0] = near
    ends_ref[1] = base
    apply_operator(inner_planes(v_ref), v_ref, shift_ref, (), y_in, near, out_ref)


def outer_operator_kernel(nx_r, ny_r, v_ref, shift_ref, inner_ref, ends_ref, *refs):
    x_in, y_in, (out_ref,), x_out, y_out = split(refs, nx_r, ny_r, 1, nx_r)
    width, nx, ny, _ = v_ref.shape
    near = ends_ref[0]
    apply_operator(outer_planes(v_ref), v_ref, shift_ref, x_in, y_in, near, out_ref)
    for k, ref in enumerate(x_out):
        ref[:width] = out_ref[:, x_plane(k, nx)]
        ref[width] = near
    write_y_faces(out_ref, [ref.at[:width] for ref in y_out])
    for k, ref in enumerate(y_out):
        high = jnp.logical_xor(parity("gy"), k == 0)
        line = jnp.where(high, near[ny - 1 : ny], near[0:1])
        for x in range(nx):
            ref[width, x] = line


def pairs_of(width):
    return [(i, j) for i in range(width) for j in range(i + 1)]


def moment_sums(first, last, step, a_ref, b_ref, sums):
    width, _, ny, _ = a_ref.shape
    pairs = pairs_of(width)

    def plane(k, sums):
        sums, x = list(sums), first + k * step
        for y in range(0, ny, 8):
            a = [a_ref[f, x, y : y + 8, :] for f in range(width)]
            b = a if b_ref is a_ref else [b_ref[f, x, y : y + 8, :] for f in range(width)]
            for k, (i, j) in enumerate(pairs):
                sums[k] = sums[k] + a[i] * b[j]
        return tuple(sums)

    return lax.fori_loop(0, -((first - last) // step), plane, tuple(sums))


def no_sums(width):
    return [jnp.zeros((8, LANES), F32) for _ in pairs_of(width)]


def put_moment(width, sums, at, payload):
    rows = {}
    for (i, j), value in zip(pairs_of(width), sums):
        rows[i, j] = rows[j, i] = jnp.sum(value, axis=0, keepdims=True)
    lane = lax.broadcasted_iota(jnp.int32, (8, LANES), 1)
    for i in range(width):
        column = jnp.sum(jnp.concatenate([rows[i, j] for j in range(width)], axis=0), axis=1, keepdims=True)
        payload = jnp.where(lane == at + i, column, payload)
    return payload


def early_moments_kernel(b_ref, u_ref, out_ref):
    width, nx = b_ref.shape[:2]
    payload = jnp.zeros((8, LANES), F32)
    for k, (left, right) in enumerate(((b_ref, b_ref), (b_ref, u_ref), (u_ref, u_ref))):
        payload = put_moment(width, moment_sums(0, nx, 1, left, right, no_sums(width)), k * width, payload)
    out_ref[...] = payload


def inner_late_kernel(ny_r, u_ref, shift_ref, ends_ref, *refs):
    y_in, (sums_ref, t_ref) = split(refs, ny_r)
    width, nx = u_ref.shape[:2]
    ends = finished_ends(nx, ends_ref[1], (), y_in, width)
    apply_operator(inner_planes(u_ref), u_ref, shift_ref, (), y_in, ends, t_ref)
    for h, left in enumerate((u_ref, t_ref)):
        for k, value in enumerate(moment_sums(1, nx - 1, 1, left, t_ref, no_sums(width))):
            sums_ref[h, k] = value


def outer_late_kernel(nx_r, ny_r, u_ref, shift_ref, ends_ref, sums_ref, early_ref, *refs):
    x_in, y_in, (out_ref, t_ref) = split(refs, nx_r, ny_r)
    width, nx = u_ref.shape[:2]
    ends = finished_ends(nx, ends_ref[1], x_in, y_in, width)
    apply_operator(outer_planes(u_ref), u_ref, shift_ref, x_in, y_in, ends, t_ref)
    payload = early_ref[...]
    for h, left in enumerate((u_ref, t_ref)):
        inner = [sums_ref[h, k] for k in range(len(pairs_of(width)))]
        payload = put_moment(width, moment_sums(0, nx, nx - 1, left, t_ref, inner), (3 + h) * width, payload)
    out_ref[...] = jnp.broadcast_to(payload[None], out_ref.shape)


def lanes_of(matrix, j):
    return jnp.broadcast_to(matrix[:, j : j + 1], matrix.shape)


def rows_of(matrix, i):
    return jnp.broadcast_to(matrix[i : i + 1, :], matrix.shape)


def times(left, at, right):
    count = left.shape[0]
    total = lanes_of(left, at) * rows_of(right, 0)
    for k in range(1, count):
        total = total + lanes_of(left, at + k) * rows_of(right, k)
    return total


def shift_lanes(matrix, by):
    return pltpu.roll(matrix, by % LANES, 1)


def solve(columns, right):
    size = right[0].shape[0]
    sub = lax.broadcasted_iota(jnp.int32, right[0].shape, 0)
    for j in range(0, len(columns), 2):
        own, local = divmod(j, size)
        first, second = columns[j], columns[j + 1]
        a, b = rows_of(first[own], local), rows_of(second[own], local)
        c, d = rows_of(first[own], local + 1), rows_of(second[own], local + 1)
        scale = 1.0 / (a * d - b * c)
        a, b, c, d = a * scale, b * scale, c * scale, d * scale

        def step(value):
            upper, lower = rows_of(value[own], local), rows_of(value[own], local + 1)
            upper, lower = d * upper - b * lower, a * lower - c * upper
            value = [v - (f * upper + s * lower) for v, f, s in zip(value, first, second)]
            value[own] = jnp.where(sub == local, upper, jnp.where(sub == local + 1, lower, value[own]))
            return value

        columns = columns[: j + 2] + [step(column) for column in columns[j + 2 :]]
        right = step(right)
    return right


def small_algebra(s):
    n = s.shape[0]
    c0 = CENTRE
    lane = lax.broadcasted_iota(jnp.int32, s.shape, 1)
    sub = lax.broadcasted_iota(jnp.int32, s.shape, 0)
    n0, n1, n2, n3, n4 = shift_lanes(s, n), s, shift_lanes(s, -n), shift_lanes(s, -2 * n), shift_lanes(s, -3 * n)
    (e,) = solve([[lanes_of(s, j)] for j in range(n)], [s])
    p1 = times(s, n, e)
    p2 = times(s, 2 * n, e)
    p3 = times(s, 3 * n, e)
    cc = times(e, n, e)
    e2c = times(e, 2 * n, e)
    e2 = shift_lanes(e, -n)
    g = n2 - p1
    q = e2 - cc
    n3c = n3 - p2
    f3 = n3c - times(s, n, q)
    f4 = n4 - p3 - times(s, n, shift_lanes(e, -2 * n) - e2c)
    m11 = n2 + 2.0 * c0 * n1 + c0 * c0 * n0
    m12 = n3c + 2.0 * c0 * g
    m21 = n3 - times(s, n, e2) + 2.0 * c0 * g
    m22 = f4 + 2.0 * c0 * f3 + c0 * c0 * g
    columns = [[lanes_of(m11, n + j), lanes_of(m21, n + j)] for j in range(n)]
    columns += [[lanes_of(m12, n + j), lanes_of(m22, n + j)] for j in range(n)]
    pa, qa = solve(columns, [n1 + c0 * n0, g])
    on_b = pa - times(e, n, qa)
    unit = jnp.where(lane == sub + n, 1.0, 0.0)
    part = unit - times(e, n, pa) - c0 * pa - times(q, n, qa)
    squares = part * times(s, 0, part)
    pq = pa + c0 * qa
    squares = squares + pq * (times(g, n, pq) + 2.0 * times(f3, n, qa))
    squares = squares + qa * times(f4 - times(g, n, q), n, qa)
    return on_b, qa, jnp.sum(squares, axis=0, keepdims=True)


def finish_kernel(parts_ref, b_ref, u_ref, out_ref, norms_ref, coeff_ref):
    width, nx, ny, _ = b_ref.shape
    n = width
    total = jnp.sum(parts_ref[...], axis=0)
    on_b, on_u, squares = small_algebra(total)
    norms_ref[...] = jnp.sqrt(shift_lanes(squares, -n))[:, :n]
    for f in range(width):
        coeff_ref[0, f] = lanes_of(on_b, n + f)
        coeff_ref[1, f] = lanes_of(on_u, n + f)
    group = 2

    def fields(k, carry):
        first = [[[rows_of(coeff_ref[h, group * k + d], g) for g in range(width)] for h in range(2)] for d in range(group)]

        def plane(x, carry):
            for y in range(0, ny, 8):
                b = [b_ref[g, x, y : y + 8, :] for g in range(width)]
                u = [u_ref[g, x, y : y + 8, :] for g in range(width)]
                for d in range(group):
                    total = first[d][0][0] * b[0] + first[d][1][0] * u[0]
                    for g in range(1, width):
                        total = total + (first[d][0][g] * b[g] + first[d][1][g] * u[g])
                    out_ref[group * k + d, x, y : y + 8, :] = total
            return carry

        return lax.fori_loop(0, nx, plane, carry)

    lax.fori_loop(0, width // group, fields, 0)


def call(kernel, out_shape, operands, scratch=(), flops=1_000_000, name=None, aliases=None, far=False):
    return pl.pallas_call(
        kernel,
        out_shape=out_shape,
        in_specs=[pl.BlockSpec(memory_space=pl.ANY if far else pltpu.VMEM)] * len(operands),
        out_specs=jax.tree.map(lambda _: pl.BlockSpec(memory_space=pltpu.VMEM), out_shape),
        scratch_shapes=list(scratch),
        input_output_aliases=aliases or {},
        compiler_params=pltpu.CompilerParams(vmem_limit_bytes=8 << 20),
        cost_estimate=pl.CostEstimate(flops=flops, bytes_accessed=1 << 20, transcendentals=0),
        name=name,
    )(*operands)


def trade(turn, axis, faces):
    out = []
    for k, (face, pairs) in enumerate(zip(faces, swap_pairs(lax.axis_size(axis)))):
        with jax.named_scope(f"turn{turn}_{axis}_{k}"):
            out.append(swap(face, axis, pairs))
    return out


def body(right_side, shift):
    width, nx, ny, nz = right_side.shape
    assert width == 8 and nz == LANES and ny % 8 == 0 and nx > 2 and width * nx <= LANES // 2
    nx_r, ny_r, nz_r = rounds_of()
    devices = 1
    for axis in AXES:
        devices *= lax.axis_size(axis)
    assert nz_r > 0
    block = jax.ShapeDtypeStruct(right_side.shape, F32)
    full = pltpu.VMEM(right_side.shape, F32)
    kernel = functools.partial

    def x_faces(fields):
        return [jax.ShapeDtypeStruct((fields, ny, nz), F32)] * nx_r

    def y_faces(fields):
        return [jax.ShapeDtypeStruct((fields, nx, 1, nz), F32)] * ny_r

    def ends_of(layers):
        return jax.ShapeDtypeStruct((layers, ny, LANES), F32)

    faces = call(cut_x_kernel, x_faces(width), [right_side], scratch=[pltpu.SemaphoreType.DMA((max(nx_r, 1),))], name="cut", far=True)
    halo_x = trade(1, "gx", faces)
    *faces, own = call(pack_kernel, [*y_faces(width), ends_of(3)], [right_side, shift], name="pack")
    halo_y = trade(1, "gy", faces)
    halo_z = trade(1, "gz", [own] * nz_r)
    inner, ends = call(
        kernel(inner_operator_kernel, ny_r, nz_r),
        [block, ends_of(2)],
        [right_side, shift, own, *halo_y, *halo_z],
        flops=20_000_000,
        name="inner1",
    )
    u, *faces = call(
        kernel(outer_operator_kernel, nx_r, ny_r),
        [block, *x_faces(width + 1), *y_faces(width + 1)],
        [right_side, shift, inner, ends, *halo_x, *halo_y],
        aliases={2: 0},
        name="outer1",
    )
    halo_x = trade(2, "gx", faces[:nx_r])
    halo_y = trade(2, "gy", faces[nx_r:])
    early = call(early_moments_kernel, jax.ShapeDtypeStruct((8, LANES), F32), [right_side, u], flops=15_000_000, name="early")
    sums = call(
        kernel(inner_late_kernel, ny_r),
        jax.ShapeDtypeStruct((2, len(pairs_of(width)), 8, LANES), F32),
        [u, shift, ends, *halo_y],
        scratch=[full],
        flops=15_000_000,
        name="inner2",
    )
    copies = call(
        kernel(outer_late_kernel, nx_r, ny_r),
        jax.ShapeDtypeStruct((devices, 8, LANES), F32),
        [u, shift, ends, sums, early, *halo_x, *halo_y],
        scratch=[full],
        name="outer2",
    )
    parts = lax.all_to_all(copies, AXES, 0, 0, tiled=True)
    out, norms = call(
        finish_kernel,
        [block, jax.ShapeDtypeStruct((1, width), F32)],
        [parts, right_side, u],
        scratch=[pltpu.VMEM((2, width, 8, LANES), F32)],
        name="finish",
    )
    return out, norms.reshape(width)


def solution(mesh):
    in_specs = (P(None, "gx", "gy", "gz"), P("gx", "gy", "gz"))
    out_specs = (P(None, "gx", "gy", "gz"), P())
    return jax.shard_map(body, mesh=mesh, in_specs=in_specs, out_specs=out_specs, check_vma=False)
```

```python
import functools

import jax
import jax.numpy as jnp
from jax import lax
from jax.experimental import pallas as pl
from jax.experimental.pallas import tpu as pltpu
from jax.sharding import PartitionSpec as P

AXES = ("gx", "gy", "gz")
CENTRE = 7.0
LANES = 128
F32 = jnp.float32


def swap_pairs(count):
    first = [(i, j) for a in range(0, count - 1, 2) for i, j in ((a, a + 1), (a + 1, a))]
    second = [(i, j) for a in range(1, count - 1, 2) for i, j in ((a, a + 1), (a + 1, a))]
    return [pairs for pairs in (first, second) if pairs]


def swap(values, axis, pairs):
    side = lax.axis_size("gy")
    if axis == "gy" or side % 2:
        return lax.ppermute(values, axis, pairs)
    count = lax.axis_size(axis)
    named = {i for i, _ in pairs}
    at = (lambda i, y: i * side + y) if axis == "gx" else (lambda i, y: y * count + i)
    joint = [(at(i, y), at(j, y)) for i, j in pairs for y in range(side)]
    joint += [(at(i, y), at(i, y ^ 1)) for i in range(count) if i not in named for y in range(side)]
    return lax.ppermute(values, ("gx", "gy") if axis == "gx" else ("gy", "gz"), joint)


def rounds_of():
    return tuple(len(swap_pairs(lax.axis_size(axis))) for axis in AXES)


def parity(axis):
    return lax.rem(lax.axis_index(axis), 2) == 1


def x_plane(k, nx):
    return jnp.where(jnp.logical_xor(parity("gx"), k == 0), nx - 1, 0)


def cut_x_kernel(v_ref, *refs):
    faces, sems = refs[:-1], refs[-1]
    copies = [
        pltpu.make_async_copy(v_ref.at[:, x_plane(k, v_ref.shape[1])], ref, sems.at[k]) for k, ref in enumerate(faces)
    ]
    for copy in copies:
        copy.start()
    for copy in copies:
        copy.wait()


def write_y_faces(v_ref, y_refs):
    ny = v_ref.shape[2]
    odd = parity("gy")
    for k, ref in enumerate(y_refs):
        high = jnp.logical_xor(odd, k == 0)
        ref[...] = jnp.where(high, v_ref[:, :, ny - 1 : ny, :], v_ref[:, :, 0:1, :])


def packed_ends(tile, m, lane, near, far=None):
    def at(offset):
        return lane == lax.rem(2 * m + offset + LANES, LANES)

    turned = pltpu.roll(tile, 2 * m, 1)
    near = jnp.where(at(0) | at(-1), turned, near)
    if far is None:
        return near
    return near, jnp.where(at(1) | at(-2), turned, far)


def pack_kernel(v_ref, shift_ref, *refs):
    width, nx, ny, _ = v_ref.shape
    write_y_faces(v_ref, refs[:-1])
    lane = lax.broadcasted_iota(jnp.int32, (ny, LANES), 1)
    nothing = jnp.zeros((ny, LANES), F32)

    def field(f, packed):
        for x in range(nx):
            packed = packed_ends(v_ref[f, x], f * nx + x, lane, *packed)
        return packed

    near, far = lax.fori_loop(0, width, field, (nothing, nothing), unroll=width)
    diagonal = nothing
    for x in range(nx):
        diagonal = packed_ends((6.0 - CENTRE) + shift_ref[x], x, lane, diagonal)
    copies = 1
    while copies < width:
        diagonal = diagonal + pltpu.roll(diagonal, 2 * nx * copies, 1)
        copies *= 2
    refs[-1][0] = near
    refs[-1][1] = far
    refs[-1][2] = diagonal


def pick(axis, refs, load):
    if not refs:
        return 0.0, 0.0
    odd, at = parity(axis), lax.axis_index(axis)
    first = load(refs[0])
    second = load(refs[1]) if len(refs) > 1 else jnp.zeros_like(first)
    low = jnp.where(at == 0, 0.0, jnp.where(odd, first, second))
    high = jnp.where(at == lax.axis_size(axis) - 1, 0.0, jnp.where(odd, second, first))
    return low, high


def halo_ends(z_in, layer):
    low, high = pick("gz", z_in, lambda ref: ref[layer])
    if not z_in:
        return None
    lane = lax.broadcasted_iota(jnp.int32, low.shape, 1)
    by = 2 if layer == 1 else 1
    return jnp.where(lax.rem(lane, 2) == 0, pltpu.roll(low, by, 1), pltpu.roll(high, LANES - by, 1))


def inside_grid(lane):
    low = jnp.where(lax.axis_index("gz") == 0, 0.0, 1.0)
    high = jnp.where(lax.axis_index("gz") == lax.axis_size("gz") - 1, 0.0, 1.0)
    return jnp.where(lax.rem(lane, 2) == 0, low, high)


def lane_x(lane, nx):
    return lax.rem((lane + 1) // 2, nx)


def operator_on_ends(nx, own, z_in):
    near, far, diagonal = (halo_ends(z_in, layer) for layer in range(3))
    ny = near.shape[0]
    lane = lax.broadcasted_iota(jnp.int32, near.shape, 1)
    row = lax.broadcasted_iota(jnp.int32, near.shape, 0)
    x = lane_x(lane, nx)
    beside = own + far
    beside += jnp.where(x == 0, 0.0, pltpu.roll(near, 2, 1)) + jnp.where(x == nx - 1, 0.0, pltpu.roll(near, LANES - 2, 1))
    beside += jnp.where(row == 0, 0.0, pltpu.roll(near, 1, 0)) + jnp.where(row == ny - 1, 0.0, pltpu.roll(near, ny - 1, 0))
    return near, inside_grid(lane) * (diagonal * near - beside)


def finished_ends(nx, base, x_in, y_in, width):
    ny = base.shape[0]
    lane = lax.broadcasted_iota(jnp.int32, base.shape, 1)
    row = lax.broadcasted_iota(jnp.int32, base.shape, 0)
    low_y, high_y = pick("gy", y_in, lambda ref: ref[width, 0])
    beside = jnp.where(row == 0, low_y, 0.0) + jnp.where(row == ny - 1, high_y, 0.0)
    if x_in:
        x, by = lane_x(lane, nx), 2 * (nx - 1)
        low_x, high_x = pick("gx", x_in, lambda ref: ref[width])
        beside += jnp.where(x == 0, pltpu.roll(low_x, LANES - by, 1), 0.0)
        beside += jnp.where(x == nx - 1, pltpu.roll(high_x, by, 1), 0.0)
    return base - inside_grid(lane) * beside


def apply_operator(planes, v_ref, shift_ref, x_in, y_in, ends, out_ref):
    width, nx, ny, _ = v_ref.shape
    lane = lax.broadcasted_iota(jnp.int32, (ny, LANES), 1)
    row = lax.broadcasted_iota(jnp.int32, (ny, LANES), 0)
    def field(f, carry):
        low_x, high_x = pick("gx", x_in, lambda ref: ref[f])
        for x in planes:
            low_y, high_y = pick("gy", y_in, lambda ref: ref[f, x])
            v = v_ref[f, x]
            end = pltpu.roll(ends, lax.rem(LANES - 2 * (f * nx + x), LANES), 1)
            beside = (v_ref[f, x - 1] if x > 0 else low_x) + (v_ref[f, x + 1] if x < nx - 1 else high_x)
            beside += jnp.where(row == 0, low_y, pltpu.roll(v, 1, 0))
            beside += jnp.where(row == ny - 1, high_y, pltpu.roll(v, ny - 1, 0))
            beside += jnp.where(lane == 0, end, pltpu.roll(v, 1, 1))
            beside += jnp.where(lane == LANES - 1, end, pltpu.roll(v, LANES - 1, 1))
            out_ref[f, x] = ((6.0 - CENTRE) + shift_ref[x]) * v - beside
        return carry

    lax.fori_loop(0, width, field, 0, unroll=width)


def split(refs, *counts):
    parts, at = [], 0
    for count in counts:
        parts.append(refs[at : at + count])
        at += count
    return (*parts, refs[at:])


def inner_planes(ref):
    return range(1, ref.shape[1] - 1)


def outer_planes(ref):
    return (0, ref.shape[1] - 1)


def inner_operator_kernel(ny_r, nz_r, v_ref, shift_ref, own_ref, *refs):
    y_in, z_in, (out_ref, ends_ref) = split(refs, ny_r, nz_r)
    near, base = operator_on_ends(v_ref.shape[1], own_ref[0], z_in)
    ends_ref[0] = near
    ends_ref[1] = base
    apply_operator(inner_planes(v_ref), v_ref, shift_ref, (), y_in, near, out_ref)


def outer_operator_kernel(nx_r, ny_r, v_ref, shift_ref, inner_ref, ends_ref, *refs):
    x_in, y_in, (out_ref,), x_out, y_out = split(refs, nx_r, ny_r, 1, nx_r)
    width, nx, ny, _ = v_ref.shape
    near = ends_ref[0]
    apply_operator(outer_planes(v_ref), v_ref, shift_ref, x_in, y_in, near, out_ref)
    for k, ref in enumerate(x_out):
        ref[:width] = out_ref[:, x_plane(k, nx)]
        ref[width] = near
    write_y_faces(out_ref, [ref.at[:width] for ref in y_out])
    for k, ref in enumerate(y_out):
        high = jnp.logical_xor(parity("gy"), k == 0)
        line = jnp.where(high, near[ny - 1 : ny], near[0:1])
        for x in range(nx):
            ref[width, x] = line


def pairs_of(width):
    return [(i, j) for i in range(width) for j in range(i + 1)]


def moment_sums(first, last, step, a_ref, b_ref, sums):
    width, _, ny, _ = a_ref.shape
    pairs = pairs_of(width)

    def plane(k, sums):
        sums, x = list(sums), first + k * step
        for y in range(0, ny, 8):
            a = [a_ref[f, x, y : y + 8, :] for f in range(width)]
            b = a if b_ref is a_ref else [b_ref[f, x, y : y + 8, :] for f in range(width)]
            for k, (i, j) in enumerate(pairs):
                sums[k] = sums[k] + a[i] * b[j]
        return tuple(sums)

    return lax.fori_loop(0, -((first - last) // step), plane, tuple(sums))


def no_sums(width):
    return [jnp.zeros((8, LANES), F32) for _ in pairs_of(width)]


def put_moment(width, sums, at, payload):
    rows = {}
    for (i, j), value in zip(pairs_of(width), sums):
        rows[i, j] = rows[j, i] = jnp.sum(value, axis=0, keepdims=True)
    lane = lax.broadcasted_iota(jnp.int32, (8, LANES), 1)
    for i in range(width):
        column = jnp.sum(jnp.concatenate([rows[i, j] for j in range(width)], axis=0), axis=1, keepdims=True)
        payload = jnp.where(lane == at + i, column, payload)
    return payload


def early_moments_kernel(b_ref, u_ref, out_ref):
    width, nx = b_ref.shape[:2]
    payload = jnp.zeros((8, LANES), F32)
    for k, (left, right) in enumerate(((b_ref, b_ref), (b_ref, u_ref), (u_ref, u_ref))):
        payload = put_moment(width, moment_sums(0, nx, 1, left, right, no_sums(width)), k * width, payload)
    out_ref[...] = payload


def inner_late_kernel(ny_r, u_ref, shift_ref, ends_ref, *refs):
    y_in, (sums_ref, t_ref) = split(refs, ny_r)
    width, nx = u_ref.shape[:2]
    ends = finished_ends(nx, ends_ref[1], (), y_in, width)
    apply_operator(inner_planes(u_ref), u_ref, shift_ref, (), y_in, ends, t_ref)
    for h, left in enumerate((u_ref, t_ref)):
        for k, value in enumerate(moment_sums(1, nx - 1, 1, left, t_ref, no_sums(width))):
            sums_ref[h, k] = value


def outer_late_kernel(nx_r, ny_r, u_ref, shift_ref, ends_ref, sums_ref, early_ref, *refs):
    x_in, y_in, (out_ref, t_ref) = split(refs, nx_r, ny_r)
    width, nx = u_ref.shape[:2]
    ends = finished_ends(nx, ends_ref[1], x_in, y_in, width)
    apply_operator(outer_planes(u_ref), u_ref, shift_ref, x_in, y_in, ends, t_ref)
    payload = early_ref[...]
    for h, left in enumerate((u_ref, t_ref)):
        inner = [sums_ref[h, k] for k in range(len(pairs_of(width)))]
        payload = put_moment(width, moment_sums(0, nx, nx - 1, left, t_ref, inner), (3 + h) * width, payload)
    out_ref[...] = jnp.broadcast_to(payload[None], out_ref.shape)


def lanes_of(matrix, j):
    return jnp.broadcast_to(matrix[:, j : j + 1], matrix.shape)


def rows_of(matrix, i):
    return jnp.broadcast_to(matrix[i : i + 1, :], matrix.shape)


def times(left, at, right):
    count = left.shape[0]
    total = lanes_of(left, at) * rows_of(right, 0)
    for k in range(1, count):
        total = total + lanes_of(left, at + k) * rows_of(right, k)
    return total


def shift_lanes(matrix, by):
    return pltpu.roll(matrix, by % LANES, 1)


def solve(columns, right):
    size = right[0].shape[0]
    sub = lax.broadcasted_iota(jnp.int32, right[0].shape, 0)
    for j in range(0, len(columns), 2):
        own, local = divmod(j, size)
        first, second = columns[j], columns[j + 1]
        a, b = rows_of(first[own], local), rows_of(second[own], local)
        c, d = rows_of(first[own], local + 1), rows_of(second[own], local + 1)
        scale = 1.0 / (a * d - b * c)
        a, b, c, d = a * scale, b * scale, c * scale, d * scale

        def step(value):
            upper, lower = rows_of(value[own], local), rows_of(value[own], local + 1)
            upper, lower = d * upper - b * lower, a * lower - c * upper
            value = [v - (f * upper + s * lower) for v, f, s in zip(value, first, second)]
            value[own] = jnp.where(sub == local, upper, jnp.where(sub == local + 1, lower, value[own]))
            return value

        columns = columns[: j + 2] + [step(column) for column in columns[j + 2 :]]
        right = step(right)
    return right


def small_algebra(s):
    n = s.shape[0]
    c0 = CENTRE
    lane = lax.broadcasted_iota(jnp.int32, s.shape, 1)
    sub = lax.broadcasted_iota(jnp.int32, s.shape, 0)
    n0, n1, n2, n3, n4 = shift_lanes(s, n), s, shift_lanes(s, -n), shift_lanes(s, -2 * n), shift_lanes(s, -3 * n)
    (e,) = solve([[lanes_of(s, j)] for j in range(n)], [s])
    p1 = times(s, n, e)
    p2 = times(s, 2 * n, e)
    p3 = times(s, 3 * n, e)
    cc = times(e, n, e)
    e2c = times(e, 2 * n, e)
    e2 = shift_lanes(e, -n)
    g = n2 - p1
    q = e2 - cc
    n3c = n3 - p2
    f3 = n3c - times(s, n, q)
    f4 = n4 - p3 - times(s, n, shift_lanes(e, -2 * n) - e2c)
    m11 = n2 + 2.0 * c0 * n1 + c0 * c0 * n0
    m12 = n3c + 2.0 * c0 * g
    m21 = n3 - times(s, n, e2) + 2.0 * c0 * g
    m22 = f4 + 2.0 * c0 * f3 + c0 * c0 * g
    columns = [[lanes_of(m11, n + j), lanes_of(m21, n + j)] for j in range(n)]
    columns += [[lanes_of(m12, n + j), lanes_of(m22, n + j)] for j in range(n)]
    pa, qa = solve(columns, [n1 + c0 * n0, g])
    on_b = pa - times(e, n, qa)
    unit = jnp.where(lane == sub + n, 1.0, 0.0)
    part = unit - times(e, n, pa) - c0 * pa - times(q, n, qa)
    squares = part * times(s, 0, part)
    pq = pa + c0 * qa
    squares = squares + pq * (times(g, n, pq) + 2.0 * times(f3, n, qa))
    squares = squares + qa * times(f4 - times(g, n, q), n, qa)
    return on_b, qa, jnp.sum(squares, axis=0, keepdims=True)


def finish_kernel(parts_ref, b_ref, u_ref, out_ref, norms_ref, coeff_ref):
    width, nx, ny, _ = b_ref.shape
    n = width
    total = jnp.sum(parts_ref[...], axis=0)
    on_b, on_u, squares = small_algebra(total)
    norms_ref[...] = jnp.sqrt(shift_lanes(squares, -n))[:, :n]
    for f in range(width):
        coeff_ref[0, f] = lanes_of(on_b, n + f)
        coeff_ref[1, f] = lanes_of(on_u, n + f)
    group = 2

    def fields(k, carry):
        first = [[[rows_of(coeff_ref[h, group * k + d], g) for g in range(width)] for h in range(2)] for d in range(group)]

        def plane(x, carry):
            for y in range(0, ny, 8):
                b = [b_ref[g, x, y : y + 8, :] for g in range(width)]
                u = [u_ref[g, x, y : y + 8, :] for g in range(width)]
                for d in range(group):
                    total = first[d][0][0] * b[0] + first[d][1][0] * u[0]
                    for g in range(1, width):
                        total = total + (first[d][0][g] * b[g] + first[d][1][g] * u[g])
                    out_ref[group * k + d, x, y : y + 8, :] = total
            return carry

        return lax.fori_loop(0, nx, plane, carry)

    lax.fori_loop(0, width // group, fields, 0)


def call(kernel, out_shape, operands, scratch=(), flops=1_000_000, name=None, aliases=None, far=False):
    return pl.pallas_call(
        kernel,
        out_shape=out_shape,
        in_specs=[pl.BlockSpec(memory_space=pl.ANY if far else pltpu.VMEM)] * len(operands),
        out_specs=jax.tree.map(lambda _: pl.BlockSpec(memory_space=pltpu.VMEM), out_shape),
        scratch_shapes=list(scratch),
        input_output_aliases=aliases or {},
        compiler_params=pltpu.CompilerParams(vmem_limit_bytes=8 << 20),
        cost_estimate=pl.CostEstimate(flops=flops, bytes_accessed=1 << 20, transcendentals=0),
        name=name,
    )(*operands)


def trade(turn, axis, faces):
    out = []
    for k, (face, pairs) in enumerate(zip(faces, swap_pairs(lax.axis_size(axis)))):
        with jax.named_scope(f"turn{turn}_{axis}_{k}"):
            out.append(swap(face, axis, pairs))
    return out


def body(right_side, shift):
    width, nx, ny, nz = right_side.shape
    assert width == 8 and nz == LANES and ny % 8 == 0 and nx > 2 and width * nx <= LANES // 2
    nx_r, ny_r, nz_r = rounds_of()
    devices = 1
    for axis in AXES:
        devices *= lax.axis_size(axis)
    assert nz_r > 0
    block = jax.ShapeDtypeStruct(right_side.shape, F32)
    full = pltpu.VMEM(right_side.shape, F32)
    kernel = functools.partial

    def x_faces(fields):
        return [jax.ShapeDtypeStruct((fields, ny, nz), F32)] * nx_r

    def y_faces(fields):
        return [jax.ShapeDtypeStruct((fields, nx, 1, nz), F32)] * ny_r

    def ends_of(layers):
        return jax.ShapeDtypeStruct((layers, ny, LANES), F32)

    faces = call(cut_x_kernel, x_faces(width), [right_side], scratch=[pltpu.SemaphoreType.DMA((max(nx_r, 1),))], name="cut", far=True)
    halo_x = trade(1, "gx", faces)
    *faces, own = call(pack_kernel, [*y_faces(width), ends_of(3)], [right_side, shift], name="pack")
    halo_y = trade(1, "gy", faces)
    halo_z = trade(1, "gz", [own] * nz_r)
    inner, ends = call(
        kernel(inner_operator_kernel, ny_r, nz_r),
        [block, ends_of(2)],
        [right_side, shift, own, *halo_y, *halo_z],
        flops=20_000_000,
        name="inner1",
    )
    u, *faces = call(
        kernel(outer_operator_kernel, nx_r, ny_r),
        [block, *x_faces(width + 1), *y_faces(width + 1)],
        [right_side, shift, inner, ends, *halo_x, *halo_y],
        aliases={2: 0},
        name="outer1",
    )
    halo_x = trade(2, "gx", faces[:nx_r])
    halo_y = trade(2, "gy", faces[nx_r:])
    early = call(early_moments_kernel, jax.ShapeDtypeStruct((8, LANES), F32), [right_side, u], flops=15_000_000, name="early")
    sums = call(
        kernel(inner_late_kernel, ny_r),
        jax.ShapeDtypeStruct((2, len(pairs_of(width)), 8, LANES), F32),
        [u, shift, ends, *halo_y],
        scratch=[full],
        flops=15_000_000,
        name="inner2",
    )
    copies = call(
        kernel(outer_late_kernel, nx_r, ny_r),
        jax.ShapeDtypeStruct((devices, 8, LANES), F32),
        [u, shift, ends, sums, early, *halo_x, *halo_y],
        scratch=[full],
        name="outer2",
    )
    parts = lax.all_to_all(copies, AXES, 0, 0, tiled=True)
    out, norms = call(
        finish_kernel,
        [block, jax.ShapeDtypeStruct((1, width), F32)],
        [parts, right_side, u],
        scratch=[pltpu.VMEM((2, width, 8, LANES), F32)],
        name="finish",
    )
    return out, norms.reshape(width)


def solution(mesh):
    in_specs = (P(None, "gx", "gy", "gz"), P("gx", "gy", "gz"))
    out_specs = (P(None, "gx", "gy", "gz"), P())
    return jax.shard_map(body, mesh=mesh, in_specs=in_specs, out_specs=out_specs, check_vma=False)
```

```python
import functools

import jax
import jax.numpy as jnp
from jax import lax
from jax.experimental import pallas as pl
from jax.experimental.pallas import tpu as pltpu
from jax.sharding import PartitionSpec as P

AXES = ("gx", "gy", "gz")
CENTRE = 7.0
LANES = 128
F32 = jnp.float32


def swap_pairs(count):
    first = [(i, j) for a in range(0, count - 1, 2) for i, j in ((a, a + 1), (a + 1, a))]
    second = [(i, j) for a in range(1, count - 1, 2) for i, j in ((a, a + 1), (a + 1, a))]
    return [pairs for pairs in (first, second) if pairs]


def swap(values, axis, pairs):
    side = lax.axis_size("gy")
    if axis == "gy" or side % 2:
        return lax.ppermute(values, axis, pairs)
    count = lax.axis_size(axis)
    named = {i for i, _ in pairs}
    at = (lambda i, y: i * side + y) if axis == "gx" else (lambda i, y: y * count + i)
    joint = [(at(i, y), at(j, y)) for i, j in pairs for y in range(side)]
    joint += [(at(i, y), at(i, y ^ 1)) for i in range(count) if i not in named for y in range(side)]
    return lax.ppermute(values, ("gx", "gy") if axis == "gx" else ("gy", "gz"), joint)


def rounds_of():
    return tuple(len(swap_pairs(lax.axis_size(axis))) for axis in AXES)


def parity(axis):
    return lax.rem(lax.axis_index(axis), 2) == 1


def x_plane(k, nx):
    return jnp.where(jnp.logical_xor(parity("gx"), k == 0), nx - 1, 0)


def cut_x_kernel(v_ref, *refs):
    faces, sems = refs[:-1], refs[-1]
    copies = [
        pltpu.make_async_copy(v_ref.at[:, x_plane(k, v_ref.shape[1])], ref, sems.at[k]) for k, ref in enumerate(faces)
    ]
    for copy in copies:
        copy.start()
    for copy in copies:
        copy.wait()


def write_y_faces(v_ref, y_refs):
    ny = v_ref.shape[2]
    odd = parity("gy")
    for k, ref in enumerate(y_refs):
        high = jnp.logical_xor(odd, k == 0)
        ref[...] = jnp.where(high, v_ref[:, :, ny - 1 : ny, :], v_ref[:, :, 0:1, :])


def packed_ends(tile, m, lane, near, far=None):
    def at(offset):
        return lane == lax.rem(2 * m + offset + LANES, LANES)

    turned = pltpu.roll(tile, 2 * m, 1)
    near = jnp.where(at(0) | at(-1), turned, near)
    if far is None:
        return near
    return near, jnp.where(at(1) | at(-2), turned, far)


def pack_kernel(v_ref, shift_ref, *refs):
    width, nx, ny, _ = v_ref.shape
    write_y_faces(v_ref, refs[:-1])
    lane = lax.broadcasted_iota(jnp.int32, (ny, LANES), 1)
    nothing = jnp.zeros((ny, LANES), F32)

    def field(f, packed):
        for x in range(nx):
            packed = packed_ends(v_ref[f, x], f * nx + x, lane, *packed)
        return packed

    near, far = lax.fori_loop(0, width, field, (nothing, nothing), unroll=width)
    diagonal = nothing
    for x in range(nx):
        diagonal = packed_ends((6.0 - CENTRE) + shift_ref[x], x, lane, diagonal)
    copies = 1
    while copies < width:
        diagonal = diagonal + pltpu.roll(diagonal, 2 * nx * copies, 1)
        copies *= 2
    refs[-1][0] = near
    refs[-1][1] = far
    refs[-1][2] = diagonal


def pick(axis, refs, load):
    if not refs:
        return 0.0, 0.0
    odd, at = parity(axis), lax.axis_index(axis)
    first = load(refs[0])
    second = load(refs[1]) if len(refs) > 1 else jnp.zeros_like(first)
    low = jnp.where(at == 0, 0.0, jnp.where(odd, first, second))
    high = jnp.where(at == lax.axis_size(axis) - 1, 0.0, jnp.where(odd, second, first))
    return low, high


def halo_ends(z_in, layer):
    low, high = pick("gz", z_in, lambda ref: ref[layer])
    if not z_in:
        return None
    lane = lax.broadcasted_iota(jnp.int32, low.shape, 1)
    by = 2 if layer == 1 else 1
    return jnp.where(lax.rem(lane, 2) == 0, pltpu.roll(low, by, 1), pltpu.roll(high, LANES - by, 1))


def inside_grid(lane):
    low = jnp.where(lax.axis_index("gz") == 0, 0.0, 1.0)
    high = jnp.where(lax.axis_index("gz") == lax.axis_size("gz") - 1, 0.0, 1.0)
    return jnp.where(lax.rem(lane, 2) == 0, low, high)


def lane_x(lane, nx):
    return lax.rem((lane + 1) // 2, nx)


def operator_on_ends(nx, own, z_in):
    near, far, diagonal = (halo_ends(z_in, layer) for layer in range(3))
    ny = near.shape[0]
    lane = lax.broadcasted_iota(jnp.int32, near.shape, 1)
    row = lax.broadcasted_iota(jnp.int32, near.shape, 0)
    x = lane_x(lane, nx)
    beside = own + far
    beside += jnp.where(x == 0, 0.0, pltpu.roll(near, 2, 1)) + jnp.where(x == nx - 1, 0.0, pltpu.roll(near, LANES - 2, 1))
    beside += jnp.where(row == 0, 0.0, pltpu.roll(near, 1, 0)) + jnp.where(row == ny - 1, 0.0, pltpu.roll(near, ny - 1, 0))
    return near, inside_grid(lane) * (diagonal * near - beside)


def finished_ends(nx, base, x_in, y_in, width):
    ny = base.shape[0]
    lane = lax.broadcasted_iota(jnp.int32, base.shape, 1)
    row = lax.broadcasted_iota(jnp.int32, base.shape, 0)
    low_y, high_y = pick("gy", y_in, lambda ref: ref[width, 0])
    beside = jnp.where(row == 0, low_y, 0.0) + jnp.where(row == ny - 1, high_y, 0.0)
    if x_in:
        x, by = lane_x(lane, nx), 2 * (nx - 1)
        low_x, high_x = pick("gx", x_in, lambda ref: ref[width])
        beside += jnp.where(x == 0, pltpu.roll(low_x, LANES - by, 1), 0.0)
        beside += jnp.where(x == nx - 1, pltpu.roll(high_x, by, 1), 0.0)
    return base - inside_grid(lane) * beside


def apply_operator(planes, v_ref, shift_ref, x_in, y_in, ends, out_ref):
    width, nx, ny, _ = v_ref.shape
    lane = lax.broadcasted_iota(jnp.int32, (ny, LANES), 1)
    row = lax.broadcasted_iota(jnp.int32, (ny, LANES), 0)
    def field(f, carry):
        low_x, high_x = pick("gx", x_in, lambda ref: ref[f])
        for x in planes:
            low_y, high_y = pick("gy", y_in, lambda ref: ref[f, x])
            v = v_ref[f, x]
            end = pltpu.roll(ends, lax.rem(LANES - 2 * (f * nx + x), LANES), 1)
            beside = (v_ref[f, x - 1] if x > 0 else low_x) + (v_ref[f, x + 1] if x < nx - 1 else high_x)
            beside += jnp.where(row == 0, low_y, pltpu.roll(v, 1, 0))
            beside += jnp.where(row == ny - 1, high_y, pltpu.roll(v, ny - 1, 0))
            beside += jnp.where(lane == 0, end, pltpu.roll(v, 1, 1))
            beside += jnp.where(lane == LANES - 1, end, pltpu.roll(v, LANES - 1, 1))
            out_ref[f, x] = ((6.0 - CENTRE) + shift_ref[x]) * v - beside
        return carry

    lax.fori_loop(0, width, field, 0, unroll=width)


def split(refs, *counts):
    parts, at = [], 0
    for count in counts:
        parts.append(refs[at : at + count])
        at += count
    return (*parts, refs[at:])


def inner_planes(ref):
    return range(1, ref.shape[1] - 1)


def outer_planes(ref):
    return (0, ref.shape[1] - 1)


def inner_operator_kernel(ny_r, nz_r, v_ref, shift_ref, own_ref, *refs):
    y_in, z_in, (out_ref, ends_ref) = split(refs, ny_r, nz_r)
    near, base = operator_on_ends(v_ref.shape[1], own_ref[0], z_in)
    ends_ref[0] = near
    ends_ref[1] = base
    apply_operator(inner_planes(v_ref), v_ref, shift_ref, (), y_in, near, out_ref)


def outer_operator_kernel(nx_r, ny_r, v_ref, shift_ref, inner_ref, ends_ref, *refs):
    x_in, y_in, (out_ref,), x_out, y_out = split(refs, nx_r, ny_r, 1, nx_r)
    width, nx, ny, _ = v_ref.shape
    near = ends_ref[0]
    apply_operator(outer_planes(v_ref), v_ref, shift_ref, x_in, y_in, near, out_ref)
    for k, ref in enumerate(x_out):
        ref[:width] = out_ref[:, x_plane(k, nx)]
        ref[width] = near
    write_y_faces(out_ref, [ref.at[:width] for ref in y_out])
    for k, ref in enumerate(y_out):
        high = jnp.logical_xor(parity("gy"), k == 0)
        line = jnp.where(high, near[ny - 1 : ny], near[0:1])
        for x in range(nx):
            ref[width, x] = line


def pairs_of(width):
    return [(i, j) for i in range(width) for j in range(i + 1)]


def moment_sums(first, last, step, a_ref, b_ref, sums):
    width, _, ny, _ = a_ref.shape
    pairs = pairs_of(width)

    def plane(k, sums):
        sums, x = list(sums), first + k * step
        for y in range(0, ny, 8):
            a = [a_ref[f, x, y : y + 8, :] for f in range(width)]
            b = a if b_ref is a_ref else [b_ref[f, x, y : y + 8, :] for f in range(width)]
            for k, (i, j) in enumerate(pairs):
                sums[k] = sums[k] + a[i] * b[j]
        return tuple(sums)

    return lax.fori_loop(0, -((first - last) // step), plane, tuple(sums))


def no_sums(width):
    return [jnp.zeros((8, LANES), F32) for _ in pairs_of(width)]


def put_moment(width, sums, at, payload):
    rows = {}
    for (i, j), value in zip(pairs_of(width), sums):
        rows[i, j] = rows[j, i] = jnp.sum(value, axis=0, keepdims=True)
    lane = lax.broadcasted_iota(jnp.int32, (8, LANES), 1)
    for i in range(width):
        column = jnp.sum(jnp.concatenate([rows[i, j] for j in range(width)], axis=0), axis=1, keepdims=True)
        payload = jnp.where(lane == at + i, column, payload)
    return payload


def early_moments_kernel(b_ref, u_ref, out_ref):
    width, nx = b_ref.shape[:2]
    payload = jnp.zeros((8, LANES), F32)
    for k, (left, right) in enumerate(((b_ref, b_ref), (b_ref, u_ref), (u_ref, u_ref))):
        payload = put_moment(width, moment_sums(0, nx, 1, left, right, no_sums(width)), k * width, payload)
    out_ref[...] = payload


def inner_late_kernel(ny_r, u_ref, shift_ref, ends_ref, *refs):
    y_in, (sums_ref, t_ref) = split(refs, ny_r)
    width, nx = u_ref.shape[:2]
    ends = finished_ends(nx, ends_ref[1], (), y_in, width)
    apply_operator(inner_planes(u_ref), u_ref, shift_ref, (), y_in, ends, t_ref)
    for h, left in enumerate((u_ref, t_ref)):
        for k, value in enumerate(moment_sums(1, nx - 1, 1, left, t_ref, no_sums(width))):
            sums_ref[h, k] = value


def outer_late_kernel(nx_r, ny_r, u_ref, shift_ref, ends_ref, sums_ref, early_ref, *refs):
    x_in, y_in, (out_ref, t_ref) = split(refs, nx_r, ny_r)
    width, nx = u_ref.shape[:2]
    ends = finished_ends(nx, ends_ref[1], x_in, y_in, width)
    apply_operator(outer_planes(u_ref), u_ref, shift_ref, x_in, y_in, ends, t_ref)
    payload = early_ref[...]
    for h, left in enumerate((u_ref, t_ref)):
        inner = [sums_ref[h, k] for k in range(len(pairs_of(width)))]
        payload = put_moment(width, moment_sums(0, nx, nx - 1, left, t_ref, inner), (3 + h) * width, payload)
    folded = payload[:4] + shift_lanes(payload, LANES // 2)[4:]
    out_ref[...] = jnp.broadcast_to(folded[None], out_ref.shape)


def lanes_of(matrix, j):
    return jnp.broadcast_to(matrix[:, j : j + 1], matrix.shape)


def rows_of(matrix, i):
    return jnp.broadcast_to(matrix[i : i + 1, :], matrix.shape)


def times(left, at, right):
    count = left.shape[0]
    total = lanes_of(left, at) * rows_of(right, 0)
    for k in range(1, count):
        total = total + lanes_of(left, at + k) * rows_of(right, k)
    return total


def shift_lanes(matrix, by):
    return pltpu.roll(matrix, by % LANES, 1)


def solve(columns, right):
    size = right[0].shape[0]
    sub = lax.broadcasted_iota(jnp.int32, right[0].shape, 0)
    for j in range(0, len(columns), 2):
        own, local = divmod(j, size)
        first, second = columns[j], columns[j + 1]
        a, b = rows_of(first[own], local), rows_of(second[own], local)
        c, d = rows_of(first[own], local + 1), rows_of(second[own], local + 1)
        scale = 1.0 / (a * d - b * c)
        a, b, c, d = a * scale, b * scale, c * scale, d * scale

        def step(value):
            upper, lower = rows_of(value[own], local), rows_of(value[own], local + 1)
            upper, lower = d * upper - b * lower, a * lower - c * upper
            value = [v - (f * upper + s * lower) for v, f, s in zip(value, first, second)]
            value[own] = jnp.where(sub == local, upper, jnp.where(sub == local + 1, lower, value[own]))
            return value

        columns = columns[: j + 2] + [step(column) for column in columns[j + 2 :]]
        right = step(right)
    return right


def small_algebra(s):
    n = s.shape[0]
    c0 = CENTRE
    lane = lax.broadcasted_iota(jnp.int32, s.shape, 1)
    sub = lax.broadcasted_iota(jnp.int32, s.shape, 0)
    n0, n1, n2, n3, n4 = shift_lanes(s, n), s, shift_lanes(s, -n), shift_lanes(s, -2 * n), shift_lanes(s, -3 * n)
    (e,) = solve([[lanes_of(s, j)] for j in range(n)], [s])
    p1 = times(s, n, e)
    p2 = times(s, 2 * n, e)
    p3 = times(s, 3 * n, e)
    cc = times(e, n, e)
    e2c = times(e, 2 * n, e)
    e2 = shift_lanes(e, -n)
    g = n2 - p1
    q = e2 - cc
    n3c = n3 - p2
    f3 = n3c - times(s, n, q)
    f4 = n4 - p3 - times(s, n, shift_lanes(e, -2 * n) - e2c)
    m11 = n2 + 2.0 * c0 * n1 + c0 * c0 * n0
    m12 = n3c + 2.0 * c0 * g
    m21 = n3 - times(s, n, e2) + 2.0 * c0 * g
    m22 = f4 + 2.0 * c0 * f3 + c0 * c0 * g
    columns = [[lanes_of(m11, n + j), lanes_of(m21, n + j)] for j in range(n)]
    columns += [[lanes_of(m12, n + j), lanes_of(m22, n + j)] for j in range(n)]
    pa, qa = solve(columns, [n1 + c0 * n0, g])
    on_b = pa - times(e, n, qa)
    unit = jnp.where(lane == sub + n, 1.0, 0.0)
    part = unit - times(e, n, pa) - c0 * pa - times(q, n, qa)
    squares = part * times(s, 0, part)
    pq = pa + c0 * qa
    squares = squares + pq * (times(g, n, pq) + 2.0 * times(f3, n, qa))
    squares = squares + qa * times(f4 - times(g, n, q), n, qa)
    return on_b, qa, jnp.sum(squares, axis=0, keepdims=True)


def finish_kernel(parts_ref, b_ref, u_ref, out_ref, norms_ref, coeff_ref):
    width, nx, ny, _ = b_ref.shape
    n = width
    folded = jnp.sum(parts_ref[...], axis=0)
    total = jnp.concatenate([folded, shift_lanes(folded, LANES // 2)], axis=0)
    on_b, on_u, squares = small_algebra(total)
    norms_ref[...] = jnp.sqrt(shift_lanes(squares, -n))[:, :n]
    for f in range(width):
        coeff_ref[0, f] = lanes_of(on_b, n + f)
        coeff_ref[1, f] = lanes_of(on_u, n + f)
    group = 2

    def fields(k, carry):
        first = [[[rows_of(coeff_ref[h, group * k + d], g) for g in range(width)] for h in range(2)] for d in range(group)]

        def plane(x, carry):
            for y in range(0, ny, 8):
                b = [b_ref[g, x, y : y + 8, :] for g in range(width)]
                u = [u_ref[g, x, y : y + 8, :] for g in range(width)]
                for d in range(group):
                    total = first[d][0][0] * b[0] + first[d][1][0] * u[0]
                    for g in range(1, width):
                        total = total + (first[d][0][g] * b[g] + first[d][1][g] * u[g])
                    out_ref[group * k + d, x, y : y + 8, :] = total
            return carry

        return lax.fori_loop(0, nx, plane, carry, unroll=nx)

    lax.fori_loop(0, width // group, fields, 0)


def call(kernel, out_shape, operands, scratch=(), flops=1_000_000, name=None, aliases=None, far=False):
    return pl.pallas_call(
        kernel,
        out_shape=out_shape,
        in_specs=[pl.BlockSpec(memory_space=pl.ANY if far else pltpu.VMEM)] * len(operands),
        out_specs=jax.tree.map(lambda _: pl.BlockSpec(memory_space=pltpu.VMEM), out_shape),
        scratch_shapes=list(scratch),
        input_output_aliases=aliases or {},
        compiler_params=pltpu.CompilerParams(vmem_limit_bytes=8 << 20),
        cost_estimate=pl.CostEstimate(flops=flops, bytes_accessed=1 << 20, transcendentals=0),
        name=name,
    )(*operands)


def trade(turn, axis, faces):
    out = []
    for k, (face, pairs) in enumerate(zip(faces, swap_pairs(lax.axis_size(axis)))):
        with jax.named_scope(f"turn{turn}_{axis}_{k}"):
            out.append(swap(face, axis, pairs))
    return out


def body(right_side, shift):
    width, nx, ny, nz = right_side.shape
    assert width == 8 and nz == LANES and ny % 8 == 0 and nx > 2 and width * nx <= LANES // 2
    nx_r, ny_r, nz_r = rounds_of()
    devices = 1
    for axis in AXES:
        devices *= lax.axis_size(axis)
    assert nz_r > 0
    block = jax.ShapeDtypeStruct(right_side.shape, F32)
    full = pltpu.VMEM(right_side.shape, F32)
    kernel = functools.partial

    def x_faces(fields):
        return [jax.ShapeDtypeStruct((fields, ny, nz), F32)] * nx_r

    def y_faces(fields):
        return [jax.ShapeDtypeStruct((fields, nx, 1, nz), F32)] * ny_r

    def ends_of(layers):
        return jax.ShapeDtypeStruct((layers, ny, LANES), F32)

    faces = call(cut_x_kernel, x_faces(width), [right_side], scratch=[pltpu.SemaphoreType.DMA((max(nx_r, 1),))], name="cut", far=True)
    halo_x = trade(1, "gx", faces)
    *faces, own = call(pack_kernel, [*y_faces(width), ends_of(3)], [right_side, shift], name="pack")
    halo_y = trade(1, "gy", faces)
    halo_z = trade(1, "gz", [own] * nz_r)
    inner, ends = call(
        kernel(inner_operator_kernel, ny_r, nz_r),
        [block, ends_of(2)],
        [right_side, shift, own, *halo_y, *halo_z],
        flops=20_000_000,
        name="inner1",
    )
    u, *faces = call(
        kernel(outer_operator_kernel, nx_r, ny_r),
        [block, *x_faces(width + 1), *y_faces(width + 1)],
        [right_side, shift, inner, ends, *halo_x, *halo_y],
        aliases={2: 0},
        name="outer1",
    )
    halo_x = trade(2, "gx", faces[:nx_r])
    halo_y = trade(2, "gy", faces[nx_r:])
    early = call(early_moments_kernel, jax.ShapeDtypeStruct((8, LANES), F32), [right_side, u], flops=15_000_000, name="early")
    sums = call(
        kernel(inner_late_kernel, ny_r),
        jax.ShapeDtypeStruct((2, len(pairs_of(width)), 8, LANES), F32),
        [u, shift, ends, *halo_y],
        scratch=[full],
        flops=15_000_000,
        name="inner2",
    )
    copies = call(
        kernel(outer_late_kernel, nx_r, ny_r),
        jax.ShapeDtypeStruct((devices, 4, LANES), F32),
        [u, shift, ends, sums, early, *halo_x, *halo_y],
        scratch=[full],
        name="outer2",
    )
    parts = lax.all_to_all(copies, AXES, 0, 0, tiled=True)
    out, norms = call(
        finish_kernel,
        [block, jax.ShapeDtypeStruct((1, width), F32)],
        [parts, right_side, u],
        scratch=[pltpu.VMEM((2, width, 8, LANES), F32)],
        name="finish",
    )
    return out, norms.reshape(width)


def solution(mesh):
    in_specs = (P(None, "gx", "gy", "gz"), P("gx", "gy", "gz"))
    out_specs = (P(None, "gx", "gy", "gz"), P())
    return jax.shard_map(body, mesh=mesh, in_specs=in_specs, out_specs=out_specs, check_vma=False)
```

```python
import functools

import jax
import jax.numpy as jnp
from jax import lax
from jax.experimental import pallas as pl
from jax.experimental.pallas import tpu as pltpu
from jax.sharding import PartitionSpec as P

AXES = ("gx", "gy", "gz")
CENTRE = 7.0
LANES = 128
F32 = jnp.float32


def swap_pairs(count):
    first = [(i, j) for a in range(0, count - 1, 2) for i, j in ((a, a + 1), (a + 1, a))]
    second = [(i, j) for a in range(1, count - 1, 2) for i, j in ((a, a + 1), (a + 1, a))]
    return [pairs for pairs in (first, second) if pairs]


def swap(values, axis, pairs):
    side = lax.axis_size("gy")
    if axis == "gy" or side % 2:
        return lax.ppermute(values, axis, pairs)
    count = lax.axis_size(axis)
    named = {i for i, _ in pairs}
    at = (lambda i, y: i * side + y) if axis == "gx" else (lambda i, y: y * count + i)
    joint = [(at(i, y), at(j, y)) for i, j in pairs for y in range(side)]
    joint += [(at(i, y), at(i, y ^ 1)) for i in range(count) if i not in named for y in range(side)]
    return lax.ppermute(values, ("gx", "gy") if axis == "gx" else ("gy", "gz"), joint)


def rounds_of():
    return tuple(len(swap_pairs(lax.axis_size(axis))) for axis in AXES)


def parity(axis):
    return lax.rem(lax.axis_index(axis), 2) == 1


def x_plane(k, nx):
    return jnp.where(jnp.logical_xor(parity("gx"), k == 0), nx - 1, 0)


def cut_x_kernel(v_ref, *refs):
    for k, ref in enumerate(refs):
        ref[...] = v_ref[:, x_plane(k, v_ref.shape[1])].reshape(ref.shape)


def write_y_faces(v_ref, y_refs):
    ny = v_ref.shape[2]
    odd = parity("gy")
    for k, ref in enumerate(y_refs):
        high = jnp.logical_xor(odd, k == 0)
        ref[...] = jnp.where(high, v_ref[:, :, ny - 1 : ny, :], v_ref[:, :, 0:1, :])


def packed_ends(tile, m, lane, near, far=None):
    def at(offset):
        return lane == lax.rem(2 * m + offset + LANES, LANES)

    turned = pltpu.roll(tile, 2 * m, 1)
    near = jnp.where(at(0) | at(-1), turned, near)
    if far is None:
        return near
    return near, jnp.where(at(1) | at(-2), turned, far)


def pack_kernel(v_ref, shift_ref, *refs):
    width, nx, ny, _ = v_ref.shape
    write_y_faces(v_ref, refs[:-1])
    lane = lax.broadcasted_iota(jnp.int32, (ny, LANES), 1)
    nothing = jnp.zeros((ny, LANES), F32)

    def field(f, packed):
        for x in range(nx):
            packed = packed_ends(v_ref[f, x], f * nx + x, lane, *packed)
        return packed

    near, far = lax.fori_loop(0, width, field, (nothing, nothing), unroll=width)
    diagonal = nothing
    for x in range(nx):
        diagonal = packed_ends((6.0 - CENTRE) + shift_ref[x], x, lane, diagonal)
    copies = 1
    while copies < width:
        diagonal = diagonal + pltpu.roll(diagonal, 2 * nx * copies, 1)
        copies *= 2
    refs[-1][0] = near
    refs[-1][1] = far
    refs[-1][2] = diagonal


def pick(axis, refs, load):
    if not refs:
        return 0.0, 0.0
    odd, at = parity(axis), lax.axis_index(axis)
    first = load(refs[0])
    second = load(refs[1]) if len(refs) > 1 else jnp.zeros_like(first)
    low = jnp.where(at == 0, 0.0, jnp.where(odd, first, second))
    high = jnp.where(at == lax.axis_size(axis) - 1, 0.0, jnp.where(odd, second, first))
    return low, high


def halo_ends(z_in, layer):
    low, high = pick("gz", z_in, lambda ref: ref[layer])
    if not z_in:
        return None
    lane = lax.broadcasted_iota(jnp.int32, low.shape, 1)
    by = 2 if layer == 1 else 1
    return jnp.where(lax.rem(lane, 2) == 0, pltpu.roll(low, by, 1), pltpu.roll(high, LANES - by, 1))


def inside_grid(lane):
    low = jnp.where(lax.axis_index("gz") == 0, 0.0, 1.0)
    high = jnp.where(lax.axis_index("gz") == lax.axis_size("gz") - 1, 0.0, 1.0)
    return jnp.where(lax.rem(lane, 2) == 0, low, high)


def lane_x(lane, nx):
    return lax.rem((lane + 1) // 2, nx)


def fold_plane(ends, x, nx):
    ny = ends.shape[0]
    lane = lax.broadcasted_iota(jnp.int32, (8, LANES), 1)
    mine = lane_x(lane, nx) == x
    groups = [jnp.where(mine, ends[8 * r : 8 * r + 8], 0.0) for r in range(ny // 8)]
    return sum(pltpu.roll(group, lax.rem(LANES + 2 * r - 2 * x, LANES), 1) for r, group in enumerate(groups))


def unfold_plane(folded, x, ny):
    return jnp.concatenate([shift_lanes(folded, 2 * x - 2 * r) for r in range(ny // 8)], axis=0)


def operator_on_ends(nx, own, z_in):
    near, far, diagonal = (halo_ends(z_in, layer) for layer in range(3))
    ny = near.shape[0]
    lane = lax.broadcasted_iota(jnp.int32, near.shape, 1)
    row = lax.broadcasted_iota(jnp.int32, near.shape, 0)
    x = lane_x(lane, nx)
    beside = own + far
    beside += jnp.where(x == 0, 0.0, pltpu.roll(near, 2, 1)) + jnp.where(x == nx - 1, 0.0, pltpu.roll(near, LANES - 2, 1))
    beside += jnp.where(row == 0, 0.0, pltpu.roll(near, 1, 0)) + jnp.where(row == ny - 1, 0.0, pltpu.roll(near, ny - 1, 0))
    return near, inside_grid(lane) * (diagonal * near - beside)


def finished_ends(nx, base, x_in, y_in, width):
    ny = base.shape[0]
    lane = lax.broadcasted_iota(jnp.int32, base.shape, 1)
    row = lax.broadcasted_iota(jnp.int32, base.shape, 0)
    low_y, high_y = pick("gy", y_in, lambda ref: ref[width, 0])
    beside = jnp.where(row == 0, low_y, 0.0) + jnp.where(row == ny - 1, high_y, 0.0)
    if x_in:
        x = lane_x(lane, nx)
        low_x, high_x = pick("gx", x_in, lambda ref: ref[ref.shape[0] - 1])
        beside += jnp.where(x == 0, unfold_plane(low_x, 0, ny), 0.0)
        beside += jnp.where(x == nx - 1, unfold_plane(high_x, nx - 1, ny), 0.0)
    return base - inside_grid(lane) * beside


def face_of(ref, f, ny):
    groups = ny // 8
    return ref[pl.ds(f * groups, groups)].reshape(ny, LANES)


def apply_operator(planes, v_ref, shift_ref, x_in, y_in, ends, out_ref):
    width, nx, ny, _ = v_ref.shape
    lane = lax.broadcasted_iota(jnp.int32, (ny, LANES), 1)
    row = lax.broadcasted_iota(jnp.int32, (ny, LANES), 0)
    def field(f, carry):
        low_x, high_x = pick("gx", x_in, lambda ref: face_of(ref, f, ny))
        for x in planes:
            low_y, high_y = pick("gy", y_in, lambda ref: ref[f, x])
            v = v_ref[f, x]
            end = pltpu.roll(ends, lax.rem(LANES - 2 * (f * nx + x), LANES), 1)
            beside = (v_ref[f, x - 1] if x > 0 else low_x) + (v_ref[f, x + 1] if x < nx - 1 else high_x)
            beside += jnp.where(row == 0, low_y, pltpu.roll(v, 1, 0))
            beside += jnp.where(row == ny - 1, high_y, pltpu.roll(v, ny - 1, 0))
            beside += jnp.where(lane == 0, end, pltpu.roll(v, 1, 1))
            beside += jnp.where(lane == LANES - 1, end, pltpu.roll(v, LANES - 1, 1))
            out_ref[f, x] = ((6.0 - CENTRE) + shift_ref[x]) * v - beside
        return carry

    lax.fori_loop(0, width, field, 0, unroll=width)


def split(refs, *counts):
    parts, at = [], 0
    for count in counts:
        parts.append(refs[at : at + count])
        at += count
    return (*parts, refs[at:])


def inner_planes(ref):
    return range(1, ref.shape[1] - 1)


def outer_planes(ref):
    return (0, ref.shape[1] - 1)


def inner_operator_kernel(ny_r, nz_r, v_ref, shift_ref, own_ref, *refs):
    y_in, z_in, (out_ref, ends_ref) = split(refs, ny_r, nz_r)
    near, base = operator_on_ends(v_ref.shape[1], own_ref[0], z_in)
    ends_ref[0] = near
    ends_ref[1] = base
    apply_operator(inner_planes(v_ref), v_ref, shift_ref, (), y_in, near, out_ref)


def outer_operator_kernel(nx_r, ny_r, v_ref, shift_ref, inner_ref, ends_ref, *refs):
    x_in, y_in, (out_ref,), x_out, y_out = split(refs, nx_r, ny_r, 1, nx_r)
    width, nx, ny, _ = v_ref.shape
    near = ends_ref[0]
    apply_operator(outer_planes(v_ref), v_ref, shift_ref, x_in, y_in, near, out_ref)
    for k, ref in enumerate(x_out):
        plane, rows = x_plane(k, nx), width * ny // 8
        ref[:rows] = out_ref[:, plane].reshape(rows, 8, LANES)
        ref[rows] = fold_plane(near, plane, nx)
    write_y_faces(out_ref, [ref.at[:width] for ref in y_out])
    for k, ref in enumerate(y_out):
        high = jnp.logical_xor(parity("gy"), k == 0)
        line = jnp.where(high, near[ny - 1 : ny], near[0:1])
        for x in range(nx):
            ref[width, x] = line


def pairs_of(width):
    return [(i, j) for i in range(width) for j in range(i + 1)]


def moment_sums(first, last, step, a_ref, b_ref, sums):
    width, _, ny, _ = a_ref.shape
    pairs = pairs_of(width)

    def plane(k, sums):
        sums, x = list(sums), first + k * step
        for y in range(0, ny, 8):
            a = [a_ref[f, x, y : y + 8, :] for f in range(width)]
            b = a if b_ref is a_ref else [b_ref[f, x, y : y + 8, :] for f in range(width)]
            for k, (i, j) in enumerate(pairs):
                sums[k] = sums[k] + a[i] * b[j]
        return tuple(sums)

    return lax.fori_loop(0, -((first - last) // step), plane, tuple(sums))


def no_sums(width):
    return [jnp.zeros((8, LANES), F32) for _ in pairs_of(width)]


def put_moment(width, sums, at, payload):
    rows = {}
    for (i, j), value in zip(pairs_of(width), sums):
        rows[i, j] = rows[j, i] = jnp.sum(value, axis=0, keepdims=True)
    lane = lax.broadcasted_iota(jnp.int32, (8, LANES), 1)
    for i in range(width):
        column = jnp.sum(jnp.concatenate([rows[i, j] for j in range(width)], axis=0), axis=1, keepdims=True)
        payload = jnp.where(lane == at + i, column, payload)
    return payload


def early_moments_kernel(b_ref, u_ref, out_ref):
    width, nx = b_ref.shape[:2]
    payload = jnp.zeros((8, LANES), F32)
    for k, (left, right) in enumerate(((b_ref, b_ref), (b_ref, u_ref), (u_ref, u_ref))):
        payload = put_moment(width, moment_sums(0, nx, 1, left, right, no_sums(width)), k * width, payload)
    out_ref[...] = payload


def inner_late_kernel(ny_r, u_ref, shift_ref, ends_ref, *refs):
    y_in, (sums_ref, t_ref) = split(refs, ny_r)
    width, nx = u_ref.shape[:2]
    ends = finished_ends(nx, ends_ref[1], (), y_in, width)
    apply_operator(inner_planes(u_ref), u_ref, shift_ref, (), y_in, ends, t_ref)
    for h, left in enumerate((u_ref, t_ref)):
        for k, value in enumerate(moment_sums(1, nx - 1, 1, left, t_ref, no_sums(width))):
            sums_ref[h, k] = value


def outer_late_kernel(nx_r, ny_r, u_ref, shift_ref, ends_ref, sums_ref, early_ref, *refs):
    x_in, y_in, (out_ref, t_ref) = split(refs, nx_r, ny_r)
    width, nx = u_ref.shape[:2]
    ends = finished_ends(nx, ends_ref[1], x_in, y_in, width)
    apply_operator(outer_planes(u_ref), u_ref, shift_ref, x_in, y_in, ends, t_ref)
    payload = early_ref[...]
    for h, left in enumerate((u_ref, t_ref)):
        inner = [sums_ref[h, k] for k in range(len(pairs_of(width)))]
        payload = put_moment(width, moment_sums(0, nx, nx - 1, left, t_ref, inner), (3 + h) * width, payload)
    folded = payload[:4] + shift_lanes(payload, LANES // 2)[4:]
    out_ref[...] = jnp.broadcast_to(folded[None], out_ref.shape)


def lanes_of(matrix, j):
    return jnp.broadcast_to(matrix[:, j : j + 1], matrix.shape)


def rows_of(matrix, i):
    return jnp.broadcast_to(matrix[i : i + 1, :], matrix.shape)


def times(left, at, right):
    count = left.shape[0]
    total = lanes_of(left, at) * rows_of(right, 0)
    for k in range(1, count):
        total = total + lanes_of(left, at + k) * rows_of(right, k)
    return total


def shift_lanes(matrix, by):
    return pltpu.roll(matrix, by % LANES, 1)


def solve(columns, right):
    size = right[0].shape[0]
    sub = lax.broadcasted_iota(jnp.int32, right[0].shape, 0)
    for j in range(0, len(columns), 2):
        own, local = divmod(j, size)
        first, second = columns[j], columns[j + 1]
        a, b = rows_of(first[own], local), rows_of(second[own], local)
        c, d = rows_of(first[own], local + 1), rows_of(second[own], local + 1)
        scale = 1.0 / (a * d - b * c)
        a, b, c, d = a * scale, b * scale, c * scale, d * scale

        def step(value):
            upper, lower = rows_of(value[own], local), rows_of(value[own], local + 1)
            upper, lower = d * upper - b * lower, a * lower - c * upper
            value = [v - (f * upper + s * lower) for v, f, s in zip(value, first, second)]
            value[own] = jnp.where(sub == local, upper, jnp.where(sub == local + 1, lower, value[own]))
            return value

        columns = columns[: j + 2] + [step(column) for column in columns[j + 2 :]]
        right = step(right)
    return right


def small_algebra(s):
    n = s.shape[0]
    c0 = CENTRE
    lane = lax.broadcasted_iota(jnp.int32, s.shape, 1)
    sub = lax.broadcasted_iota(jnp.int32, s.shape, 0)
    n0, n1, n2, n3, n4 = shift_lanes(s, n), s, shift_lanes(s, -n), shift_lanes(s, -2 * n), shift_lanes(s, -3 * n)
    (e,) = solve([[lanes_of(s, j)] for j in range(n)], [s])
    p1 = times(s, n, e)
    p2 = times(s, 2 * n, e)
    p3 = times(s, 3 * n, e)
    cc = times(e, n, e)
    e2c = times(e, 2 * n, e)
    e2 = shift_lanes(e, -n)
    g = n2 - p1
    q = e2 - cc
    n3c = n3 - p2
    f3 = n3c - times(s, n, q)
    f4 = n4 - p3 - times(s, n, shift_lanes(e, -2 * n) - e2c)
    m11 = n2 + 2.0 * c0 * n1 + c0 * c0 * n0
    m12 = n3c + 2.0 * c0 * g
    m21 = n3 - times(s, n, e2) + 2.0 * c0 * g
    m22 = f4 + 2.0 * c0 * f3 + c0 * c0 * g
    columns = [[lanes_of(m11, n + j), lanes_of(m21, n + j)] for j in range(n)]
    columns += [[lanes_of(m12, n + j), lanes_of(m22, n + j)] for j in range(n)]
    pa, qa = solve(columns, [n1 + c0 * n0, g])
    on_b = pa - times(e, n, qa)
    unit = jnp.where(lane == sub + n, 1.0, 0.0)
    part = unit - times(e, n, pa) - c0 * pa - times(q, n, qa)
    squares = part * times(s, 0, part)
    pq = pa + c0 * qa
    squares = squares + pq * (times(g, n, pq) + 2.0 * times(f3, n, qa))
    squares = squares + qa * times(f4 - times(g, n, q), n, qa)
    return on_b, qa, jnp.sum(squares, axis=0, keepdims=True)


def finish_kernel(parts_ref, b_ref, u_ref, out_ref, norms_ref, coeff_ref):
    width, nx, ny, _ = b_ref.shape
    n = width
    folded = jnp.sum(parts_ref[...], axis=0)
    total = jnp.concatenate([folded, shift_lanes(folded, LANES // 2)], axis=0)
    on_b, on_u, squares = small_algebra(total)
    norms_ref[...] = jnp.sqrt(shift_lanes(squares, -n))[:, :n]
    for f in range(width):
        coeff_ref[0, f] = lanes_of(on_b, n + f)
        coeff_ref[1, f] = lanes_of(on_u, n + f)
    group = 2

    def fields(k, carry):
        first = [[[rows_of(coeff_ref[h, group * k + d], g) for g in range(width)] for h in range(2)] for d in range(group)]

        def plane(x, carry):
            for y in range(0, ny, 8):
                b = [b_ref[g, x, y : y + 8, :] for g in range(width)]
                u = [u_ref[g, x, y : y + 8, :] for g in range(width)]
                for d in range(group):
                    total = first[d][0][0] * b[0] + first[d][1][0] * u[0]
                    for g in range(1, width):
                        total = total + (first[d][0][g] * b[g] + first[d][1][g] * u[g])
                    out_ref[group * k + d, x, y : y + 8, :] = total
            return carry

        return lax.fori_loop(0, nx, plane, carry, unroll=nx)

    lax.fori_loop(0, width // group, fields, 0)


def call(kernel, out_shape, operands, scratch=(), flops=1_000_000, name=None, aliases=None):
    return pl.pallas_call(
        kernel,
        out_shape=out_shape,
        in_specs=[pl.BlockSpec(memory_space=pltpu.VMEM)] * len(operands),
        out_specs=jax.tree.map(lambda _: pl.BlockSpec(memory_space=pltpu.VMEM), out_shape),
        scratch_shapes=list(scratch),
        input_output_aliases=aliases or {},
        compiler_params=pltpu.CompilerParams(vmem_limit_bytes=8 << 20),
        cost_estimate=pl.CostEstimate(flops=flops, bytes_accessed=1 << 20, transcendentals=0),
        name=name,
    )(*operands)


def trade(turn, axis, faces):
    out = []
    for k, (face, pairs) in enumerate(zip(faces, swap_pairs(lax.axis_size(axis)))):
        with jax.named_scope(f"turn{turn}_{axis}_{k}"):
            out.append(swap(face, axis, pairs))
    return out


def body(right_side, shift):
    width, nx, ny, nz = right_side.shape
    assert width == 8 and nz == LANES and ny % 8 == 0 and nx > 2 and width * nx <= LANES // 2 and ny <= 8 * nx
    nx_r, ny_r, nz_r = rounds_of()
    devices = 1
    for axis in AXES:
        devices *= lax.axis_size(axis)
    assert nz_r > 0
    block = jax.ShapeDtypeStruct(right_side.shape, F32)
    full = pltpu.VMEM(right_side.shape, F32)
    kernel = functools.partial

    def x_faces(extra):
        return [jax.ShapeDtypeStruct((width * ny // 8 + extra, 8, nz), F32)] * nx_r

    def y_faces(fields):
        return [jax.ShapeDtypeStruct((fields, nx, 1, nz), F32)] * ny_r

    def ends_of(layers):
        return jax.ShapeDtypeStruct((layers, ny, LANES), F32)

    faces = call(cut_x_kernel, x_faces(0), [right_side], name="cut")
    halo_x = trade(1, "gx", faces)
    *faces, own = call(pack_kernel, [*y_faces(width), ends_of(3)], [right_side, shift], name="pack")
    halo_y = trade(1, "gy", faces)
    halo_z = trade(1, "gz", [own] * nz_r)
    inner, ends = call(
        kernel(inner_operator_kernel, ny_r, nz_r),
        [block, ends_of(2)],
        [right_side, shift, own, *halo_y, *halo_z],
        flops=20_000_000,
        name="inner1",
    )
    u, *faces = call(
        kernel(outer_operator_kernel, nx_r, ny_r),
        [block, *x_faces(1), *y_faces(width + 1)],
        [right_side, shift, inner, ends, *halo_x, *halo_y],
        aliases={2: 0},
        name="outer1",
    )
    halo_x = trade(2, "gx", faces[:nx_r])
    halo_y = trade(2, "gy", faces[nx_r:])
    early = call(early_moments_kernel, jax.ShapeDtypeStruct((8, LANES), F32), [right_side, u], flops=15_000_000, name="early")
    sums = call(
        kernel(inner_late_kernel, ny_r),
        jax.ShapeDtypeStruct((2, len(pairs_of(width)), 8, LANES), F32),
        [u, shift, ends, *halo_y],
        scratch=[full],
        flops=15_000_000,
        name="inner2",
    )
    copies = call(
        kernel(outer_late_kernel, nx_r, ny_r),
        jax.ShapeDtypeStruct((devices, 4, LANES), F32),
        [u, shift, ends, sums, early, *halo_x, *halo_y],
        scratch=[full],
        name="outer2",
    )
    parts = lax.all_to_all(copies, AXES, 0, 0, tiled=True)
    out, norms = call(
        finish_kernel,
        [block, jax.ShapeDtypeStruct((1, width), F32)],
        [parts, right_side, u],
        scratch=[pltpu.VMEM((2, width, 8, LANES), F32)],
        name="finish",
    )
    return out, norms.reshape(width)


def solution(mesh):
    in_specs = (P(None, "gx", "gy", "gz"), P("gx", "gy", "gz"))
    out_specs = (P(None, "gx", "gy", "gz"), P())
    return jax.shard_map(body, mesh=mesh, in_specs=in_specs, out_specs=out_specs, check_vma=False)
```

```python
import functools

import jax
import jax.numpy as jnp
from jax import lax
from jax.experimental import pallas as pl
from jax.experimental.pallas import tpu as pltpu
from jax.sharding import PartitionSpec as P

AXES = ("gx", "gy", "gz")
CENTRE = 7.0
LANES = 128
F32 = jnp.float32


def swap_pairs(count):
    first = [(i, j) for a in range(0, count - 1, 2) for i, j in ((a, a + 1), (a + 1, a))]
    second = [(i, j) for a in range(1, count - 1, 2) for i, j in ((a, a + 1), (a + 1, a))]
    return [pairs for pairs in (first, second) if pairs]


def swap(values, axis, pairs):
    side = lax.axis_size("gy")
    if axis == "gy" or side % 2:
        return lax.ppermute(values, axis, pairs)
    count = lax.axis_size(axis)
    named = {i for i, _ in pairs}
    at = (lambda i, y: i * side + y) if axis == "gx" else (lambda i, y: y * count + i)
    joint = [(at(i, y), at(j, y)) for i, j in pairs for y in range(side)]
    joint += [(at(i, y), at(i, y ^ 1)) for i in range(count) if i not in named for y in range(side)]
    return lax.ppermute(values, ("gx", "gy") if axis == "gx" else ("gy", "gz"), joint)


def rounds_of():
    return tuple(len(swap_pairs(lax.axis_size(axis))) for axis in AXES)


def parity(axis):
    return lax.rem(lax.axis_index(axis), 2) == 1


def x_plane(k, nx):
    return jnp.where(jnp.logical_xor(parity("gx"), k == 0), nx - 1, 0)


def cut_x_kernel(v_ref, *refs):
    for k, ref in enumerate(refs):
        ref[...] = v_ref[:, x_plane(k, v_ref.shape[1])].reshape(ref.shape)


def write_y_faces(v_ref, y_refs):
    ny = v_ref.shape[2]
    odd = parity("gy")
    for k, ref in enumerate(y_refs):
        high = jnp.logical_xor(odd, k == 0)
        ref[...] = jnp.where(high, v_ref[:, :, ny - 1 : ny, :], v_ref[:, :, 0:1, :])


def packed_ends(tile, m, lane, near, far=None):
    def at(offset):
        return lane == lax.rem(2 * m + offset + LANES, LANES)

    turned = pltpu.roll(tile, 2 * m, 1)
    near = jnp.where(at(0) | at(-1), turned, near)
    if far is None:
        return near
    return near, jnp.where(at(1) | at(-2), turned, far)


def pack_kernel(ny_r, v_ref, shift_ref, *refs):
    width, nx, ny, _ = v_ref.shape
    y_refs, (near_ref, *z_refs) = refs[:ny_r], refs[ny_r:]
    write_y_faces(v_ref, y_refs)
    lane = lax.broadcasted_iota(jnp.int32, (ny, LANES), 1)
    nothing = jnp.zeros((ny, LANES), F32)

    def field(f, packed):
        for x in range(nx):
            packed = packed_ends(v_ref[f, x], f * nx + x, lane, *packed)
        return packed

    near, far = lax.fori_loop(0, width, field, (nothing, nothing), unroll=width)
    diagonal = nothing
    for x in range(nx):
        diagonal = packed_ends((6.0 - CENTRE) + shift_ref[x], x, lane, diagonal)
    groups = ny // 8
    folded = sum(shift_lanes(diagonal[8 * r : 8 * r + 8], 2 * nx * r) for r in range(groups))
    near_ref[...] = near
    for k, ref in enumerate(z_refs):
        first = jnp.where(jnp.logical_xor(parity("gz"), k == 0), 1, 0)
        ref[:groups] = jnp.where(lax.rem(lane, 2) == first, near, far).reshape(groups, 8, LANES)
        ref[groups] = folded


def pick(axis, refs, load):
    if not refs:
        return 0.0, 0.0
    odd, at = parity(axis), lax.axis_index(axis)
    first = load(refs[0])
    second = load(refs[1]) if len(refs) > 1 else jnp.zeros_like(first)
    low = jnp.where(at == 0, 0.0, jnp.where(odd, first, second))
    high = jnp.where(at == lax.axis_size(axis) - 1, 0.0, jnp.where(odd, second, first))
    return low, high


def by_side(low, high, by):
    lane = lax.broadcasted_iota(jnp.int32, low.shape, 1)
    return jnp.where(lax.rem(lane, 2) == 0, shift_lanes(low, by), shift_lanes(high, -by))


def halo_ends(z_in, nx, width):
    groups = z_in[0].shape[0] - 1
    low, high = pick("gz", z_in, lambda ref: ref[:groups].reshape(8 * groups, LANES))
    folded = by_side(*pick("gz", z_in, lambda ref: ref[groups]), 1)
    lane = lax.broadcasted_iota(jnp.int32, folded.shape, 1)
    mine = lax.rem(lane + 1, LANES) < 2 * nx
    rows = [jnp.where(mine, shift_lanes(folded, -2 * nx * r), 0.0) for r in range(groups)]
    diagonal, copies = jnp.concatenate(rows, axis=0), 1
    while copies < width:
        diagonal = diagonal + shift_lanes(diagonal, 2 * nx * copies)
        copies *= 2
    return by_side(low, high, 1), by_side(low, high, 2), diagonal


def inside_grid(lane):
    low = jnp.where(lax.axis_index("gz") == 0, 0.0, 1.0)
    high = jnp.where(lax.axis_index("gz") == lax.axis_size("gz") - 1, 0.0, 1.0)
    return jnp.where(lax.rem(lane, 2) == 0, low, high)


def lane_x(lane, nx):
    return lax.rem((lane + 1) // 2, nx)


def fold_plane(ends, x, nx):
    ny = ends.shape[0]
    lane = lax.broadcasted_iota(jnp.int32, (8, LANES), 1)
    mine = lane_x(lane, nx) == x
    groups = [jnp.where(mine, ends[8 * r : 8 * r + 8], 0.0) for r in range(ny // 8)]
    return sum(pltpu.roll(group, lax.rem(LANES + 2 * r - 2 * x, LANES), 1) for r, group in enumerate(groups))


def unfold_plane(folded, x, ny):
    return jnp.concatenate([shift_lanes(folded, 2 * x - 2 * r) for r in range(ny // 8)], axis=0)


def operator_on_ends(nx, width, own, z_in):
    near, far, diagonal = halo_ends(z_in, nx, width)
    ny = near.shape[0]
    lane = lax.broadcasted_iota(jnp.int32, near.shape, 1)
    row = lax.broadcasted_iota(jnp.int32, near.shape, 0)
    x = lane_x(lane, nx)
    beside = own + far
    beside += jnp.where(x == 0, 0.0, pltpu.roll(near, 2, 1)) + jnp.where(x == nx - 1, 0.0, pltpu.roll(near, LANES - 2, 1))
    beside += jnp.where(row == 0, 0.0, pltpu.roll(near, 1, 0)) + jnp.where(row == ny - 1, 0.0, pltpu.roll(near, ny - 1, 0))
    return near, inside_grid(lane) * (diagonal * near - beside)


def finished_ends(nx, base, x_in, y_in, width):
    ny = base.shape[0]
    lane = lax.broadcasted_iota(jnp.int32, base.shape, 1)
    row = lax.broadcasted_iota(jnp.int32, base.shape, 0)
    low_y, high_y = pick("gy", y_in, lambda ref: ref[width, 0])
    beside = jnp.where(row == 0, low_y, 0.0) + jnp.where(row == ny - 1, high_y, 0.0)
    if x_in:
        x = lane_x(lane, nx)
        low_x, high_x = pick("gx", x_in, lambda ref: ref[ref.shape[0] - 1])
        beside += jnp.where(x == 0, unfold_plane(low_x, 0, ny), 0.0)
        beside += jnp.where(x == nx - 1, unfold_plane(high_x, nx - 1, ny), 0.0)
    return base - inside_grid(lane) * beside


def face_of(ref, f, ny):
    groups = ny // 8
    return ref[pl.ds(f * groups, groups)].reshape(ny, LANES)


def apply_operator(planes, v_ref, shift_ref, x_in, y_in, ends, out_ref):
    width, nx, ny, _ = v_ref.shape
    lane = lax.broadcasted_iota(jnp.int32, (ny, LANES), 1)
    row = lax.broadcasted_iota(jnp.int32, (ny, LANES), 0)
    def field(f, carry):
        low_x, high_x = pick("gx", x_in, lambda ref: face_of(ref, f, ny))
        for x in planes:
            low_y, high_y = pick("gy", y_in, lambda ref: ref[f, x])
            v = v_ref[f, x]
            end = pltpu.roll(ends, lax.rem(LANES - 2 * (f * nx + x), LANES), 1)
            beside = (v_ref[f, x - 1] if x > 0 else low_x) + (v_ref[f, x + 1] if x < nx - 1 else high_x)
            beside += jnp.where(row == 0, low_y, pltpu.roll(v, 1, 0))
            beside += jnp.where(row == ny - 1, high_y, pltpu.roll(v, ny - 1, 0))
            beside += jnp.where(lane == 0, end, pltpu.roll(v, 1, 1))
            beside += jnp.where(lane == LANES - 1, end, pltpu.roll(v, LANES - 1, 1))
            out_ref[f, x] = ((6.0 - CENTRE) + shift_ref[x]) * v - beside
        return carry

    lax.fori_loop(0, width, field, 0, unroll=width)


def split(refs, *counts):
    parts, at = [], 0
    for count in counts:
        parts.append(refs[at : at + count])
        at += count
    return (*parts, refs[at:])


def inner_planes(ref):
    return range(1, ref.shape[1] - 1)


def outer_planes(ref):
    return (0, ref.shape[1] - 1)


def inner_operator_kernel(ny_r, nz_r, v_ref, shift_ref, own_ref, *refs):
    y_in, z_in, (out_ref, ends_ref) = split(refs, ny_r, nz_r)
    near, base = operator_on_ends(v_ref.shape[1], v_ref.shape[0], own_ref[...], z_in)
    ends_ref[0] = near
    ends_ref[1] = base
    apply_operator(inner_planes(v_ref), v_ref, shift_ref, (), y_in, near, out_ref)


def outer_operator_kernel(nx_r, ny_r, v_ref, shift_ref, inner_ref, ends_ref, *refs):
    x_in, y_in, (out_ref,), x_out, y_out = split(refs, nx_r, ny_r, 1, nx_r)
    width, nx, ny, _ = v_ref.shape
    near = ends_ref[0]
    apply_operator(outer_planes(v_ref), v_ref, shift_ref, x_in, y_in, near, out_ref)
    for k, ref in enumerate(x_out):
        plane, rows = x_plane(k, nx), width * ny // 8
        ref[:rows] = out_ref[:, plane].reshape(rows, 8, LANES)
        ref[rows] = fold_plane(near, plane, nx)
    write_y_faces(out_ref, [ref.at[:width] for ref in y_out])
    for k, ref in enumerate(y_out):
        high = jnp.logical_xor(parity("gy"), k == 0)
        line = jnp.where(high, near[ny - 1 : ny], near[0:1])
        for x in range(nx):
            ref[width, x] = line


def pairs_of(width):
    return [(i, j) for i in range(width) for j in range(i + 1)]


def moment_sums(first, last, step, a_ref, b_ref, sums):
    width, _, ny, _ = a_ref.shape
    pairs = pairs_of(width)

    def plane(k, sums):
        sums, x = list(sums), first + k * step
        for y in range(0, ny, 8):
            a = [a_ref[f, x, y : y + 8, :] for f in range(width)]
            b = a if b_ref is a_ref else [b_ref[f, x, y : y + 8, :] for f in range(width)]
            for k, (i, j) in enumerate(pairs):
                sums[k] = sums[k] + a[i] * b[j]
        return tuple(sums)

    return lax.fori_loop(0, -((first - last) // step), plane, tuple(sums))


def no_sums(width):
    return [jnp.zeros((8, LANES), F32) for _ in pairs_of(width)]


def put_moment(width, sums, at, payload):
    rows = {}
    for (i, j), value in zip(pairs_of(width), sums):
        rows[i, j] = rows[j, i] = jnp.sum(value, axis=0, keepdims=True)
    lane = lax.broadcasted_iota(jnp.int32, (8, LANES), 1)
    for i in range(width):
        column = jnp.sum(jnp.concatenate([rows[i, j] for j in range(width)], axis=0), axis=1, keepdims=True)
        payload = jnp.where(lane == at + i, column, payload)
    return payload


def early_moments_kernel(b_ref, u_ref, out_ref):
    width, nx = b_ref.shape[:2]
    payload = jnp.zeros((8, LANES), F32)
    for k, (left, right) in enumerate(((b_ref, b_ref), (b_ref, u_ref), (u_ref, u_ref))):
        payload = put_moment(width, moment_sums(0, nx, 1, left, right, no_sums(width)), k * width, payload)
    out_ref[...] = payload


def inner_late_kernel(ny_r, u_ref, shift_ref, ends_ref, *refs):
    y_in, (sums_ref, t_ref) = split(refs, ny_r)
    width, nx = u_ref.shape[:2]
    ends = finished_ends(nx, ends_ref[1], (), y_in, width)
    apply_operator(inner_planes(u_ref), u_ref, shift_ref, (), y_in, ends, t_ref)
    for h, left in enumerate((u_ref, t_ref)):
        for k, value in enumerate(moment_sums(1, nx - 1, 1, left, t_ref, no_sums(width))):
            sums_ref[h, k] = value


def outer_late_kernel(nx_r, ny_r, u_ref, shift_ref, ends_ref, sums_ref, early_ref, *refs):
    x_in, y_in, (out_ref, t_ref) = split(refs, nx_r, ny_r)
    width, nx = u_ref.shape[:2]
    ends = finished_ends(nx, ends_ref[1], x_in, y_in, width)
    apply_operator(outer_planes(u_ref), u_ref, shift_ref, x_in, y_in, ends, t_ref)
    payload = early_ref[...]
    for h, left in enumerate((u_ref, t_ref)):
        inner = [sums_ref[h, k] for k in range(len(pairs_of(width)))]
        payload = put_moment(width, moment_sums(0, nx, nx - 1, left, t_ref, inner), (3 + h) * width, payload)
    folded = payload[:4] + shift_lanes(payload, LANES // 2)[4:]
    out_ref[...] = jnp.broadcast_to(folded[None], out_ref.shape)


def lanes_of(matrix, j):
    return jnp.broadcast_to(matrix[:, j : j + 1], matrix.shape)


def rows_of(matrix, i):
    return jnp.broadcast_to(matrix[i : i + 1, :], matrix.shape)


def times(left, at, right):
    count = left.shape[0]
    total = lanes_of(left, at) * rows_of(right, 0)
    for k in range(1, count):
        total = total + lanes_of(left, at + k) * rows_of(right, k)
    return total


def shift_lanes(matrix, by):
    return pltpu.roll(matrix, by % LANES, 1)


def solve(columns, right):
    size = right[0].shape[0]
    sub = lax.broadcasted_iota(jnp.int32, right[0].shape, 0)
    for j in range(0, len(columns), 2):
        own, local = divmod(j, size)
        first, second = columns[j], columns[j + 1]
        a, b = rows_of(first[own], local), rows_of(second[own], local)
        c, d = rows_of(first[own], local + 1), rows_of(second[own], local + 1)
        scale = 1.0 / (a * d - b * c)
        a, b, c, d = a * scale, b * scale, c * scale, d * scale

        def step(value):
            upper, lower = rows_of(value[own], local), rows_of(value[own], local + 1)
            upper, lower = d * upper - b * lower, a * lower - c * upper
            value = [v - (f * upper + s * lower) for v, f, s in zip(value, first, second)]
            value[own] = jnp.where(sub == local, upper, jnp.where(sub == local + 1, lower, value[own]))
            return value

        columns = columns[: j + 2] + [step(column) for column in columns[j + 2 :]]
        right = step(right)
    return right


def small_algebra(s):
    n = s.shape[0]
    c0 = CENTRE
    lane = lax.broadcasted_iota(jnp.int32, s.shape, 1)
    sub = lax.broadcasted_iota(jnp.int32, s.shape, 0)
    n0, n1, n2, n3, n4 = shift_lanes(s, n), s, shift_lanes(s, -n), shift_lanes(s, -2 * n), shift_lanes(s, -3 * n)
    (e,) = solve([[lanes_of(s, j)] for j in range(n)], [s])
    p1 = times(s, n, e)
    p2 = times(s, 2 * n, e)
    p3 = times(s, 3 * n, e)
    cc = times(e, n, e)
    e2c = times(e, 2 * n, e)
    e2 = shift_lanes(e, -n)
    g = n2 - p1
    q = e2 - cc
    n3c = n3 - p2
    f3 = n3c - times(s, n, q)
    f4 = n4 - p3 - times(s, n, shift_lanes(e, -2 * n) - e2c)
    m11 = n2 + 2.0 * c0 * n1 + c0 * c0 * n0
    m12 = n3c + 2.0 * c0 * g
    m21 = n3 - times(s, n, e2) + 2.0 * c0 * g
    m22 = f4 + 2.0 * c0 * f3 + c0 * c0 * g
    columns = [[lanes_of(m11, n + j), lanes_of(m21, n + j)] for j in range(n)]
    columns += [[lanes_of(m12, n + j), lanes_of(m22, n + j)] for j in range(n)]
    pa, qa = solve(columns, [n1 + c0 * n0, g])
    on_b = pa - times(e, n, qa)
    unit = jnp.where(lane == sub + n, 1.0, 0.0)
    part = unit - times(e, n, pa) - c0 * pa - times(q, n, qa)
    squares = part * times(s, 0, part)
    pq = pa + c0 * qa
    squares = squares + pq * (times(g, n, pq) + 2.0 * times(f3, n, qa))
    squares = squares + qa * times(f4 - times(g, n, q), n, qa)
    return on_b, qa, jnp.sum(squares, axis=0, keepdims=True)


def finish_kernel(parts_ref, b_ref, u_ref, out_ref, norms_ref, coeff_ref):
    width, nx, ny, _ = b_ref.shape
    n = width
    folded = jnp.sum(parts_ref[...], axis=0)
    total = jnp.concatenate([folded, shift_lanes(folded, LANES // 2)], axis=0)
    on_b, on_u, squares = small_algebra(total)
    norms_ref[...] = jnp.sqrt(shift_lanes(squares, -n))[:, :n]
    for f in range(width):
        coeff_ref[0, f] = lanes_of(on_b, n + f)
        coeff_ref[1, f] = lanes_of(on_u, n + f)
    group = 2

    def fields(k, carry):
        first = [[[rows_of(coeff_ref[h, group * k + d], g) for g in range(width)] for h in range(2)] for d in range(group)]

        def plane(x, carry):
            for y in range(0, ny, 8):
                b = [b_ref[g, x, y : y + 8, :] for g in range(width)]
                u = [u_ref[g, x, y : y + 8, :] for g in range(width)]
                for d in range(group):
                    total = first[d][0][0] * b[0] + first[d][1][0] * u[0]
                    for g in range(1, width):
                        total = total + (first[d][0][g] * b[g] + first[d][1][g] * u[g])
                    out_ref[group * k + d, x, y : y + 8, :] = total
            return carry

        return lax.fori_loop(0, nx, plane, carry, unroll=nx)

    lax.fori_loop(0, width // group, fields, 0)


def call(kernel, out_shape, operands, scratch=(), flops=1_000_000, name=None, aliases=None):
    return pl.pallas_call(
        kernel,
        out_shape=out_shape,
        in_specs=[pl.BlockSpec(memory_space=pltpu.VMEM)] * len(operands),
        out_specs=jax.tree.map(lambda _: pl.BlockSpec(memory_space=pltpu.VMEM), out_shape),
        scratch_shapes=list(scratch),
        input_output_aliases=aliases or {},
        compiler_params=pltpu.CompilerParams(vmem_limit_bytes=8 << 20),
        cost_estimate=pl.CostEstimate(flops=flops, bytes_accessed=1 << 20, transcendentals=0),
        name=name,
    )(*operands)


def trade(turn, axis, faces):
    out = []
    for k, (face, pairs) in enumerate(zip(faces, swap_pairs(lax.axis_size(axis)))):
        with jax.named_scope(f"turn{turn}_{axis}_{k}"):
            out.append(swap(face, axis, pairs))
    return out


def body(right_side, shift):
    width, nx, ny, nz = right_side.shape
    assert width == 8 and nz == LANES and ny % 8 == 0 and nx > 2 and width * nx <= LANES // 2 and ny <= 8 * nx and ny * nx <= 4 * LANES
    nx_r, ny_r, nz_r = rounds_of()
    devices = 1
    for axis in AXES:
        devices *= lax.axis_size(axis)
    assert nz_r > 0
    block = jax.ShapeDtypeStruct(right_side.shape, F32)
    full = pltpu.VMEM(right_side.shape, F32)
    kernel = functools.partial

    def x_faces(extra):
        return [jax.ShapeDtypeStruct((width * ny // 8 + extra, 8, nz), F32)] * nx_r

    def y_faces(fields):
        return [jax.ShapeDtypeStruct((fields, nx, 1, nz), F32)] * ny_r

    def ends_of(layers):
        return jax.ShapeDtypeStruct((layers, ny, LANES), F32)

    faces = call(cut_x_kernel, x_faces(0), [right_side], name="cut")
    halo_x = trade(1, "gx", faces)
    packed = call(
        kernel(pack_kernel, ny_r),
        [*y_faces(width), jax.ShapeDtypeStruct((ny, LANES), F32), *[jax.ShapeDtypeStruct((ny // 8 + 1, 8, LANES), F32)] * nz_r],
        [right_side, shift],
        name="pack",
    )
    halo_y, own = trade(1, "gy", packed[:ny_r]), packed[ny_r]
    halo_z = trade(1, "gz", packed[ny_r + 1 :])
    inner, ends = call(
        kernel(inner_operator_kernel, ny_r, nz_r),
        [block, ends_of(2)],
        [right_side, shift, own, *halo_y, *halo_z],
        flops=20_000_000,
        name="inner1",
    )
    u, *faces = call(
        kernel(outer_operator_kernel, nx_r, ny_r),
        [block, *x_faces(1), *y_faces(width + 1)],
        [right_side, shift, inner, ends, *halo_x, *halo_y],
        aliases={2: 0},
        name="outer1",
    )
    halo_x = trade(2, "gx", faces[:nx_r])
    halo_y = trade(2, "gy", faces[nx_r:])
    early = call(early_moments_kernel, jax.ShapeDtypeStruct((8, LANES), F32), [right_side, u], flops=15_000_000, name="early")
    sums = call(
        kernel(inner_late_kernel, ny_r),
        jax.ShapeDtypeStruct((2, len(pairs_of(width)), 8, LANES), F32),
        [u, shift, ends, *halo_y],
        scratch=[full],
        flops=15_000_000,
        name="inner2",
    )
    copies = call(
        kernel(outer_late_kernel, nx_r, ny_r),
        jax.ShapeDtypeStruct((devices, 4, LANES), F32),
        [u, shift, ends, sums, early, *halo_x, *halo_y],
        scratch=[full],
        name="outer2",
    )
    parts = lax.all_to_all(copies, AXES, 0, 0, tiled=True)
    out, norms = call(
        finish_kernel,
        [block, jax.ShapeDtypeStruct((1, width), F32)],
        [parts, right_side, u],
        scratch=[pltpu.VMEM((2, width, 8, LANES), F32)],
        name="finish",
    )
    return out, norms.reshape(width)


def solution(mesh):
    in_specs = (P(None, "gx", "gy", "gz"), P("gx", "gy", "gz"))
    out_specs = (P(None, "gx", "gy", "gz"), P())
    return jax.shard_map(body, mesh=mesh, in_specs=in_specs, out_specs=out_specs, check_vma=False)
```

```python
import functools

import jax
import jax.numpy as jnp
from jax import lax
from jax.experimental import pallas as pl
from jax.experimental.pallas import tpu as pltpu
from jax.sharding import PartitionSpec as P

AXES = ("gx", "gy", "gz")
CENTRE = 4.0
LANES = 128
F32 = jnp.float32


def swap_pairs(count):
    first = [(i, j) for a in range(0, count - 1, 2) for i, j in ((a, a + 1), (a + 1, a))]
    second = [(i, j) for a in range(1, count - 1, 2) for i, j in ((a, a + 1), (a + 1, a))]
    return [pairs for pairs in (first, second) if pairs]


def swap(values, axis, pairs):
    side = lax.axis_size("gy")
    if axis == "gy" or side % 2:
        return lax.ppermute(values, axis, pairs)
    count = lax.axis_size(axis)
    named = {i for i, _ in pairs}
    at = (lambda i, y: i * side + y) if axis == "gx" else (lambda i, y: y * count + i)
    joint = [(at(i, y), at(j, y)) for i, j in pairs for y in range(side)]
    joint += [(at(i, y), at(i, y ^ 1)) for i in range(count) if i not in named for y in range(side)]
    return lax.ppermute(values, ("gx", "gy") if axis == "gx" else ("gy", "gz"), joint)


def rounds_of():
    return tuple(len(swap_pairs(lax.axis_size(axis))) for axis in AXES)


def parity(axis):
    return lax.rem(lax.axis_index(axis), 2) == 1


def x_plane(k, nx):
    return jnp.where(jnp.logical_xor(parity("gx"), k == 0), nx - 1, 0)


def cut_x_kernel(v_ref, *refs):
    for k, ref in enumerate(refs):
        ref[...] = v_ref[:, x_plane(k, v_ref.shape[1])].reshape(ref.shape)


def write_y_faces(v_ref, y_refs):
    ny = v_ref.shape[2]
    odd = parity("gy")
    for k, ref in enumerate(y_refs):
        high = jnp.logical_xor(odd, k == 0)
        ref[...] = jnp.where(high, v_ref[:, :, ny - 1 : ny, :], v_ref[:, :, 0:1, :])


def packed_ends(tile, m, lane, near, far=None):
    def at(offset):
        return lane == lax.rem(2 * m + offset + LANES, LANES)

    turned = pltpu.roll(tile, 2 * m, 1)
    near = jnp.where(at(0) | at(-1), turned, near)
    if far is None:
        return near
    return near, jnp.where(at(1) | at(-2), turned, far)


def pack_kernel(ny_r, v_ref, shift_ref, *refs):
    width, nx, ny, _ = v_ref.shape
    y_refs, (near_ref, *z_refs) = refs[:ny_r], refs[ny_r:]
    write_y_faces(v_ref, y_refs)
    lane = lax.broadcasted_iota(jnp.int32, (ny, LANES), 1)
    nothing = jnp.zeros((ny, LANES), F32)

    def field(f, packed):
        for x in range(nx):
            packed = packed_ends(v_ref[f, x], f * nx + x, lane, *packed)
        return packed

    near, far = lax.fori_loop(0, width, field, (nothing, nothing), unroll=width)
    diagonal = nothing
    for x in range(nx):
        diagonal = packed_ends((6.0 - CENTRE) + shift_ref[x], x, lane, diagonal)
    groups = ny // 8
    folded = sum(shift_lanes(diagonal[8 * r : 8 * r + 8], 2 * nx * r) for r in range(groups))
    near_ref[...] = near
    for k, ref in enumerate(z_refs):
        first = jnp.where(jnp.logical_xor(parity("gz"), k == 0), 1, 0)
        ref[:groups] = jnp.where(lax.rem(lane, 2) == first, near, far).reshape(groups, 8, LANES)
        ref[groups] = folded


def pick(axis, refs, load):
    if not refs:
        return 0.0, 0.0
    odd, at = parity(axis), lax.axis_index(axis)
    first = load(refs[0])
    second = load(refs[1]) if len(refs) > 1 else jnp.zeros_like(first)
    low = jnp.where(at == 0, 0.0, jnp.where(odd, first, second))
    high = jnp.where(at == lax.axis_size(axis) - 1, 0.0, jnp.where(odd, second, first))
    return low, high


def by_side(low, high, by):
    lane = lax.broadcasted_iota(jnp.int32, low.shape, 1)
    return jnp.where(lax.rem(lane, 2) == 0, shift_lanes(low, by), shift_lanes(high, -by))


def halo_ends(z_in, nx, width):
    groups = z_in[0].shape[0] - 1
    low, high = pick("gz", z_in, lambda ref: ref[:groups].reshape(8 * groups, LANES))
    folded = by_side(*pick("gz", z_in, lambda ref: ref[groups]), 1)
    lane = lax.broadcasted_iota(jnp.int32, folded.shape, 1)
    mine = lax.rem(lane + 1, LANES) < 2 * nx
    rows = [jnp.where(mine, shift_lanes(folded, -2 * nx * r), 0.0) for r in range(groups)]
    diagonal, copies = jnp.concatenate(rows, axis=0), 1
    while copies < width:
        diagonal = diagonal + shift_lanes(diagonal, 2 * nx * copies)
        copies *= 2
    return by_side(low, high, 1), by_side(low, high, 2), diagonal


def inside_grid(lane):
    low = jnp.where(lax.axis_index("gz") == 0, 0.0, 1.0)
    high = jnp.where(lax.axis_index("gz") == lax.axis_size("gz") - 1, 0.0, 1.0)
    return jnp.where(lax.rem(lane, 2) == 0, low, high)


def lane_x(lane, nx):
    return lax.rem((lane + 1) // 2, nx)


def fold_plane(ends, x, nx):
    ny = ends.shape[0]
    lane = lax.broadcasted_iota(jnp.int32, (8, LANES), 1)
    mine = lane_x(lane, nx) == x
    groups = [jnp.where(mine, ends[8 * r : 8 * r + 8], 0.0) for r in range(ny // 8)]
    return sum(pltpu.roll(group, lax.rem(LANES + 2 * r - 2 * x, LANES), 1) for r, group in enumerate(groups))


def unfold_plane(folded, x, ny):
    return jnp.concatenate([shift_lanes(folded, 2 * x - 2 * r) for r in range(ny // 8)], axis=0)


def operator_on_ends(nx, width, own, z_in):
    near, far, diagonal = halo_ends(z_in, nx, width)
    ny = near.shape[0]
    lane = lax.broadcasted_iota(jnp.int32, near.shape, 1)
    row = lax.broadcasted_iota(jnp.int32, near.shape, 0)
    x = lane_x(lane, nx)
    beside = own + far
    beside += jnp.where(x == 0, 0.0, pltpu.roll(near, 2, 1)) + jnp.where(x == nx - 1, 0.0, pltpu.roll(near, LANES - 2, 1))
    beside += jnp.where(row == 0, 0.0, pltpu.roll(near, 1, 0)) + jnp.where(row == ny - 1, 0.0, pltpu.roll(near, ny - 1, 0))
    return near, inside_grid(lane) * (diagonal * near - beside)


def finished_ends(nx, base, x_in, y_in, width):
    ny = base.shape[0]
    lane = lax.broadcasted_iota(jnp.int32, base.shape, 1)
    row = lax.broadcasted_iota(jnp.int32, base.shape, 0)
    low_y, high_y = pick("gy", y_in, lambda ref: ref[width, 0])
    beside = jnp.where(row == 0, low_y, 0.0) + jnp.where(row == ny - 1, high_y, 0.0)
    if x_in:
        x = lane_x(lane, nx)
        low_x, high_x = pick("gx", x_in, lambda ref: ref[ref.shape[0] - 1])
        beside += jnp.where(x == 0, unfold_plane(low_x, 0, ny), 0.0)
        beside += jnp.where(x == nx - 1, unfold_plane(high_x, nx - 1, ny), 0.0)
    return base - inside_grid(lane) * beside


def face_of(ref, f, ny):
    groups = ny // 8
    return ref[pl.ds(f * groups, groups)].reshape(ny, LANES)


def apply_operator(planes, v_ref, shift_ref, x_in, y_in, ends, out_ref):
    width, nx, ny, _ = v_ref.shape
    lane = lax.broadcasted_iota(jnp.int32, (ny, LANES), 1)
    row = lax.broadcasted_iota(jnp.int32, (ny, LANES), 0)
    def field(f, carry):
        low_x, high_x = pick("gx", x_in, lambda ref: face_of(ref, f, ny))
        for x in planes:
            low_y, high_y = pick("gy", y_in, lambda ref: ref[f, x])
            v = v_ref[f, x]
            end = pltpu.roll(ends, lax.rem(LANES - 2 * (f * nx + x), LANES), 1)
            beside = (v_ref[f, x - 1] if x > 0 else low_x) + (v_ref[f, x + 1] if x < nx - 1 else high_x)
            beside += jnp.where(row == 0, low_y, pltpu.roll(v, 1, 0))
            beside += jnp.where(row == ny - 1, high_y, pltpu.roll(v, ny - 1, 0))
            beside += jnp.where(lane == 0, end, pltpu.roll(v, 1, 1))
            beside += jnp.where(lane == LANES - 1, end, pltpu.roll(v, LANES - 1, 1))
            out_ref[f, x] = ((6.0 - CENTRE) + shift_ref[x]) * v - beside
        return carry

    lax.fori_loop(0, width, field, 0, unroll=width)


def split(refs, *counts):
    parts, at = [], 0
    for count in counts:
        parts.append(refs[at : at + count])
        at += count
    return (*parts, refs[at:])


def inner_planes(ref):
    return range(1, ref.shape[1] - 1)


def outer_planes(ref):
    return (0, ref.shape[1] - 1)


def inner_operator_kernel(ny_r, nz_r, v_ref, shift_ref, own_ref, *refs):
    y_in, z_in, (out_ref, ends_ref) = split(refs, ny_r, nz_r)
    near, base = operator_on_ends(v_ref.shape[1], v_ref.shape[0], own_ref[...], z_in)
    ends_ref[0] = near
    ends_ref[1] = base
    apply_operator(inner_planes(v_ref), v_ref, shift_ref, (), y_in, near, out_ref)


def outer_operator_kernel(nx_r, ny_r, v_ref, shift_ref, inner_ref, ends_ref, *refs):
    x_in, y_in, (out_ref,), x_out, y_out = split(refs, nx_r, ny_r, 1, nx_r)
    width, nx, ny, _ = v_ref.shape
    near = ends_ref[0]
    apply_operator(outer_planes(v_ref), v_ref, shift_ref, x_in, y_in, near, out_ref)
    for k, ref in enumerate(x_out):
        plane, rows = x_plane(k, nx), width * ny // 8
        ref[:rows] = out_ref[:, plane].reshape(rows, 8, LANES)
        ref[rows] = fold_plane(near, plane, nx)
    write_y_faces(out_ref, [ref.at[:width] for ref in y_out])
    for k, ref in enumerate(y_out):
        high = jnp.logical_xor(parity("gy"), k == 0)
        line = jnp.where(high, near[ny - 1 : ny], near[0:1])
        for x in range(nx):
            ref[width, x] = line


def pairs_of(width):
    return [(i, j) for i in range(width) for j in range(i + 1)]


def moment_sums(first, last, step, a_ref, b_ref, sums):
    width, _, ny, _ = a_ref.shape
    pairs = pairs_of(width)

    def plane(k, sums):
        sums, x = list(sums), first + k * step
        for y in range(0, ny, 8):
            a = [a_ref[f, x, y : y + 8, :] for f in range(width)]
            b = a if b_ref is a_ref else [b_ref[f, x, y : y + 8, :] for f in range(width)]
            for k, (i, j) in enumerate(pairs):
                sums[k] = sums[k] + a[i] * b[j]
        return tuple(sums)

    return lax.fori_loop(0, -((first - last) // step), plane, tuple(sums))


def no_sums(width):
    return [jnp.zeros((8, LANES), F32) for _ in pairs_of(width)]


def put_moment(width, sums, at, payload):
    rows = {}
    for (i, j), value in zip(pairs_of(width), sums):
        rows[i, j] = rows[j, i] = jnp.sum(value, axis=0, keepdims=True)
    lane = lax.broadcasted_iota(jnp.int32, (8, LANES), 1)
    for i in range(width):
        column = jnp.sum(jnp.concatenate([rows[i, j] for j in range(width)], axis=0), axis=1, keepdims=True)
        payload = jnp.where(lane == at + i, column, payload)
    return payload


def early_moments_kernel(b_ref, u_ref, out_ref):
    width, nx = b_ref.shape[:2]
    payload = jnp.zeros((8, LANES), F32)
    for k, (left, right) in enumerate(((b_ref, b_ref), (b_ref, u_ref), (u_ref, u_ref))):
        payload = put_moment(width, moment_sums(0, nx, 1, left, right, no_sums(width)), k * width, payload)
    out_ref[...] = payload


def inner_late_kernel(ny_r, u_ref, shift_ref, ends_ref, *refs):
    y_in, (sums_ref, t_ref) = split(refs, ny_r)
    width, nx = u_ref.shape[:2]
    ends = finished_ends(nx, ends_ref[1], (), y_in, width)
    apply_operator(inner_planes(u_ref), u_ref, shift_ref, (), y_in, ends, t_ref)
    for h, left in enumerate((u_ref, t_ref)):
        for k, value in enumerate(moment_sums(1, nx - 1, 1, left, t_ref, no_sums(width))):
            sums_ref[h, k] = value


def outer_late_kernel(nx_r, ny_r, u_ref, shift_ref, ends_ref, sums_ref, early_ref, *refs):
    x_in, y_in, (out_ref, t_ref) = split(refs, nx_r, ny_r)
    width, nx = u_ref.shape[:2]
    ends = finished_ends(nx, ends_ref[1], x_in, y_in, width)
    apply_operator(outer_planes(u_ref), u_ref, shift_ref, x_in, y_in, ends, t_ref)
    payload = early_ref[...]
    for h, left in enumerate((u_ref, t_ref)):
        inner = [sums_ref[h, k] for k in range(len(pairs_of(width)))]
        payload = put_moment(width, moment_sums(0, nx, nx - 1, left, t_ref, inner), (3 + h) * width, payload)
    folded = payload[:4] + shift_lanes(payload, LANES // 2)[4:]
    out_ref[...] = jnp.broadcast_to(folded[None], out_ref.shape)


def lanes_of(matrix, j):
    return jnp.broadcast_to(matrix[:, j : j + 1], matrix.shape)


def rows_of(matrix, i):
    return jnp.broadcast_to(matrix[i : i + 1, :], matrix.shape)


def times(left, at, right):
    count = left.shape[0]
    total = lanes_of(left, at) * rows_of(right, 0)
    for k in range(1, count):
        total = total + lanes_of(left, at + k) * rows_of(right, k)
    return total


def shift_lanes(matrix, by):
    return pltpu.roll(matrix, by % LANES, 1)


def solve(columns, right):
    size = right[0].shape[0]
    sub = lax.broadcasted_iota(jnp.int32, right[0].shape, 0)
    for j in range(0, len(columns), 2):
        own, local = divmod(j, size)
        first, second = columns[j], columns[j + 1]
        a, b = rows_of(first[own], local), rows_of(second[own], local)
        c, d = rows_of(first[own], local + 1), rows_of(second[own], local + 1)
        scale = 1.0 / (a * d - b * c)
        a, b, c, d = a * scale, b * scale, c * scale, d * scale

        def step(value):
            upper, lower = rows_of(value[own], local), rows_of(value[own], local + 1)
            upper, lower = d * upper - b * lower, a * lower - c * upper
            value = [v - (f * upper + s * lower) for v, f, s in zip(value, first, second)]
            value[own] = jnp.where(sub == local, upper, jnp.where(sub == local + 1, lower, value[own]))
            return value

        columns = columns[: j + 2] + [step(column) for column in columns[j + 2 :]]
        right = step(right)
    return right


def small_algebra(s):
    n = s.shape[0]
    c0 = CENTRE
    lane = lax.broadcasted_iota(jnp.int32, s.shape, 1)
    sub = lax.broadcasted_iota(jnp.int32, s.shape, 0)
    n0, n1, n2, n3, n4 = shift_lanes(s, n), s, shift_lanes(s, -n), shift_lanes(s, -2 * n), shift_lanes(s, -3 * n)
    (e,) = solve([[lanes_of(s, j)] for j in range(n)], [s])
    p1 = times(s, n, e)
    p2 = times(s, 2 * n, e)
    p3 = times(s, 3 * n, e)
    cc = times(e, n, e)
    e2c = times(e, 2 * n, e)
    e2 = shift_lanes(e, -n)
    g = n2 - p1
    q = e2 - cc
    n3c = n3 - p2
    f3 = n3c - times(s, n, q)
    f4 = n4 - p3 - times(s, n, shift_lanes(e, -2 * n) - e2c)
    m11 = n2 + 2.0 * c0 * n1 + c0 * c0 * n0
    m12 = n3c + 2.0 * c0 * g
    m21 = n3 - times(s, n, e2) + 2.0 * c0 * g
    m22 = f4 + 2.0 * c0 * f3 + c0 * c0 * g
    columns = [[lanes_of(m11, n + j), lanes_of(m21, n + j)] for j in range(n)]
    columns += [[lanes_of(m12, n + j), lanes_of(m22, n + j)] for j in range(n)]
    pa, qa = solve(columns, [n1 + c0 * n0, g])
    on_b = pa - times(e, n, qa)
    unit = jnp.where(lane == sub + n, 1.0, 0.0)
    part = unit - times(e, n, pa) - c0 * pa - times(q, n, qa)
    squares = part * times(s, 0, part)
    pq = pa + c0 * qa
    squares = squares + pq * (times(g, n, pq) + 2.0 * times(f3, n, qa))
    squares = squares + qa * times(f4 - times(g, n, q), n, qa)
    return on_b, qa, jnp.sum(squares, axis=0, keepdims=True)


def finish_kernel(parts_ref, b_ref, u_ref, out_ref, norms_ref, coeff_ref):
    width, nx, ny, _ = b_ref.shape
    n = width
    folded = jnp.sum(parts_ref[...], axis=0)
    total = jnp.concatenate([folded, shift_lanes(folded, LANES // 2)], axis=0)
    on_b, on_u, squares = small_algebra(total)
    norms_ref[...] = jnp.sqrt(shift_lanes(squares, -n))[:, :n]
    for f in range(width):
        coeff_ref[0, f] = lanes_of(on_b, n + f)
        coeff_ref[1, f] = lanes_of(on_u, n + f)
    group = 2

    def fields(k, carry):
        first = [[[rows_of(coeff_ref[h, group * k + d], g) for g in range(width)] for h in range(2)] for d in range(group)]

        def plane(x, carry):
            for y in range(0, ny, 8):
                b = [b_ref[g, x, y : y + 8, :] for g in range(width)]
                u = [u_ref[g, x, y : y + 8, :] for g in range(width)]
                for d in range(group):
                    total = first[d][0][0] * b[0] + first[d][1][0] * u[0]
                    for g in range(1, width):
                        total = total + (first[d][0][g] * b[g] + first[d][1][g] * u[g])
                    out_ref[group * k + d, x, y : y + 8, :] = total
            return carry

        return lax.fori_loop(0, nx, plane, carry, unroll=nx)

    lax.fori_loop(0, width // group, fields, 0)


def call(kernel, out_shape, operands, scratch=(), flops=1_000_000, name=None, aliases=None):
    return pl.pallas_call(
        kernel,
        out_shape=out_shape,
        in_specs=[pl.BlockSpec(memory_space=pltpu.VMEM)] * len(operands),
        out_specs=jax.tree.map(lambda _: pl.BlockSpec(memory_space=pltpu.VMEM), out_shape),
        scratch_shapes=list(scratch),
        input_output_aliases=aliases or {},
        compiler_params=pltpu.CompilerParams(vmem_limit_bytes=8 << 20),
        cost_estimate=pl.CostEstimate(flops=flops, bytes_accessed=1 << 20, transcendentals=0),
        name=name,
    )(*operands)


def trade(turn, axis, faces):
    out = []
    for k, (face, pairs) in enumerate(zip(faces, swap_pairs(lax.axis_size(axis)))):
        with jax.named_scope(f"turn{turn}_{axis}_{k}"):
            out.append(swap(face, axis, pairs))
    return out


def body(right_side, shift):
    width, nx, ny, nz = right_side.shape
    assert width == 8 and nz == LANES and ny % 8 == 0 and nx > 2 and width * nx <= LANES // 2 and ny <= 8 * nx and ny * nx <= 4 * LANES
    nx_r, ny_r, nz_r = rounds_of()
    devices = 1
    for axis in AXES:
        devices *= lax.axis_size(axis)
    assert nz_r > 0
    block = jax.ShapeDtypeStruct(right_side.shape, F32)
    full = pltpu.VMEM(right_side.shape, F32)
    kernel = functools.partial

    def x_faces(extra):
        return [jax.ShapeDtypeStruct((width * ny // 8 + extra, 8, nz), F32)] * nx_r

    def y_faces(fields):
        return [jax.ShapeDtypeStruct((fields, nx, 1, nz), F32)] * ny_r

    def ends_of(layers):
        return jax.ShapeDtypeStruct((layers, ny, LANES), F32)

    faces = call(cut_x_kernel, x_faces(0), [right_side], name="cut")
    halo_x = trade(1, "gx", faces)
    packed = call(
        kernel(pack_kernel, ny_r),
        [*y_faces(width), jax.ShapeDtypeStruct((ny, LANES), F32), *[jax.ShapeDtypeStruct((ny // 8 + 1, 8, LANES), F32)] * nz_r],
        [right_side, shift],
        name="pack",
    )
    halo_y, own = trade(1, "gy", packed[:ny_r]), packed[ny_r]
    halo_z = trade(1, "gz", packed[ny_r + 1 :])
    inner, ends = call(
        kernel(inner_operator_kernel, ny_r, nz_r),
        [block, ends_of(2)],
        [right_side, shift, own, *halo_y, *halo_z],
        flops=20_000_000,
        name="inner1",
    )
    u, *faces = call(
        kernel(outer_operator_kernel, nx_r, ny_r),
        [block, *x_faces(1), *y_faces(width + 1)],
        [right_side, shift, inner, ends, *halo_x, *halo_y],
        aliases={2: 0},
        name="outer1",
    )
    halo_x = trade(2, "gx", faces[:nx_r])
    halo_y = trade(2, "gy", faces[nx_r:])
    early = call(early_moments_kernel, jax.ShapeDtypeStruct((8, LANES), F32), [right_side, u], flops=15_000_000, name="early")
    sums = call(
        kernel(inner_late_kernel, ny_r),
        jax.ShapeDtypeStruct((2, len(pairs_of(width)), 8, LANES), F32),
        [u, shift, ends, *halo_y],
        scratch=[full],
        flops=15_000_000,
        name="inner2",
    )
    copies = call(
        kernel(outer_late_kernel, nx_r, ny_r),
        jax.ShapeDtypeStruct((devices, 4, LANES), F32),
        [u, shift, ends, sums, early, *halo_x, *halo_y],
        scratch=[full],
        name="outer2",
    )
    parts = lax.all_to_all(copies, AXES, 0, 0, tiled=True)
    out, norms = call(
        finish_kernel,
        [block, jax.ShapeDtypeStruct((1, width), F32)],
        [parts, right_side, u],
        scratch=[pltpu.VMEM((2, width, 8, LANES), F32)],
        name="finish",
    )
    return out, norms.reshape(width)


def solution(mesh):
    in_specs = (P(None, "gx", "gy", "gz"), P("gx", "gy", "gz"))
    out_specs = (P(None, "gx", "gy", "gz"), P())
    return jax.shard_map(body, mesh=mesh, in_specs=in_specs, out_specs=out_specs, check_vma=False)
```

```python
import functools

import jax
import jax.numpy as jnp
from jax import lax
from jax.experimental import pallas as pl
from jax.experimental.pallas import tpu as pltpu
from jax.sharding import PartitionSpec as P

AXES = ("gx", "gy", "gz")
CENTRE = 4.0
LANES = 128
F32 = jnp.float32


def swap_pairs(count):
    first = [(i, j) for a in range(0, count - 1, 2) for i, j in ((a, a + 1), (a + 1, a))]
    second = [(i, j) for a in range(1, count - 1, 2) for i, j in ((a, a + 1), (a + 1, a))]
    return [pairs for pairs in (first, second) if pairs]


def swap(values, axis, pairs):
    side = lax.axis_size("gy")
    if axis == "gy" or side % 2:
        return lax.ppermute(values, axis, pairs)
    count = lax.axis_size(axis)
    named = {i for i, _ in pairs}
    at = (lambda i, y: i * side + y) if axis == "gx" else (lambda i, y: y * count + i)
    joint = [(at(i, y), at(j, y)) for i, j in pairs for y in range(side)]
    joint += [(at(i, y), at(i, y ^ 1)) for i in range(count) if i not in named for y in range(side)]
    return lax.ppermute(values, ("gx", "gy") if axis == "gx" else ("gy", "gz"), joint)


def rounds_of():
    return tuple(len(swap_pairs(lax.axis_size(axis))) for axis in AXES)


def parity(axis):
    return lax.rem(lax.axis_index(axis), 2) == 1


def x_plane(k, nx):
    return jnp.where(jnp.logical_xor(parity("gx"), k == 0), nx - 1, 0)


def cut_x_kernel(v_ref, *refs):
    for k, ref in enumerate(refs):
        ref[...] = v_ref[:, x_plane(k, v_ref.shape[1])].reshape(ref.shape)


def write_y_faces(v_ref, y_refs):
    ny = v_ref.shape[2]
    odd = parity("gy")
    for k, ref in enumerate(y_refs):
        high = jnp.logical_xor(odd, k == 0)
        ref[...] = jnp.where(high, v_ref[:, :, ny - 1 : ny, :], v_ref[:, :, 0:1, :])


def packed_ends(tile, m, lane, near, far=None):
    def at(offset):
        return lane == lax.rem(2 * m + offset + LANES, LANES)

    turned = pltpu.roll(tile, 2 * m, 1)
    near = jnp.where(at(0) | at(-1), turned, near)
    if far is None:
        return near
    return near, jnp.where(at(1) | at(-2), turned, far)


def pack_kernel(ny_r, v_ref, shift_ref, *refs):
    width, nx, ny, _ = v_ref.shape
    y_refs, (near_ref, *z_refs) = refs[:ny_r], refs[ny_r:]
    write_y_faces(v_ref, y_refs)
    lane = lax.broadcasted_iota(jnp.int32, (ny, LANES), 1)
    nothing = jnp.zeros((ny, LANES), F32)

    def field(f, packed):
        for x in range(nx):
            packed = packed_ends(v_ref[f, x], f * nx + x, lane, *packed)
        return packed

    near, far = lax.fori_loop(0, width, field, (nothing, nothing), unroll=width)
    diagonal = nothing
    for x in range(nx):
        diagonal = packed_ends((6.0 - CENTRE) + shift_ref[x], x, lane, diagonal)
    groups = ny // 8
    folded = sum(shift_lanes(diagonal[8 * r : 8 * r + 8], 2 * nx * r) for r in range(groups))
    near_ref[...] = near
    for k, ref in enumerate(z_refs):
        first = jnp.where(jnp.logical_xor(parity("gz"), k == 0), 1, 0)
        ref[:groups] = jnp.where(lax.rem(lane, 2) == first, near, far).reshape(groups, 8, LANES)
        ref[groups] = folded


def pick(axis, refs, load):
    if not refs:
        return 0.0, 0.0
    odd, at = parity(axis), lax.axis_index(axis)
    first = load(refs[0])
    second = load(refs[1]) if len(refs) > 1 else jnp.zeros_like(first)
    low = jnp.where(at == 0, 0.0, jnp.where(odd, first, second))
    high = jnp.where(at == lax.axis_size(axis) - 1, 0.0, jnp.where(odd, second, first))
    return low, high


def by_side(low, high, by):
    lane = lax.broadcasted_iota(jnp.int32, low.shape, 1)
    return jnp.where(lax.rem(lane, 2) == 0, shift_lanes(low, by), shift_lanes(high, -by))


def halo_ends(z_in, nx, width):
    groups = z_in[0].shape[0] - 1
    low, high = pick("gz", z_in, lambda ref: ref[:groups].reshape(8 * groups, LANES))
    folded = by_side(*pick("gz", z_in, lambda ref: ref[groups]), 1)
    lane = lax.broadcasted_iota(jnp.int32, folded.shape, 1)
    mine = lax.rem(lane + 1, LANES) < 2 * nx
    rows = [jnp.where(mine, shift_lanes(folded, -2 * nx * r), 0.0) for r in range(groups)]
    diagonal, copies = jnp.concatenate(rows, axis=0), 1
    while copies < width:
        diagonal = diagonal + shift_lanes(diagonal, 2 * nx * copies)
        copies *= 2
    return by_side(low, high, 1), by_side(low, high, 2), diagonal


def inside_grid(lane):
    low = jnp.where(lax.axis_index("gz") == 0, 0.0, 1.0)
    high = jnp.where(lax.axis_index("gz") == lax.axis_size("gz") - 1, 0.0, 1.0)
    return jnp.where(lax.rem(lane, 2) == 0, low, high)


def lane_x(lane, nx):
    return lax.rem((lane + 1) // 2, nx)


def fold_plane(ends, x, nx):
    ny = ends.shape[0]
    lane = lax.broadcasted_iota(jnp.int32, (8, LANES), 1)
    mine = lane_x(lane, nx) == x
    groups = [jnp.where(mine, ends[8 * r : 8 * r + 8], 0.0) for r in range(ny // 8)]
    return sum(pltpu.roll(group, lax.rem(LANES + 2 * r - 2 * x, LANES), 1) for r, group in enumerate(groups))


def unfold_plane(folded, x, ny):
    return jnp.concatenate([shift_lanes(folded, 2 * x - 2 * r) for r in range(ny // 8)], axis=0)


def operator_on_ends(nx, width, own, z_in):
    near, far, diagonal = halo_ends(z_in, nx, width)
    ny = near.shape[0]
    lane = lax.broadcasted_iota(jnp.int32, near.shape, 1)
    row = lax.broadcasted_iota(jnp.int32, near.shape, 0)
    x = lane_x(lane, nx)
    beside = own + far
    beside += jnp.where(x == 0, 0.0, pltpu.roll(near, 2, 1)) + jnp.where(x == nx - 1, 0.0, pltpu.roll(near, LANES - 2, 1))
    beside += jnp.where(row == 0, 0.0, pltpu.roll(near, 1, 0)) + jnp.where(row == ny - 1, 0.0, pltpu.roll(near, ny - 1, 0))
    return near, inside_grid(lane) * (diagonal * near - beside)


def finished_ends(nx, base, x_in, y_in, width):
    ny = base.shape[0]
    lane = lax.broadcasted_iota(jnp.int32, base.shape, 1)
    row = lax.broadcasted_iota(jnp.int32, base.shape, 0)
    low_y, high_y = pick("gy", y_in, lambda ref: ref[width, 0])
    beside = jnp.where(row == 0, low_y, 0.0) + jnp.where(row == ny - 1, high_y, 0.0)
    if x_in:
        x = lane_x(lane, nx)
        low_x, high_x = pick("gx", x_in, lambda ref: ref[ref.shape[0] - 1])
        beside += jnp.where(x == 0, unfold_plane(low_x, 0, ny), 0.0)
        beside += jnp.where(x == nx - 1, unfold_plane(high_x, nx - 1, ny), 0.0)
    return base - inside_grid(lane) * beside


def face_of(ref, f, ny):
    groups = ny // 8
    return ref[pl.ds(f * groups, groups)].reshape(ny, LANES)


def apply_operator(planes, v_ref, shift_ref, x_in, y_in, ends, out_ref):
    width, nx, ny, _ = v_ref.shape
    lane = lax.broadcasted_iota(jnp.int32, (ny, LANES), 1)
    row = lax.broadcasted_iota(jnp.int32, (ny, LANES), 0)
    def field(f, carry):
        low_x, high_x = pick("gx", x_in, lambda ref: face_of(ref, f, ny))
        for x in planes:
            low_y, high_y = pick("gy", y_in, lambda ref: ref[f, x])
            v = v_ref[f, x]
            end = pltpu.roll(ends, lax.rem(LANES - 2 * (f * nx + x), LANES), 1)
            beside = (v_ref[f, x - 1] if x > 0 else low_x) + (v_ref[f, x + 1] if x < nx - 1 else high_x)
            beside += jnp.where(row == 0, low_y, pltpu.roll(v, 1, 0))
            beside += jnp.where(row == ny - 1, high_y, pltpu.roll(v, ny - 1, 0))
            beside += jnp.where(lane == 0, end, pltpu.roll(v, 1, 1))
            beside += jnp.where(lane == LANES - 1, end, pltpu.roll(v, LANES - 1, 1))
            out_ref[f, x] = ((6.0 - CENTRE) + shift_ref[x]) * v - beside
        return carry

    lax.fori_loop(0, width, field, 0, unroll=width)


def split(refs, *counts):
    parts, at = [], 0
    for count in counts:
        parts.append(refs[at : at + count])
        at += count
    return (*parts, refs[at:])


def inner_planes(ref):
    return range(1, ref.shape[1] - 1)


def outer_planes(ref):
    return (0, ref.shape[1] - 1)


def inner_operator_kernel(ny_r, nz_r, v_ref, shift_ref, own_ref, *refs):
    y_in, z_in, (out_ref, ends_ref) = split(refs, ny_r, nz_r)
    near, base = operator_on_ends(v_ref.shape[1], v_ref.shape[0], own_ref[...], z_in)
    ends_ref[0] = near
    ends_ref[1] = base
    apply_operator(inner_planes(v_ref), v_ref, shift_ref, (), y_in, near, out_ref)


def outer_operator_kernel(nx_r, ny_r, v_ref, shift_ref, inner_ref, ends_ref, *refs):
    x_in, y_in, (out_ref,), x_out, y_out = split(refs, nx_r, ny_r, 1, nx_r)
    width, nx, ny, _ = v_ref.shape
    near = ends_ref[0]
    apply_operator(outer_planes(v_ref), v_ref, shift_ref, x_in, y_in, near, out_ref)
    for k, ref in enumerate(x_out):
        plane, rows = x_plane(k, nx), width * ny // 8
        ref[:rows] = out_ref[:, plane].reshape(rows, 8, LANES)
        ref[rows] = fold_plane(near, plane, nx)
    write_y_faces(out_ref, [ref.at[:width] for ref in y_out])
    for k, ref in enumerate(y_out):
        high = jnp.logical_xor(parity("gy"), k == 0)
        line = jnp.where(high, near[ny - 1 : ny], near[0:1])
        for x in range(nx):
            ref[width, x] = line


def pairs_of(width):
    return [(i, j) for i in range(width) for j in range(i + 1)]


def moment_sums(first, last, step, a_ref, b_ref, sums):
    width, _, ny, _ = a_ref.shape
    pairs = pairs_of(width)

    def plane(k, sums):
        sums, x = list(sums), first + k * step
        for y in range(0, ny, 8):
            a = [a_ref[f, x, y : y + 8, :] for f in range(width)]
            b = a if b_ref is a_ref else [b_ref[f, x, y : y + 8, :] for f in range(width)]
            for k, (i, j) in enumerate(pairs):
                sums[k] = sums[k] + a[i] * b[j]
        return tuple(sums)

    return lax.fori_loop(0, -((first - last) // step), plane, tuple(sums), unroll=2)


def no_sums(width):
    return [jnp.zeros((8, LANES), F32) for _ in pairs_of(width)]


def put_moment(width, sums, at, payload):
    rows = {}
    for (i, j), value in zip(pairs_of(width), sums):
        rows[i, j] = rows[j, i] = jnp.sum(value, axis=0, keepdims=True)
    lane = lax.broadcasted_iota(jnp.int32, (8, LANES), 1)
    for i in range(width):
        column = jnp.sum(jnp.concatenate([rows[i, j] for j in range(width)], axis=0), axis=1, keepdims=True)
        payload = jnp.where(lane == at + i, column, payload)
    return payload


def early_moments_kernel(b_ref, u_ref, out_ref):
    width, nx = b_ref.shape[:2]
    payload = jnp.zeros((8, LANES), F32)
    for k, (left, right) in enumerate(((b_ref, b_ref), (b_ref, u_ref), (u_ref, u_ref))):
        payload = put_moment(width, moment_sums(0, nx, 1, left, right, no_sums(width)), k * width, payload)
    out_ref[...] = payload


def inner_late_kernel(ny_r, u_ref, shift_ref, ends_ref, *refs):
    y_in, (sums_ref, t_ref) = split(refs, ny_r)
    width, nx = u_ref.shape[:2]
    ends = finished_ends(nx, ends_ref[1], (), y_in, width)
    apply_operator(inner_planes(u_ref), u_ref, shift_ref, (), y_in, ends, t_ref)
    for h, left in enumerate((u_ref, t_ref)):
        for k, value in enumerate(moment_sums(1, nx - 1, 1, left, t_ref, no_sums(width))):
            sums_ref[h, k] = value


def outer_late_kernel(nx_r, ny_r, u_ref, shift_ref, ends_ref, sums_ref, early_ref, *refs):
    x_in, y_in, (out_ref, t_ref) = split(refs, nx_r, ny_r)
    width, nx = u_ref.shape[:2]
    ends = finished_ends(nx, ends_ref[1], x_in, y_in, width)
    apply_operator(outer_planes(u_ref), u_ref, shift_ref, x_in, y_in, ends, t_ref)
    payload = early_ref[...]
    for h, left in enumerate((u_ref, t_ref)):
        inner = [sums_ref[h, k] for k in range(len(pairs_of(width)))]
        payload = put_moment(width, moment_sums(0, nx, nx - 1, left, t_ref, inner), (3 + h) * width, payload)
    folded = payload[:4] + shift_lanes(payload, LANES // 2)[4:]
    out_ref[...] = jnp.broadcast_to(folded[None], out_ref.shape)


def lanes_of(matrix, j):
    return jnp.broadcast_to(matrix[:, j : j + 1], matrix.shape)


def rows_of(matrix, i):
    return jnp.broadcast_to(matrix[i : i + 1, :], matrix.shape)


def times(left, at, right):
    count = left.shape[0]
    total = lanes_of(left, at) * rows_of(right, 0)
    for k in range(1, count):
        total = total + lanes_of(left, at + k) * rows_of(right, k)
    return total


def shift_lanes(matrix, by):
    return pltpu.roll(matrix, by % LANES, 1)


def solve(columns, right):
    size = right[0].shape[0]
    sub = lax.broadcasted_iota(jnp.int32, right[0].shape, 0)
    for j in range(0, len(columns), 2):
        own, local = divmod(j, size)
        first, second = columns[j], columns[j + 1]
        a, b = rows_of(first[own], local), rows_of(second[own], local)
        c, d = rows_of(first[own], local + 1), rows_of(second[own], local + 1)
        scale = 1.0 / (a * d - b * c)
        a, b, c, d = a * scale, b * scale, c * scale, d * scale

        def step(value):
            upper, lower = rows_of(value[own], local), rows_of(value[own], local + 1)
            upper, lower = d * upper - b * lower, a * lower - c * upper
            value = [v - (f * upper + s * lower) for v, f, s in zip(value, first, second)]
            value[own] = jnp.where(sub == local, upper, jnp.where(sub == local + 1, lower, value[own]))
            return value

        columns = columns[: j + 2] + [step(column) for column in columns[j + 2 :]]
        right = step(right)
    return right


def small_algebra(s):
    n = s.shape[0]
    c0 = CENTRE
    lane = lax.broadcasted_iota(jnp.int32, s.shape, 1)
    sub = lax.broadcasted_iota(jnp.int32, s.shape, 0)
    n0, n1, n2, n3, n4 = shift_lanes(s, n), s, shift_lanes(s, -n), shift_lanes(s, -2 * n), shift_lanes(s, -3 * n)
    (e,) = solve([[lanes_of(s, j)] for j in range(n)], [s])
    p1 = times(s, n, e)
    p2 = times(s, 2 * n, e)
    p3 = times(s, 3 * n, e)
    cc = times(e, n, e)
    e2c = times(e, 2 * n, e)
    e2 = shift_lanes(e, -n)
    g = n2 - p1
    q = e2 - cc
    n3c = n3 - p2
    f3 = n3c - times(s, n, q)
    f4 = n4 - p3 - times(s, n, shift_lanes(e, -2 * n) - e2c)
    m11 = n2 + 2.0 * c0 * n1 + c0 * c0 * n0
    m12 = n3c + 2.0 * c0 * g
    m21 = n3 - times(s, n, e2) + 2.0 * c0 * g
    m22 = f4 + 2.0 * c0 * f3 + c0 * c0 * g
    columns = [[lanes_of(m11, n + j), lanes_of(m21, n + j)] for j in range(n)]
    columns += [[lanes_of(m12, n + j), lanes_of(m22, n + j)] for j in range(n)]
    pa, qa = solve(columns, [n1 + c0 * n0, g])
    on_b = pa - times(e, n, qa)
    unit = jnp.where(lane == sub + n, 1.0, 0.0)
    part = unit - times(e, n, pa) - c0 * pa - times(q, n, qa)
    squares = part * times(s, 0, part)
    pq = pa + c0 * qa
    squares = squares + pq * (times(g, n, pq) + 2.0 * times(f3, n, qa))
    squares = squares + qa * times(f4 - times(g, n, q), n, qa)
    return on_b, qa, jnp.sum(squares, axis=0, keepdims=True)


def finish_kernel(parts_ref, b_ref, u_ref, out_ref, norms_ref, coeff_ref):
    width, nx, ny, _ = b_ref.shape
    n = width
    folded = jnp.sum(parts_ref[...], axis=0)
    total = jnp.concatenate([folded, shift_lanes(folded, LANES // 2)], axis=0)
    on_b, on_u, squares = small_algebra(total)
    norms_ref[...] = jnp.sqrt(shift_lanes(squares, -n))[:, :n]
    for f in range(width):
        coeff_ref[0, f] = lanes_of(on_b, n + f)
        coeff_ref[1, f] = lanes_of(on_u, n + f)
    group = 2

    def fields(k, carry):
        first = [[[rows_of(coeff_ref[h, group * k + d], g) for g in range(width)] for h in range(2)] for d in range(group)]

        def plane(x, carry):
            for y in range(0, ny, 8):
                b = [b_ref[g, x, y : y + 8, :] for g in range(width)]
                u = [u_ref[g, x, y : y + 8, :] for g in range(width)]
                for d in range(group):
                    total = first[d][0][0] * b[0] + first[d][1][0] * u[0]
                    for g in range(1, width):
                        total = total + (first[d][0][g] * b[g] + first[d][1][g] * u[g])
                    out_ref[group * k + d, x, y : y + 8, :] = total
            return carry

        return lax.fori_loop(0, nx, plane, carry, unroll=nx)

    lax.fori_loop(0, width // group, fields, 0)


def call(kernel, out_shape, operands, scratch=(), flops=1_000_000, name=None, aliases=None):
    return pl.pallas_call(
        kernel,
        out_shape=out_shape,
        in_specs=[pl.BlockSpec(memory_space=pltpu.VMEM)] * len(operands),
        out_specs=jax.tree.map(lambda _: pl.BlockSpec(memory_space=pltpu.VMEM), out_shape),
        scratch_shapes=list(scratch),
        input_output_aliases=aliases or {},
        compiler_params=pltpu.CompilerParams(vmem_limit_bytes=8 << 20),
        cost_estimate=pl.CostEstimate(flops=flops, bytes_accessed=1 << 20, transcendentals=0),
        name=name,
    )(*operands)


def trade(turn, axis, faces):
    out = []
    for k, (face, pairs) in enumerate(zip(faces, swap_pairs(lax.axis_size(axis)))):
        with jax.named_scope(f"turn{turn}_{axis}_{k}"):
            out.append(swap(face, axis, pairs))
    return out


def body(right_side, shift):
    width, nx, ny, nz = right_side.shape
    assert width == 8 and nz == LANES and ny % 8 == 0 and nx > 2 and width * nx <= LANES // 2 and ny <= 8 * nx and ny * nx <= 4 * LANES
    nx_r, ny_r, nz_r = rounds_of()
    devices = 1
    for axis in AXES:
        devices *= lax.axis_size(axis)
    assert nz_r > 0
    block = jax.ShapeDtypeStruct(right_side.shape, F32)
    full = pltpu.VMEM(right_side.shape, F32)
    kernel = functools.partial

    def x_faces(extra):
        return [jax.ShapeDtypeStruct((width * ny // 8 + extra, 8, nz), F32)] * nx_r

    def y_faces(fields):
        return [jax.ShapeDtypeStruct((fields, nx, 1, nz), F32)] * ny_r

    def ends_of(layers):
        return jax.ShapeDtypeStruct((layers, ny, LANES), F32)

    faces = call(cut_x_kernel, x_faces(0), [right_side], name="cut")
    halo_x = trade(1, "gx", faces)
    packed = call(
        kernel(pack_kernel, ny_r),
        [*y_faces(width), jax.ShapeDtypeStruct((ny, LANES), F32), *[jax.ShapeDtypeStruct((ny // 8 + 1, 8, LANES), F32)] * nz_r],
        [right_side, shift],
        name="pack",
    )
    halo_y, own = trade(1, "gy", packed[:ny_r]), packed[ny_r]
    halo_z = trade(1, "gz", packed[ny_r + 1 :])
    inner, ends = call(
        kernel(inner_operator_kernel, ny_r, nz_r),
        [block, ends_of(2)],
        [right_side, shift, own, *halo_y, *halo_z],
        flops=20_000_000,
        name="inner1",
    )
    u, *faces = call(
        kernel(outer_operator_kernel, nx_r, ny_r),
        [block, *x_faces(1), *y_faces(width + 1)],
        [right_side, shift, inner, ends, *halo_x, *halo_y],
        aliases={2: 0},
        name="outer1",
    )
    halo_x = trade(2, "gx", faces[:nx_r])
    halo_y = trade(2, "gy", faces[nx_r:])
    early = call(early_moments_kernel, jax.ShapeDtypeStruct((8, LANES), F32), [right_side, u], flops=15_000_000, name="early")
    sums = call(
        kernel(inner_late_kernel, ny_r),
        jax.ShapeDtypeStruct((2, len(pairs_of(width)), 8, LANES), F32),
        [u, shift, ends, *halo_y],
        scratch=[full],
        flops=15_000_000,
        name="inner2",
    )
    copies = call(
        kernel(outer_late_kernel, nx_r, ny_r),
        jax.ShapeDtypeStruct((devices, 4, LANES), F32),
        [u, shift, ends, sums, early, *halo_x, *halo_y],
        scratch=[full],
        name="outer2",
    )
    parts = lax.all_to_all(copies, AXES, 0, 0, tiled=True)
    out, norms = call(
        finish_kernel,
        [block, jax.ShapeDtypeStruct((1, width), F32)],
        [parts, right_side, u],
        scratch=[pltpu.VMEM((2, width, 8, LANES), F32)],
        name="finish",
    )
    return out, norms.reshape(width)


def solution(mesh):
    in_specs = (P(None, "gx", "gy", "gz"), P("gx", "gy", "gz"))
    out_specs = (P(None, "gx", "gy", "gz"), P())
    return jax.shard_map(body, mesh=mesh, in_specs=in_specs, out_specs=out_specs, check_vma=False)
```

```python
import functools

import jax
import jax.numpy as jnp
from jax import lax
from jax.experimental import pallas as pl
from jax.experimental.pallas import tpu as pltpu
from jax.sharding import PartitionSpec as P

AXES = ("gx", "gy", "gz")
CENTRE = 4.0
LANES = 128
F32 = jnp.float32


def swap_pairs(count):
    first = [(i, j) for a in range(0, count - 1, 2) for i, j in ((a, a + 1), (a + 1, a))]
    second = [(i, j) for a in range(1, count - 1, 2) for i, j in ((a, a + 1), (a + 1, a))]
    return [pairs for pairs in (first, second) if pairs]


def swap(values, axis, pairs):
    side = lax.axis_size("gy")
    if axis == "gy" or side % 2:
        return lax.ppermute(values, axis, pairs)
    count = lax.axis_size(axis)
    named = {i for i, _ in pairs}
    at = (lambda i, y: i * side + y) if axis == "gx" else (lambda i, y: y * count + i)
    joint = [(at(i, y), at(j, y)) for i, j in pairs for y in range(side)]
    joint += [(at(i, y), at(i, y ^ 1)) for i in range(count) if i not in named for y in range(side)]
    return lax.ppermute(values, ("gx", "gy") if axis == "gx" else ("gy", "gz"), joint)


def rounds_of():
    return tuple(len(swap_pairs(lax.axis_size(axis))) for axis in AXES)


def parity(axis):
    return lax.rem(lax.axis_index(axis), 2) == 1


def x_plane(k, nx):
    return jnp.where(jnp.logical_xor(parity("gx"), k == 0), nx - 1, 0)


def cut_x_kernel(v_ref, *refs):
    for k, ref in enumerate(refs):
        ref[...] = v_ref[:, x_plane(k, v_ref.shape[1])].reshape(ref.shape)


def write_y_faces(v_ref, y_refs):
    ny = v_ref.shape[2]
    odd = parity("gy")
    for k, ref in enumerate(y_refs):
        high = jnp.logical_xor(odd, k == 0)
        ref[...] = jnp.where(high, v_ref[:, :, ny - 1 : ny, :], v_ref[:, :, 0:1, :])


def packed_ends(tile, m, lane, near, far=None):
    def at(offset):
        return lane == lax.rem(2 * m + offset + LANES, LANES)

    turned = pltpu.roll(tile, 2 * m, 1)
    near = jnp.where(at(0) | at(-1), turned, near)
    if far is None:
        return near
    return near, jnp.where(at(1) | at(-2), turned, far)


def pack_kernel(ny_r, v_ref, shift_ref, *refs):
    width, nx, ny, _ = v_ref.shape
    y_refs, (near_ref, *z_refs) = refs[:ny_r], refs[ny_r:]
    write_y_faces(v_ref, y_refs)
    lane = lax.broadcasted_iota(jnp.int32, (ny, LANES), 1)
    nothing = jnp.zeros((ny, LANES), F32)

    def field(f, packed):
        for x in range(nx):
            packed = packed_ends(v_ref[f, x], f * nx + x, lane, *packed)
        return packed

    near, far = lax.fori_loop(0, width, field, (nothing, nothing), unroll=width)
    diagonal = nothing
    for x in range(nx):
        diagonal = packed_ends((6.0 - CENTRE) + shift_ref[x], x, lane, diagonal)
    groups = ny // 8
    folded = sum(shift_lanes(diagonal[8 * r : 8 * r + 8], 2 * nx * r) for r in range(groups))
    near_ref[...] = near
    for k, ref in enumerate(z_refs):
        first = jnp.where(jnp.logical_xor(parity("gz"), k == 0), 1, 0)
        ref[:groups] = jnp.where(lax.rem(lane, 2) == first, near, far).reshape(groups, 8, LANES)
        ref[groups] = folded


def pick(axis, refs, load):
    if not refs:
        return 0.0, 0.0
    odd, at = parity(axis), lax.axis_index(axis)
    first = load(refs[0])
    second = load(refs[1]) if len(refs) > 1 else jnp.zeros_like(first)
    low = jnp.where(at == 0, 0.0, jnp.where(odd, first, second))
    high = jnp.where(at == lax.axis_size(axis) - 1, 0.0, jnp.where(odd, second, first))
    return low, high


def by_side(low, high, by):
    lane = lax.broadcasted_iota(jnp.int32, low.shape, 1)
    return jnp.where(lax.rem(lane, 2) == 0, shift_lanes(low, by), shift_lanes(high, -by))


def halo_ends(z_in, nx, width):
    groups = z_in[0].shape[0] - 1
    low, high = pick("gz", z_in, lambda ref: ref[:groups].reshape(8 * groups, LANES))
    folded = by_side(*pick("gz", z_in, lambda ref: ref[groups]), 1)
    lane = lax.broadcasted_iota(jnp.int32, folded.shape, 1)
    mine = lax.rem(lane + 1, LANES) < 2 * nx
    rows = [jnp.where(mine, shift_lanes(folded, -2 * nx * r), 0.0) for r in range(groups)]
    diagonal, copies = jnp.concatenate(rows, axis=0), 1
    while copies < width:
        diagonal = diagonal + shift_lanes(diagonal, 2 * nx * copies)
        copies *= 2
    return by_side(low, high, 1), by_side(low, high, 2), diagonal


def inside_grid(lane):
    low = jnp.where(lax.axis_index("gz") == 0, 0.0, 1.0)
    high = jnp.where(lax.axis_index("gz") == lax.axis_size("gz") - 1, 0.0, 1.0)
    return jnp.where(lax.rem(lane, 2) == 0, low, high)


def lane_x(lane, nx):
    return lax.rem((lane + 1) // 2, nx)


def fold_plane(ends, x, nx):
    ny = ends.shape[0]
    lane = lax.broadcasted_iota(jnp.int32, (8, LANES), 1)
    mine = lane_x(lane, nx) == x
    groups = [jnp.where(mine, ends[8 * r : 8 * r + 8], 0.0) for r in range(ny // 8)]
    return sum(pltpu.roll(group, lax.rem(LANES + 2 * r - 2 * x, LANES), 1) for r, group in enumerate(groups))


def unfold_plane(folded, x, ny):
    return jnp.concatenate([shift_lanes(folded, 2 * x - 2 * r) for r in range(ny // 8)], axis=0)


def operator_on_ends(nx, width, own, z_in):
    near, far, diagonal = halo_ends(z_in, nx, width)
    ny = near.shape[0]
    lane = lax.broadcasted_iota(jnp.int32, near.shape, 1)
    row = lax.broadcasted_iota(jnp.int32, near.shape, 0)
    x = lane_x(lane, nx)
    beside = own + far
    beside += jnp.where(x == 0, 0.0, pltpu.roll(near, 2, 1)) + jnp.where(x == nx - 1, 0.0, pltpu.roll(near, LANES - 2, 1))
    beside += jnp.where(row == 0, 0.0, pltpu.roll(near, 1, 0)) + jnp.where(row == ny - 1, 0.0, pltpu.roll(near, ny - 1, 0))
    return near, inside_grid(lane) * (diagonal * near - beside)


def finished_ends(nx, base, x_in, y_in, width):
    ny = base.shape[0]
    lane = lax.broadcasted_iota(jnp.int32, base.shape, 1)
    row = lax.broadcasted_iota(jnp.int32, base.shape, 0)
    low_y, high_y = pick("gy", y_in, lambda ref: ref[width, 0])
    beside = jnp.where(row == 0, low_y, 0.0) + jnp.where(row == ny - 1, high_y, 0.0)
    if x_in:
        x = lane_x(lane, nx)
        low_x, high_x = pick("gx", x_in, lambda ref: ref[ref.shape[0] - 1])
        beside += jnp.where(x == 0, unfold_plane(low_x, 0, ny), 0.0)
        beside += jnp.where(x == nx - 1, unfold_plane(high_x, nx - 1, ny), 0.0)
    return base - inside_grid(lane) * beside


def face_of(ref, f, ny):
    groups = ny // 8
    return ref[pl.ds(f * groups, groups)].reshape(ny, LANES)


def apply_operator(planes, v_ref, shift_ref, x_in, y_in, ends, out_ref):
    width, nx, ny, _ = v_ref.shape
    lane = lax.broadcasted_iota(jnp.int32, (ny, LANES), 1)
    row = lax.broadcasted_iota(jnp.int32, (ny, LANES), 0)
    def field(f, carry):
        low_x, high_x = pick("gx", x_in, lambda ref: face_of(ref, f, ny))
        for x in planes:
            low_y, high_y = pick("gy", y_in, lambda ref: ref[f, x])
            v = v_ref[f, x]
            end = pltpu.roll(ends, lax.rem(LANES - 2 * (f * nx + x), LANES), 1)
            beside = (v_ref[f, x - 1] if x > 0 else low_x) + (v_ref[f, x + 1] if x < nx - 1 else high_x)
            beside += jnp.where(row == 0, low_y, pltpu.roll(v, 1, 0))
            beside += jnp.where(row == ny - 1, high_y, pltpu.roll(v, ny - 1, 0))
            beside += jnp.where(lane == 0, end, pltpu.roll(v, 1, 1))
            beside += jnp.where(lane == LANES - 1, end, pltpu.roll(v, LANES - 1, 1))
            out_ref[f, x] = ((6.0 - CENTRE) + shift_ref[x]) * v - beside
        return carry

    lax.fori_loop(0, width, field, 0, unroll=width)


def split(refs, *counts):
    parts, at = [], 0
    for count in counts:
        parts.append(refs[at : at + count])
        at += count
    return (*parts, refs[at:])


def inner_planes(ref):
    return range(1, ref.shape[1] - 1)


def outer_planes(ref):
    return (0, ref.shape[1] - 1)


def outer_operator_kernel(nx_r, ny_r, nz_r, v_ref, shift_ref, own_ref, *refs):
    x_in, y_in, z_in, (out_ref, ends_ref), x_out = split(refs, nx_r, ny_r, nz_r, 2)
    width, nx, ny, _ = v_ref.shape
    near, base = operator_on_ends(nx, width, own_ref[...], z_in)
    ends_ref[0] = near
    ends_ref[1] = base
    apply_operator(outer_planes(v_ref), v_ref, shift_ref, x_in, y_in, near, out_ref)
    for k, ref in enumerate(x_out):
        plane, rows = x_plane(k, nx), width * ny // 8
        ref[:rows] = out_ref[:, plane].reshape(rows, 8, LANES)
        ref[rows] = fold_plane(near, plane, nx)


def inner_operator_kernel(ny_r, v_ref, shift_ref, outer_ref, ends_ref, *refs):
    y_in, (out_ref,), y_out = split(refs, ny_r, 1)
    width, nx, ny, _ = v_ref.shape
    near = ends_ref[0]
    apply_operator(inner_planes(v_ref), v_ref, shift_ref, (), y_in, near, out_ref)
    write_y_faces(out_ref, [ref.at[:width] for ref in y_out])
    for k, ref in enumerate(y_out):
        high = jnp.logical_xor(parity("gy"), k == 0)
        line = jnp.where(high, near[ny - 1 : ny], near[0:1])
        for x in range(nx):
            ref[width, x] = line


def pairs_of(width):
    return [(i, j) for i in range(width) for j in range(i + 1)]


def moment_sums(first, last, step, a_ref, b_ref, sums):
    width, _, ny, _ = a_ref.shape
    pairs = pairs_of(width)

    def plane(k, sums):
        sums, x = list(sums), first + k * step
        for y in range(0, ny, 8):
            a = [a_ref[f, x, y : y + 8, :] for f in range(width)]
            b = a if b_ref is a_ref else [b_ref[f, x, y : y + 8, :] for f in range(width)]
            for k, (i, j) in enumerate(pairs):
                sums[k] = sums[k] + a[i] * b[j]
        return tuple(sums)

    return lax.fori_loop(0, -((first - last) // step), plane, tuple(sums), unroll=2)


def no_sums(width):
    return [jnp.zeros((8, LANES), F32) for _ in pairs_of(width)]


def put_moment(width, sums, at, payload):
    rows = {}
    for (i, j), value in zip(pairs_of(width), sums):
        rows[i, j] = rows[j, i] = jnp.sum(value, axis=0, keepdims=True)
    lane = lax.broadcasted_iota(jnp.int32, (8, LANES), 1)
    for i in range(width):
        column = jnp.sum(jnp.concatenate([rows[i, j] for j in range(width)], axis=0), axis=1, keepdims=True)
        payload = jnp.where(lane == at + i, column, payload)
    return payload


def early_moments_kernel(b_ref, u_ref, out_ref):
    width, nx = b_ref.shape[:2]
    payload = jnp.zeros((8, LANES), F32)
    for k, (left, right) in enumerate(((b_ref, b_ref), (b_ref, u_ref), (u_ref, u_ref))):
        payload = put_moment(width, moment_sums(0, nx, 1, left, right, no_sums(width)), k * width, payload)
    out_ref[...] = payload


def inner_late_kernel(ny_r, u_ref, shift_ref, ends_ref, *refs):
    y_in, (sums_ref, t_ref) = split(refs, ny_r)
    width, nx = u_ref.shape[:2]
    ends = finished_ends(nx, ends_ref[1], (), y_in, width)
    apply_operator(inner_planes(u_ref), u_ref, shift_ref, (), y_in, ends, t_ref)
    for h, left in enumerate((u_ref, t_ref)):
        for k, value in enumerate(moment_sums(1, nx - 1, 1, left, t_ref, no_sums(width))):
            sums_ref[h, k] = value


def outer_late_kernel(nx_r, ny_r, u_ref, shift_ref, ends_ref, sums_ref, early_ref, *refs):
    x_in, y_in, (out_ref, t_ref) = split(refs, nx_r, ny_r)
    width, nx = u_ref.shape[:2]
    ends = finished_ends(nx, ends_ref[1], x_in, y_in, width)
    apply_operator(outer_planes(u_ref), u_ref, shift_ref, x_in, y_in, ends, t_ref)
    payload = early_ref[...]
    for h, left in enumerate((u_ref, t_ref)):
        inner = [sums_ref[h, k] for k in range(len(pairs_of(width)))]
        payload = put_moment(width, moment_sums(0, nx, nx - 1, left, t_ref, inner), (3 + h) * width, payload)
    folded = payload[:4] + shift_lanes(payload, LANES // 2)[4:]
    out_ref[...] = jnp.broadcast_to(folded[None], out_ref.shape)


def lanes_of(matrix, j):
    return jnp.broadcast_to(matrix[:, j : j + 1], matrix.shape)


def rows_of(matrix, i):
    return jnp.broadcast_to(matrix[i : i + 1, :], matrix.shape)


def times(left, at, right):
    count = left.shape[0]
    total = lanes_of(left, at) * rows_of(right, 0)
    for k in range(1, count):
        total = total + lanes_of(left, at + k) * rows_of(right, k)
    return total


def shift_lanes(matrix, by):
    return pltpu.roll(matrix, by % LANES, 1)


def solve(columns, right):
    size = right[0].shape[0]
    sub = lax.broadcasted_iota(jnp.int32, right[0].shape, 0)
    for j in range(0, len(columns), 2):
        own, local = divmod(j, size)
        first, second = columns[j], columns[j + 1]
        a, b = rows_of(first[own], local), rows_of(second[own], local)
        c, d = rows_of(first[own], local + 1), rows_of(second[own], local + 1)
        scale = 1.0 / (a * d - b * c)
        a, b, c, d = a * scale, b * scale, c * scale, d * scale

        def step(value):
            upper, lower = rows_of(value[own], local), rows_of(value[own], local + 1)
            upper, lower = d * upper - b * lower, a * lower - c * upper
            value = [v - (f * upper + s * lower) for v, f, s in zip(value, first, second)]
            value[own] = jnp.where(sub == local, upper, jnp.where(sub == local + 1, lower, value[own]))
            return value

        columns = columns[: j + 2] + [step(column) for column in columns[j + 2 :]]
        right = step(right)
    return right


def small_algebra(s):
    n = s.shape[0]
    c0 = CENTRE
    lane = lax.broadcasted_iota(jnp.int32, s.shape, 1)
    sub = lax.broadcasted_iota(jnp.int32, s.shape, 0)
    n0, n1, n2, n3, n4 = shift_lanes(s, n), s, shift_lanes(s, -n), shift_lanes(s, -2 * n), shift_lanes(s, -3 * n)
    (e,) = solve([[lanes_of(s, j)] for j in range(n)], [s])
    p1 = times(s, n, e)
    p2 = times(s, 2 * n, e)
    p3 = times(s, 3 * n, e)
    cc = times(e, n, e)
    e2c = times(e, 2 * n, e)
    e2 = shift_lanes(e, -n)
    g = n2 - p1
    q = e2 - cc
    n3c = n3 - p2
    f3 = n3c - times(s, n, q)
    f4 = n4 - p3 - times(s, n, shift_lanes(e, -2 * n) - e2c)
    m11 = n2 + 2.0 * c0 * n1 + c0 * c0 * n0
    m12 = n3c + 2.0 * c0 * g
    m21 = n3 - times(s, n, e2) + 2.0 * c0 * g
    m22 = f4 + 2.0 * c0 * f3 + c0 * c0 * g
    columns = [[lanes_of(m11, n + j), lanes_of(m21, n + j)] for j in range(n)]
    columns += [[lanes_of(m12, n + j), lanes_of(m22, n + j)] for j in range(n)]
    pa, qa = solve(columns, [n1 + c0 * n0, g])
    on_b = pa - times(e, n, qa)
    unit = jnp.where(lane == sub + n, 1.0, 0.0)
    part = unit - times(e, n, pa) - c0 * pa - times(q, n, qa)
    squares = part * times(s, 0, part)
    pq = pa + c0 * qa
    squares = squares + pq * (times(g, n, pq) + 2.0 * times(f3, n, qa))
    squares = squares + qa * times(f4 - times(g, n, q), n, qa)
    return on_b, qa, jnp.sum(squares, axis=0, keepdims=True)


def finish_kernel(parts_ref, b_ref, u_ref, out_ref, norms_ref, coeff_ref):
    width, nx, ny, _ = b_ref.shape
    n = width
    folded = jnp.sum(parts_ref[...], axis=0)
    total = jnp.concatenate([folded, shift_lanes(folded, LANES // 2)], axis=0)
    on_b, on_u, squares = small_algebra(total)
    norms_ref[...] = jnp.sqrt(shift_lanes(squares, -n))[:, :n]
    for f in range(width):
        coeff_ref[0, f] = lanes_of(on_b, n + f)
        coeff_ref[1, f] = lanes_of(on_u, n + f)
    group = 2

    def fields(k, carry):
        first = [[[rows_of(coeff_ref[h, group * k + d], g) for g in range(width)] for h in range(2)] for d in range(group)]

        def plane(x, carry):
            for y in range(0, ny, 8):
                b = [b_ref[g, x, y : y + 8, :] for g in range(width)]
                u = [u_ref[g, x, y : y + 8, :] for g in range(width)]
                for d in range(group):
                    total = first[d][0][0] * b[0] + first[d][1][0] * u[0]
                    for g in range(1, width):
                        total = total + (first[d][0][g] * b[g] + first[d][1][g] * u[g])
                    out_ref[group * k + d, x, y : y + 8, :] = total
            return carry

        return lax.fori_loop(0, nx, plane, carry, unroll=nx)

    lax.fori_loop(0, width // group, fields, 0)


def call(kernel, out_shape, operands, scratch=(), flops=1_000_000, name=None, aliases=None):
    return pl.pallas_call(
        kernel,
        out_shape=out_shape,
        in_specs=[pl.BlockSpec(memory_space=pltpu.VMEM)] * len(operands),
        out_specs=jax.tree.map(lambda _: pl.BlockSpec(memory_space=pltpu.VMEM), out_shape),
        scratch_shapes=list(scratch),
        input_output_aliases=aliases or {},
        compiler_params=pltpu.CompilerParams(vmem_limit_bytes=8 << 20),
        cost_estimate=pl.CostEstimate(flops=flops, bytes_accessed=1 << 20, transcendentals=0),
        name=name,
    )(*operands)


def trade(turn, axis, faces):
    out = []
    for k, (face, pairs) in enumerate(zip(faces, swap_pairs(lax.axis_size(axis)))):
        with jax.named_scope(f"turn{turn}_{axis}_{k}"):
            out.append(swap(face, axis, pairs))
    return out


def body(right_side, shift):
    width, nx, ny, nz = right_side.shape
    assert width == 8 and nz == LANES and ny % 8 == 0 and nx > 2 and width * nx <= LANES // 2 and ny <= 8 * nx and ny * nx <= 4 * LANES
    nx_r, ny_r, nz_r = rounds_of()
    devices = 1
    for axis in AXES:
        devices *= lax.axis_size(axis)
    assert nz_r > 0
    block = jax.ShapeDtypeStruct(right_side.shape, F32)
    full = pltpu.VMEM(right_side.shape, F32)
    kernel = functools.partial

    def x_faces(extra):
        return [jax.ShapeDtypeStruct((width * ny // 8 + extra, 8, nz), F32)] * nx_r

    def y_faces(fields):
        return [jax.ShapeDtypeStruct((fields, nx, 1, nz), F32)] * ny_r

    def ends_of(layers):
        return jax.ShapeDtypeStruct((layers, ny, LANES), F32)

    faces = call(cut_x_kernel, x_faces(0), [right_side], name="cut")
    halo_x = trade(1, "gx", faces)
    packed = call(
        kernel(pack_kernel, ny_r),
        [*y_faces(width), jax.ShapeDtypeStruct((ny, LANES), F32), *[jax.ShapeDtypeStruct((ny // 8 + 1, 8, LANES), F32)] * nz_r],
        [right_side, shift],
        name="pack",
    )
    halo_y, own = trade(1, "gy", packed[:ny_r]), packed[ny_r]
    halo_z = trade(1, "gz", packed[ny_r + 1 :])
    outer, ends, *faces = call(
        kernel(outer_operator_kernel, nx_r, ny_r, nz_r),
        [block, ends_of(2), *x_faces(1)],
        [right_side, shift, own, *halo_x, *halo_y, *halo_z],
        name="outer1",
    )
    halo_x = trade(2, "gx", faces)
    u, *faces = call(
        kernel(inner_operator_kernel, ny_r),
        [block, *y_faces(width + 1)],
        [right_side, shift, outer, ends, *halo_y],
        aliases={2: 0},
        flops=20_000_000,
        name="inner1",
    )
    halo_y = trade(2, "gy", faces)
    early = call(early_moments_kernel, jax.ShapeDtypeStruct((8, LANES), F32), [right_side, u], flops=15_000_000, name="early")
    sums = call(
        kernel(inner_late_kernel, ny_r),
        jax.ShapeDtypeStruct((2, len(pairs_of(width)), 8, LANES), F32),
        [u, shift, ends, *halo_y],
        scratch=[full],
        flops=15_000_000,
        name="inner2",
    )
    copies = call(
        kernel(outer_late_kernel, nx_r, ny_r),
        jax.ShapeDtypeStruct((devices, 4, LANES), F32),
        [u, shift, ends, sums, early, *halo_x, *halo_y],
        scratch=[full],
        name="outer2",
    )
    parts = lax.all_to_all(copies, AXES, 0, 0, tiled=True)
    out, norms = call(
        finish_kernel,
        [block, jax.ShapeDtypeStruct((1, width), F32)],
        [parts, right_side, u],
        scratch=[pltpu.VMEM((2, width, 8, LANES), F32)],
        name="finish",
    )
    return out, norms.reshape(width)


def solution(mesh):
    in_specs = (P(None, "gx", "gy", "gz"), P("gx", "gy", "gz"))
    out_specs = (P(None, "gx", "gy", "gz"), P())
    return jax.shard_map(body, mesh=mesh, in_specs=in_specs, out_specs=out_specs, check_vma=False)
```

```python
import functools

import jax
import jax.numpy as jnp
from jax import lax
from jax.experimental import pallas as pl
from jax.experimental.pallas import tpu as pltpu
from jax.sharding import PartitionSpec as P

AXES = ("gx", "gy", "gz")
CENTRE = 4.0
LANES = 128
F32 = jnp.float32


def swap_pairs(count):
    first = [(i, j) for a in range(0, count - 1, 2) for i, j in ((a, a + 1), (a + 1, a))]
    second = [(i, j) for a in range(1, count - 1, 2) for i, j in ((a, a + 1), (a + 1, a))]
    return [pairs for pairs in (first, second) if pairs]


def swap(values, axis, pairs):
    side = lax.axis_size("gy")
    if axis == "gy" or side % 2:
        return lax.ppermute(values, axis, pairs)
    count = lax.axis_size(axis)
    named = {i for i, _ in pairs}
    at = (lambda i, y: i * side + y) if axis == "gx" else (lambda i, y: y * count + i)
    joint = [(at(i, y), at(j, y)) for i, j in pairs for y in range(side)]
    joint += [(at(i, y), at(i, y ^ 1)) for i in range(count) if i not in named for y in range(side)]
    return lax.ppermute(values, ("gx", "gy") if axis == "gx" else ("gy", "gz"), joint)


def rounds_of():
    return tuple(len(swap_pairs(lax.axis_size(axis))) for axis in AXES)


def parity(axis):
    return lax.rem(lax.axis_index(axis), 2) == 1


def x_plane(k, nx):
    return jnp.where(jnp.logical_xor(parity("gx"), k == 0), nx - 1, 0)


def cut_x_kernel(v_ref, *refs):
    for k, ref in enumerate(refs):
        ref[...] = v_ref[:, x_plane(k, v_ref.shape[1])].reshape(ref.shape)


def write_y_faces(v_ref, y_refs):
    ny = v_ref.shape[2]
    odd = parity("gy")
    for k, ref in enumerate(y_refs):
        high = jnp.logical_xor(odd, k == 0)
        ref[...] = jnp.where(high, v_ref[:, :, ny - 1 : ny, :], v_ref[:, :, 0:1, :])


def packed_ends(tile, m, lane, near, far=None):
    def at(offset):
        return lane == lax.rem(2 * m + offset + LANES, LANES)

    turned = pltpu.roll(tile, 2 * m, 1)
    near = jnp.where(at(0) | at(-1), turned, near)
    if far is None:
        return near
    return near, jnp.where(at(1) | at(-2), turned, far)


def pack_kernel(ny_r, v_ref, shift_ref, *refs):
    width, nx, ny, _ = v_ref.shape
    y_refs, (near_ref, *z_refs) = refs[:ny_r], refs[ny_r:]
    write_y_faces(v_ref, y_refs)
    lane = lax.broadcasted_iota(jnp.int32, (ny, LANES), 1)
    nothing = jnp.zeros((ny, LANES), F32)

    def field(f, packed):
        for x in range(nx):
            packed = packed_ends(v_ref[f, x], f * nx + x, lane, *packed)
        return packed

    near, far = lax.fori_loop(0, width, field, (nothing, nothing), unroll=width)
    diagonal = nothing
    for x in range(nx):
        diagonal = packed_ends((6.0 - CENTRE) + shift_ref[x], x, lane, diagonal)
    groups = ny // 8
    folded = sum(shift_lanes(diagonal[8 * r : 8 * r + 8], 2 * nx * r) for r in range(groups))
    near_ref[...] = near
    for k, ref in enumerate(z_refs):
        first = jnp.where(jnp.logical_xor(parity("gz"), k == 0), 1, 0)
        ref[:groups] = jnp.where(lax.rem(lane, 2) == first, near, far).reshape(groups, 8, LANES)
        ref[groups] = folded


def pick(axis, refs, load):
    if not refs:
        return 0.0, 0.0
    odd, at = parity(axis), lax.axis_index(axis)
    first = load(refs[0])
    second = load(refs[1]) if len(refs) > 1 else jnp.zeros_like(first)
    low = jnp.where(at == 0, 0.0, jnp.where(odd, first, second))
    high = jnp.where(at == lax.axis_size(axis) - 1, 0.0, jnp.where(odd, second, first))
    return low, high


def by_side(low, high, by):
    lane = lax.broadcasted_iota(jnp.int32, low.shape, 1)
    return jnp.where(lax.rem(lane, 2) == 0, shift_lanes(low, by), shift_lanes(high, -by))


def halo_ends(z_in, nx, width):
    groups = z_in[0].shape[0] - 1
    low, high = pick("gz", z_in, lambda ref: ref[:groups].reshape(8 * groups, LANES))
    folded = by_side(*pick("gz", z_in, lambda ref: ref[groups]), 1)
    lane = lax.broadcasted_iota(jnp.int32, folded.shape, 1)
    mine = lax.rem(lane + 1, LANES) < 2 * nx
    rows = [jnp.where(mine, shift_lanes(folded, -2 * nx * r), 0.0) for r in range(groups)]
    diagonal, copies = jnp.concatenate(rows, axis=0), 1
    while copies < width:
        diagonal = diagonal + shift_lanes(diagonal, 2 * nx * copies)
        copies *= 2
    return by_side(low, high, 1), by_side(low, high, 2), diagonal


def inside_grid(lane):
    low = jnp.where(lax.axis_index("gz") == 0, 0.0, 1.0)
    high = jnp.where(lax.axis_index("gz") == lax.axis_size("gz") - 1, 0.0, 1.0)
    return jnp.where(lax.rem(lane, 2) == 0, low, high)


def lane_x(lane, nx):
    return lax.rem((lane + 1) // 2, nx)


def fold_plane(ends, x, nx):
    ny = ends.shape[0]
    lane = lax.broadcasted_iota(jnp.int32, (8, LANES), 1)
    mine = lane_x(lane, nx) == x
    groups = [jnp.where(mine, ends[8 * r : 8 * r + 8], 0.0) for r in range(ny // 8)]
    return sum(pltpu.roll(group, lax.rem(LANES + 2 * r - 2 * x, LANES), 1) for r, group in enumerate(groups))


def unfold_plane(folded, x, ny):
    return jnp.concatenate([shift_lanes(folded, 2 * x - 2 * r) for r in range(ny // 8)], axis=0)


def operator_on_ends(nx, width, own, z_in):
    near, far, diagonal = halo_ends(z_in, nx, width)
    ny = near.shape[0]
    lane = lax.broadcasted_iota(jnp.int32, near.shape, 1)
    row = lax.broadcasted_iota(jnp.int32, near.shape, 0)
    x = lane_x(lane, nx)
    beside = own + far
    beside += jnp.where(x == 0, 0.0, pltpu.roll(near, 2, 1)) + jnp.where(x == nx - 1, 0.0, pltpu.roll(near, LANES - 2, 1))
    beside += jnp.where(row == 0, 0.0, pltpu.roll(near, 1, 0)) + jnp.where(row == ny - 1, 0.0, pltpu.roll(near, ny - 1, 0))
    return near, inside_grid(lane) * (diagonal * near - beside)


def finished_ends(nx, base, x_in, y_in, width):
    ny = base.shape[0]
    lane = lax.broadcasted_iota(jnp.int32, base.shape, 1)
    row = lax.broadcasted_iota(jnp.int32, base.shape, 0)
    low_y, high_y = pick("gy", y_in, lambda ref: ref[width, 0])
    beside = jnp.where(row == 0, low_y, 0.0) + jnp.where(row == ny - 1, high_y, 0.0)
    if x_in:
        x = lane_x(lane, nx)
        low_x, high_x = pick("gx", x_in, lambda ref: ref[ref.shape[0] - 1])
        beside += jnp.where(x == 0, unfold_plane(low_x, 0, ny), 0.0)
        beside += jnp.where(x == nx - 1, unfold_plane(high_x, nx - 1, ny), 0.0)
    return base - inside_grid(lane) * beside


def face_of(ref, f, ny):
    groups = ny // 8
    return ref[pl.ds(f * groups, groups)].reshape(ny, LANES)


def apply_operator(planes, v_ref, shift_ref, x_in, y_in, ends, out_ref):
    width, nx, ny, _ = v_ref.shape
    lane = lax.broadcasted_iota(jnp.int32, (ny, LANES), 1)
    row = lax.broadcasted_iota(jnp.int32, (ny, LANES), 0)
    def field(f, carry):
        low_x, high_x = pick("gx", x_in, lambda ref: face_of(ref, f, ny))
        for x in planes:
            low_y, high_y = pick("gy", y_in, lambda ref: ref[f, x])
            v = v_ref[f, x]
            end = pltpu.roll(ends, lax.rem(LANES - 2 * (f * nx + x), LANES), 1)
            beside = (v_ref[f, x - 1] if x > 0 else low_x) + (v_ref[f, x + 1] if x < nx - 1 else high_x)
            beside += jnp.where(row == 0, low_y, pltpu.roll(v, 1, 0))
            beside += jnp.where(row == ny - 1, high_y, pltpu.roll(v, ny - 1, 0))
            beside += jnp.where(lane == 0, end, pltpu.roll(v, 1, 1))
            beside += jnp.where(lane == LANES - 1, end, pltpu.roll(v, LANES - 1, 1))
            out_ref[f, x] = ((6.0 - CENTRE) + shift_ref[x]) * v - beside
        return carry

    lax.fori_loop(0, width, field, 0, unroll=width)


def split(refs, *counts):
    parts, at = [], 0
    for count in counts:
        parts.append(refs[at : at + count])
        at += count
    return (*parts, refs[at:])


def inner_planes(ref):
    return range(1, ref.shape[1] - 1)


def outer_planes(ref):
    return (0, ref.shape[1] - 1)


def inner_operator_kernel(ny_r, nz_r, v_ref, shift_ref, own_ref, *refs):
    y_in, z_in, (out_ref, ends_ref) = split(refs, ny_r, nz_r)
    near, base = operator_on_ends(v_ref.shape[1], v_ref.shape[0], own_ref[...], z_in)
    ends_ref[0] = near
    ends_ref[1] = base
    apply_operator(inner_planes(v_ref), v_ref, shift_ref, (), y_in, near, out_ref)


def outer_operator_kernel(nx_r, ny_r, v_ref, shift_ref, inner_ref, ends_ref, *refs):
    x_in, y_in, (out_ref,), x_out, y_out = split(refs, nx_r, ny_r, 1, nx_r)
    width, nx, ny, _ = v_ref.shape
    near = ends_ref[0]
    apply_operator(outer_planes(v_ref), v_ref, shift_ref, x_in, y_in, near, out_ref)
    for k, ref in enumerate(x_out):
        plane, rows = x_plane(k, nx), width * ny // 8
        ref[:rows] = out_ref[:, plane].reshape(rows, 8, LANES)
        ref[rows] = fold_plane(near, plane, nx)
    write_y_faces(out_ref, [ref.at[:width] for ref in y_out])
    for k, ref in enumerate(y_out):
        high = jnp.logical_xor(parity("gy"), k == 0)
        line = jnp.where(high, near[ny - 1 : ny], near[0:1])
        for x in range(nx):
            ref[width, x] = line


def pairs_of(width):
    return [(i, j) for i in range(width) for j in range(i + 1)]


def moment_sums(first, last, step, a_ref, b_ref, sums):
    width, _, ny, _ = a_ref.shape
    pairs = pairs_of(width)

    def plane(k, sums):
        sums, x = list(sums), first + k * step
        for y in range(0, ny, 8):
            a = [a_ref[f, x, y : y + 8, :] for f in range(width)]
            b = a if b_ref is a_ref else [b_ref[f, x, y : y + 8, :] for f in range(width)]
            for k, (i, j) in enumerate(pairs):
                sums[k] = sums[k] + a[i] * b[j]
        return tuple(sums)

    return lax.fori_loop(0, -((first - last) // step), plane, tuple(sums), unroll=2)


def no_sums(width):
    return [jnp.zeros((8, LANES), F32) for _ in pairs_of(width)]


def put_moment(width, sums, at, payload):
    rows = {}
    for (i, j), value in zip(pairs_of(width), sums):
        rows[i, j] = rows[j, i] = jnp.sum(value, axis=0, keepdims=True)
    lane = lax.broadcasted_iota(jnp.int32, (8, LANES), 1)
    for i in range(width):
        column = jnp.sum(jnp.concatenate([rows[i, j] for j in range(width)], axis=0), axis=1, keepdims=True)
        payload = jnp.where(lane == at + i, column, payload)
    return payload


def early_moments_kernel(b_ref, u_ref, out_ref):
    width, nx = b_ref.shape[:2]
    payload = jnp.zeros((8, LANES), F32)
    for k, (left, right) in enumerate(((b_ref, b_ref), (b_ref, u_ref), (u_ref, u_ref))):
        payload = put_moment(width, moment_sums(0, nx, 1, left, right, no_sums(width)), k * width, payload)
    out_ref[...] = payload


def inner_late_kernel(ny_r, u_ref, shift_ref, ends_ref, *refs):
    y_in, (sums_ref, t_ref) = split(refs, ny_r)
    width, nx = u_ref.shape[:2]
    ends = finished_ends(nx, ends_ref[1], (), y_in, width)
    apply_operator(inner_planes(u_ref), u_ref, shift_ref, (), y_in, ends, t_ref)
    for h, left in enumerate((u_ref, t_ref)):
        for k, value in enumerate(moment_sums(1, nx - 1, 1, left, t_ref, no_sums(width))):
            sums_ref[h, k] = value


def outer_late_kernel(nx_r, ny_r, u_ref, shift_ref, ends_ref, sums_ref, early_ref, *refs):
    x_in, y_in, (out_ref, t_ref) = split(refs, nx_r, ny_r)
    width, nx = u_ref.shape[:2]
    ends = finished_ends(nx, ends_ref[1], x_in, y_in, width)
    apply_operator(outer_planes(u_ref), u_ref, shift_ref, x_in, y_in, ends, t_ref)
    payload = early_ref[...]
    for h, left in enumerate((u_ref, t_ref)):
        inner = [sums_ref[h, k] for k in range(len(pairs_of(width)))]
        payload = put_moment(width, moment_sums(0, nx, nx - 1, left, t_ref, inner), (3 + h) * width, payload)
    folded = payload[:4] + shift_lanes(payload, LANES // 2)[4:]
    out_ref[...] = jnp.broadcast_to(folded[None], out_ref.shape)


def lanes_of(matrix, j):
    return jnp.broadcast_to(matrix[:, j : j + 1], matrix.shape)


def rows_of(matrix, i):
    return jnp.broadcast_to(matrix[i : i + 1, :], matrix.shape)


def times(left, at, right):
    count = left.shape[0]
    total = lanes_of(left, at) * rows_of(right, 0)
    for k in range(1, count):
        total = total + lanes_of(left, at + k) * rows_of(right, k)
    return total


def shift_lanes(matrix, by):
    return pltpu.roll(matrix, by % LANES, 1)


def solve(columns, right):
    size = right[0].shape[0]
    sub = lax.broadcasted_iota(jnp.int32, right[0].shape, 0)
    for j in range(0, len(columns), 2):
        own, local = divmod(j, size)
        first, second = columns[j], columns[j + 1]
        a, b = rows_of(first[own], local), rows_of(second[own], local)
        c, d = rows_of(first[own], local + 1), rows_of(second[own], local + 1)
        scale = 1.0 / (a * d - b * c)
        a, b, c, d = a * scale, b * scale, c * scale, d * scale

        def step(value):
            upper, lower = rows_of(value[own], local), rows_of(value[own], local + 1)
            upper, lower = d * upper - b * lower, a * lower - c * upper
            value = [v - (f * upper + s * lower) for v, f, s in zip(value, first, second)]
            value[own] = jnp.where(sub == local, upper, jnp.where(sub == local + 1, lower, value[own]))
            return value

        columns = columns[: j + 2] + [step(column) for column in columns[j + 2 :]]
        right = step(right)
    return right


def small_algebra(s):
    n = s.shape[0]
    c0 = CENTRE
    lane = lax.broadcasted_iota(jnp.int32, s.shape, 1)
    sub = lax.broadcasted_iota(jnp.int32, s.shape, 0)
    n0, n1, n2, n3, n4 = shift_lanes(s, n), s, shift_lanes(s, -n), shift_lanes(s, -2 * n), shift_lanes(s, -3 * n)
    (e,) = solve([[lanes_of(s, j)] for j in range(n)], [s])
    p1 = times(s, n, e)
    p2 = times(s, 2 * n, e)
    p3 = times(s, 3 * n, e)
    cc = times(e, n, e)
    e2c = times(e, 2 * n, e)
    e2 = shift_lanes(e, -n)
    g = n2 - p1
    q = e2 - cc
    n3c = n3 - p2
    f3 = n3c - times(s, n, q)
    f4 = n4 - p3 - times(s, n, shift_lanes(e, -2 * n) - e2c)
    m11 = n2 + 2.0 * c0 * n1 + c0 * c0 * n0
    m12 = n3c + 2.0 * c0 * g
    m21 = n3 - times(s, n, e2) + 2.0 * c0 * g
    m22 = f4 + 2.0 * c0 * f3 + c0 * c0 * g
    columns = [[lanes_of(m11, n + j), lanes_of(m21, n + j)] for j in range(n)]
    columns += [[lanes_of(m12, n + j), lanes_of(m22, n + j)] for j in range(n)]
    pa, qa = solve(columns, [n1 + c0 * n0, g])
    on_b = pa - times(e, n, qa)
    unit = jnp.where(lane == sub + n, 1.0, 0.0)
    part = unit - times(e, n, pa) - c0 * pa - times(q, n, qa)
    squares = part * times(s, 0, part)
    pq = pa + c0 * qa
    squares = squares + pq * (times(g, n, pq) + 2.0 * times(f3, n, qa))
    squares = squares + qa * times(f4 - times(g, n, q), n, qa)
    return on_b, qa, jnp.sum(squares, axis=0, keepdims=True)


def finish_kernel(parts_ref, b_ref, u_ref, out_ref, norms_ref, coeff_ref):
    width, nx, ny, _ = b_ref.shape
    n = width
    folded = jnp.sum(parts_ref[...], axis=0)
    total = jnp.concatenate([folded, shift_lanes(folded, LANES // 2)], axis=0)
    on_b, on_u, squares = small_algebra(total)
    norms_ref[...] = jnp.sqrt(shift_lanes(squares, -n))[:, :n]
    for f in range(width):
        coeff_ref[0, f] = lanes_of(on_b, n + f)
        coeff_ref[1, f] = lanes_of(on_u, n + f)
    group = 2

    def fields(k, carry):
        first = [[[rows_of(coeff_ref[h, group * k + d], g) for g in range(width)] for h in range(2)] for d in range(group)]

        def plane(x, carry):
            for y in range(0, ny, 8):
                b = [b_ref[g, x, y : y + 8, :] for g in range(width)]
                u = [u_ref[g, x, y : y + 8, :] for g in range(width)]
                for d in range(group):
                    total = first[d][0][0] * b[0] + first[d][1][0] * u[0]
                    for g in range(1, width):
                        total = total + (first[d][0][g] * b[g] + first[d][1][g] * u[g])
                    out_ref[group * k + d, x, y : y + 8, :] = total
            return carry

        return lax.fori_loop(0, nx, plane, carry, unroll=nx)

    lax.fori_loop(0, width // group, fields, 0, unroll=2)


def call(kernel, out_shape, operands, scratch=(), flops=1_000_000, name=None, aliases=None):
    return pl.pallas_call(
        kernel,
        out_shape=out_shape,
        in_specs=[pl.BlockSpec(memory_space=pltpu.VMEM)] * len(operands),
        out_specs=jax.tree.map(lambda _: pl.BlockSpec(memory_space=pltpu.VMEM), out_shape),
        scratch_shapes=list(scratch),
        input_output_aliases=aliases or {},
        compiler_params=pltpu.CompilerParams(vmem_limit_bytes=8 << 20),
        cost_estimate=pl.CostEstimate(flops=flops, bytes_accessed=1 << 20, transcendentals=0),
        name=name,
    )(*operands)


def trade(turn, axis, faces):
    out = []
    for k, (face, pairs) in enumerate(zip(faces, swap_pairs(lax.axis_size(axis)))):
        with jax.named_scope(f"turn{turn}_{axis}_{k}"):
            out.append(swap(face, axis, pairs))
    return out


def body(right_side, shift):
    width, nx, ny, nz = right_side.shape
    assert width == 8 and nz == LANES and ny % 8 == 0 and nx > 2 and width * nx <= LANES // 2 and ny <= 8 * nx and ny * nx <= 4 * LANES
    nx_r, ny_r, nz_r = rounds_of()
    devices = 1
    for axis in AXES:
        devices *= lax.axis_size(axis)
    assert nz_r > 0
    block = jax.ShapeDtypeStruct(right_side.shape, F32)
    full = pltpu.VMEM(right_side.shape, F32)
    kernel = functools.partial

    def x_faces(extra):
        return [jax.ShapeDtypeStruct((width * ny // 8 + extra, 8, nz), F32)] * nx_r

    def y_faces(fields):
        return [jax.ShapeDtypeStruct((fields, nx, 1, nz), F32)] * ny_r

    def ends_of(layers):
        return jax.ShapeDtypeStruct((layers, ny, LANES), F32)

    faces = call(cut_x_kernel, x_faces(0), [right_side], name="cut")
    halo_x = trade(1, "gx", faces)
    packed = call(
        kernel(pack_kernel, ny_r),
        [*y_faces(width), jax.ShapeDtypeStruct((ny, LANES), F32), *[jax.ShapeDtypeStruct((ny // 8 + 1, 8, LANES), F32)] * nz_r],
        [right_side, shift],
        name="pack",
    )
    halo_y, own = trade(1, "gy", packed[:ny_r]), packed[ny_r]
    halo_z = trade(1, "gz", packed[ny_r + 1 :])
    inner, ends = call(
        kernel(inner_operator_kernel, ny_r, nz_r),
        [block, ends_of(2)],
        [right_side, shift, own, *halo_y, *halo_z],
        flops=20_000_000,
        name="inner1",
    )
    u, *faces = call(
        kernel(outer_operator_kernel, nx_r, ny_r),
        [block, *x_faces(1), *y_faces(width + 1)],
        [right_side, shift, inner, ends, *halo_x, *halo_y],
        aliases={2: 0},
        name="outer1",
    )
    halo_x = trade(2, "gx", faces[:nx_r])
    halo_y = trade(2, "gy", faces[nx_r:])
    early = call(early_moments_kernel, jax.ShapeDtypeStruct((8, LANES), F32), [right_side, u], flops=15_000_000, name="early")
    sums = call(
        kernel(inner_late_kernel, ny_r),
        jax.ShapeDtypeStruct((2, len(pairs_of(width)), 8, LANES), F32),
        [u, shift, ends, *halo_y],
        scratch=[full],
        flops=15_000_000,
        name="inner2",
    )
    copies = call(
        kernel(outer_late_kernel, nx_r, ny_r),
        jax.ShapeDtypeStruct((devices, 4, LANES), F32),
        [u, shift, ends, sums, early, *halo_x, *halo_y],
        scratch=[full],
        name="outer2",
    )
    parts = lax.all_to_all(copies, AXES, 0, 0, tiled=True)
    out, norms = call(
        finish_kernel,
        [block, jax.ShapeDtypeStruct((1, width), F32)],
        [parts, right_side, u],
        scratch=[pltpu.VMEM((2, width, 8, LANES), F32)],
        name="finish",
    )
    return out, norms.reshape(width)


def solution(mesh):
    in_specs = (P(None, "gx", "gy", "gz"), P("gx", "gy", "gz"))
    out_specs = (P(None, "gx", "gy", "gz"), P())
    return jax.shard_map(body, mesh=mesh, in_specs=in_specs, out_specs=out_specs, check_vma=False)
```
